8 devices in a mesh: dp: 1 (over z), tp: 2 (over y), ep: 4 (over x, core).
Axes of the slice: x: 2, y: 2, z: 1, core: 2. Of those that a mesh axis runs over, the one named last changes fastest.
Arguments:
- tokens: bfloat16 [16384, 2048], P(('dp', 'ep', 'tp'))
- expert_ids: int32 [16384, 2], P(('dp', 'ep', 'tp'))
- gate_vals: float32 [16384, 2], P(('dp', 'ep', 'tp'))
- w_up: bfloat16 [8, 2048, 5632], P('ep', None, 'tp')
- w_down: bfloat16 [8, 5632, 2048], P('ep', 'tp')
Outputs:
- output: bfloat16 [16384, 2048], P(('dp', 'ep', 'tp'))
All inputs are finite; a program needn't handle non-finite values.
Results may differ from the reference program's by a relative error of at most 0.0013.
Values are sent between devices in bfloat16 or wider.
A program may use at most 1 GiB of HBM per device.

```python
import jax
import jax.numpy as jnp
from jax import lax

EXPERTS = 8
TOP_K = 2
HIDDEN = 2048
FFN_DIM = 5632
TOK_DEV = 2048
EP_SIZE = 4
TP_SIZE = 2

N_SOURCES = EP_SIZE * TP_SIZE
SLOT_CAP = ((5 * TOK_DEV * TOP_K) // (4 * EXPERTS) + 7) // 8 * 8
N_SLOTS = EXPERTS * SLOT_CAP
N_HOT = max(1, EXPERTS // (8 * TOP_K))
HOT_FILL = SLOT_CAP + SLOT_CAP // 8


def draw_routes(perm_key, order_key, offset_key):
    hot_perm = jax.random.permutation(perm_key, EXPERTS).astype(jnp.int32)
    ranks = jnp.arange(TOK_DEV, dtype=jnp.int32)
    first_rank = jnp.where(ranks < N_HOT * HOT_FILL, ranks // HOT_FILL,
                           N_HOT + (ranks - N_HOT * HOT_FILL) % (EXPERTS - N_HOT))
    orders = jax.vmap(lambda sub_key: jax.random.permutation(sub_key, TOK_DEV))(
        jax.random.split(order_key, N_SOURCES))
    first_choice = hot_perm[first_rank[orders]]
    scores = jax.random.randint(offset_key, (N_SOURCES, TOK_DEV, EXPERTS - 1), 0, 2 ** 20) * (EXPERTS - 1)
    scores = scores + jnp.arange(EXPERTS - 1, dtype=jnp.int32)
    picked = lax.top_k(scores, TOP_K)[1][:, :, :TOP_K - 1] + 1
    others = (first_choice[:, :, None] + picked) % EXPERTS
    routes = jnp.concatenate([first_choice[:, :, None], others], axis=2)
    return routes.reshape(N_SOURCES * TOK_DEV, TOP_K).astype(jnp.int32)


def setup_inputs(seed: int = 0, part: int = 0) -> dict:
    part_keys = jax.random.split(jax.random.fold_in(jax.random.key(seed), part), 5)
    weight_keys = jax.random.split(jax.random.key(seed + 1), 2)
    tokens = jax.random.normal(part_keys[0], (N_SOURCES * TOK_DEV, HIDDEN), jnp.float32).astype(jnp.bfloat16)
    expert_ids = draw_routes(part_keys[1], part_keys[2], part_keys[3])
    gate_vals = jax.random.uniform(part_keys[4], (N_SOURCES * TOK_DEV, TOP_K), jnp.float32, 0.5, 1.0)
    w_up = (jax.random.normal(weight_keys[0], (EXPERTS, HIDDEN, FFN_DIM), jnp.float32) * HIDDEN ** -0.5).astype(jnp.bfloat16)
    w_down = (jax.random.normal(weight_keys[1], (EXPERTS, FFN_DIM, HIDDEN), jnp.float32) * FFN_DIM ** -0.5).astype(jnp.bfloat16)
    return {'tokens': tokens, 'expert_ids': expert_ids, 'gate_vals': gate_vals, 'w_up': w_up, 'w_down': w_down}


def slot_table(route_ids):
    expert_hit = (route_ids[:, :, None] == jnp.arange(EXPERTS, dtype=jnp.int32)).astype(jnp.int32)
    chosen = jnp.sum(expert_hit, axis=1)
    prior_count = jnp.cumsum(chosen, axis=0) - chosen
    token_rank = jnp.sum(expert_hit * prior_count[:, None, :], axis=2)
    return jnp.where(token_rank < SLOT_CAP, route_ids * SLOT_CAP + token_rank, -1)


def reference(tokens, expert_ids, gate_vals, w_up, w_down):
    src_rows = tokens.reshape(N_SOURCES, TOK_DEV, HIDDEN)
    src_slots = jax.vmap(slot_table)(expert_ids.reshape(N_SOURCES, TOK_DEV, TOP_K))
    src_gates = gate_vals.reshape(N_SOURCES, TOK_DEV, TOP_K)
    slot_iota = jnp.arange(N_SLOTS, dtype=jnp.int32)

    def dispatch(operands):
        rows_in, slot_ids = operands
        pick_mat = jnp.zeros((N_SLOTS, TOK_DEV), jnp.bfloat16)
        for choice_idx in range(TOP_K):
            pick_mat = pick_mat + (slot_iota[:, None] == slot_ids[None, :, choice_idx]).astype(jnp.bfloat16)
        return jnp.dot(pick_mat, rows_in, preferred_element_type=jnp.float32).astype(jnp.bfloat16)

    buffers = lax.map(dispatch, (src_rows, src_slots))
    per_expert = jnp.transpose(buffers.reshape(N_SOURCES, EXPERTS, SLOT_CAP, HIDDEN), (1, 0, 2, 3))
    per_expert = per_expert.reshape(EXPERTS, N_SOURCES * SLOT_CAP, HIDDEN)

    def expert_ffn(operands):
        rows_in, up_mat, down_mat = operands
        pre_act = jnp.dot(rows_in, up_mat, preferred_element_type=jnp.float32)
        hidden_act = jax.nn.gelu(pre_act, approximate=True).astype(jnp.bfloat16)
        return jnp.dot(hidden_act, down_mat, preferred_element_type=jnp.float32).astype(jnp.bfloat16)

    expert_out = lax.map(expert_ffn, (per_expert, w_up, w_down))
    slot_out = jnp.transpose(expert_out.reshape(EXPERTS, N_SOURCES, SLOT_CAP, HIDDEN), (1, 0, 2, 3))
    slot_out = slot_out.reshape(N_SOURCES, N_SLOTS, HIDDEN)

    def combine(operands):
        results, slot_ids, gate_rows = operands
        gate_sum = jnp.zeros((TOK_DEV, HIDDEN), jnp.float32)
        for choice_idx in range(TOP_K):
            pick_mat = (slot_ids[:, choice_idx, None] == slot_iota[None, :]).astype(jnp.bfloat16)
            picked = jnp.dot(pick_mat, results, preferred_element_type=jnp.float32)
            gate_sum = gate_sum + gate_rows[:, choice_idx, None] * picked
        return gate_sum.astype(jnp.bfloat16)

    moe_out = lax.map(combine, (slot_out, src_slots, src_gates))
    return moe_out.reshape(N_SOURCES * TOK_DEV, HIDDEN)
```

```python
import functools
import math

import jax
import jax.numpy as jnp
from jax import lax
from jax.experimental import pallas as pl
from jax.experimental.pallas import tpu as pltpu
from jax.sharding import PartitionSpec as P

MESH = pl.DeviceIdType.MESH
F32, BF16, I32 = jnp.float32, jnp.bfloat16, jnp.int32
FLIPS = [(0, 0, 0), (1, 0, 0), (0, 0, 1), (0, 1, 0), (1, 0, 1), (1, 1, 0), (0, 1, 1), (1, 1, 1)]
OWN, C, Y, X, YC, XC, XY, XYC = range(8)
N_SRC = 8
CUTS = (0, 1024, 2048, 2560, 2816)


def capacity(tok_count, n_top, n_exp):
    return ((5 * tok_count * n_top) // (4 * n_exp) + 7) // 8 * 8


def gelu(x):
    c = math.sqrt(2.0 / math.pi)
    return x * (0.5 * (1.0 + jnp.tanh(c * (x + 0.044715 * (x * x * x)))))


def tile_of(i, size):
    return pl.ds(pl.multiple_of(i * size, size), size)


def slots_of(ids, experts, cap):
    shape = experts.shape
    hit = (jnp.broadcast_to(ids[0:1], shape) == experts) | (jnp.broadcast_to(ids[1:2], shape) == experts)
    hits = jnp.where(hit, 1, 0)
    lane = lax.broadcasted_iota(I32, shape, 1)
    count, step = hits, 1
    while step < shape[1]:
        count = count + jnp.where(lane >= step, pltpu.roll(count, step, 1), 0)
        step *= 2
    rank = count - hits
    return jnp.where(hit & (rank < cap), rank, -1)


def moe_kernel(cap, ids_hbm, gates_ref, tokens, w_up, w_down,
               out, tok, wuf, wdf, xs_hbm, h_hbm, part_hbm, ret,
               idsg, pad, slot_t, gate_t,
               ids_s, ids_r, tok_s, tok_r, w_s, w_r, ret_s, ret_r, lsem):
    n_tok, hidden = tokens.shape
    ffn = w_up.shape[2]
    tp, ep = lax.axis_index('tp'), lax.axis_index('ep')
    core = lax.rem(ep, 2)

    def place(k):
        fc, fx, fy = FLIPS[k]
        e = ep + (1 - 2 * core) if fc else ep
        e = lax.rem(e + 2, 4) if fx else e
        return (1 - tp if fy else tp), e

    def rcopy(src, dst, send, recv, k):
        t, e = place(k)
        return pltpu.make_async_remote_copy(src_ref=src, dst_ref=dst, send_sem=send, recv_sem=recv,
                                            device_id={'tp': t, 'ep': e}, device_id_type=MESH)

    hops = {Y: (OWN, Y), X: (OWN, X), C: (OWN, C), XY: (Y, X), YC: (Y, C), XC: (X, C), XYC: (XY, C)}

    def tok_copy(k):
        frm, to = hops[k]
        return rcopy(tokens if frm == OWN else tok.at[frm], tok.at[k], tok_s.at[k], tok_r.at[k], to)

    def ids_copy(k):
        frm, to = hops[k]
        return rcopy(ids_hbm if frm == OWN else idsg.at[frm], idsg.at[k], ids_s.at[k], ids_r.at[k], to)

    def up_copy():
        return rcopy(w_up.at[1 - tp], wuf, w_s.at[0], w_r.at[0], Y)

    def down_copy(i):
        rows = pl.ds(CUTS[i], CUTS[i + 1] - CUTS[i])
        return rcopy(w_down.at[1 - tp, rows], wdf.at[rows], w_s.at[1 + i], w_r.at[1 + i], Y)

    barrier = pltpu.get_barrier_semaphore()
    for k in range(1, N_SRC):
        t, e = place(k)
        pl.semaphore_signal(barrier, inc=1, device_id={'tp': t, 'ep': e}, device_id_type=MESH)
    pl.semaphore_wait(barrier, N_SRC - 1)

    for k in (Y, X, C):
        ids_copy(k).start()
        tok_copy(k).start()
    up_copy().start()
    for i in range(len(CUTS) - 1):
        down_copy(i).start()

    own_ids = pltpu.make_async_copy(ids_hbm, idsg.at[OWN], lsem.at[0])
    own_ids.start()
    own_ids.wait()
    row = lax.broadcasted_iota(I32, (N_SRC, n_tok), 0)
    experts = jnp.zeros((N_SRC, n_tok), I32)
    for k in range(N_SRC):
        t, e = place(k)
        experts = jnp.where(row == k, 2 * e + t, experts)
    ids, gates = idsg[OWN], gates_ref[...]
    slots8 = slots_of(ids, experts, cap)
    gates8 = (jnp.where(jnp.broadcast_to(ids[0:1], experts.shape) == experts, jnp.broadcast_to(gates[0:1], experts.shape), 0.0)
              + jnp.where(jnp.broadcast_to(ids[1:2], experts.shape) == experts, jnp.broadcast_to(gates[1:2], experts.shape), 0.0))
    pad[...] = jnp.zeros_like(pad)
    for table, rows8 in ((slot_t, slots8.astype(F32)), (gate_t, gates8)):
        pad[0:N_SRC, :] = rows8

        @pl.loop(0, n_tok // 128)
        def _(i):
            table[tile_of(i, 128), :] = jnp.transpose(pad[:, tile_of(i, 128)])

    my_exp = 2 * ep + tp

    def up_phase(tokbuf, pick, xs, wu, wd, h, part):
        load_u = pltpu.make_async_copy(w_up.at[tp], wu, lsem.at[1])
        load_d = pltpu.make_async_copy(w_down.at[tp], wd, lsem.at[2])
        load_u.start()
        load_d.start()

        def load(k):
            return pltpu.make_async_copy(tokens if k == OWN else tok.at[k], tokbuf, lsem.at[0])

        def put_x(k):
            return pltpu.make_async_copy(xs.at[0], xs_hbm.at[k], lsem.at[3])

        def put_part(k):
            return pltpu.make_async_copy(part, part_hbm.at[k], lsem.at[4])

        def arrive(k):
            if k != OWN:
                ids_copy(k).wait_recv()
                tok_copy(k).wait_recv()
            for j, (frm, _) in hops.items():
                if frm == k and k != OWN:
                    ids_copy(j).start()
                    tok_copy(j).start()
            load(k).start()

        @pl.loop(0, N_SRC)
        def _(k):
            for kk in range(N_SRC):
                pl.when(k == kk)(functools.partial(arrive, kk))
            slots = slots_of(idsg[k], jnp.full((8, n_tok), my_exp, I32), cap)[0:1]

            @pl.loop(0, cap // 80)
            def _(i):
                want = lax.broadcasted_iota(I32, (80, n_tok), 0) + i * 80
                pick[tile_of(i, 80), :] = jnp.where(jnp.broadcast_to(slots, want.shape) == want, 1.0, 0.0).astype(BF16)

            load(0).wait()

            @pl.when(k > 0)
            def _():
                put_x(k - 1).wait()

            @pl.loop(0, hidden // 512)
            def _(n):
                cols = tile_of(n, 512)
                xs[0, :, cols] = jnp.dot(pick[...], tokbuf[:, cols], preferred_element_type=F32).astype(BF16)

            put_x(k).start()

            @pl.when(k == 0)
            def _():
                load_u.wait()
                load_d.wait()

            @pl.loop(0, ffn // 256)
            def _(n):
                cols = tile_of(n, 256)
                h[0, :, cols] = gelu(jnp.dot(xs[0], wu[:, cols], preferred_element_type=F32)).astype(BF16)

            @pl.when(k > 0)
            def _():
                put_part(k - 1).wait()

            @pl.loop(0, hidden // 512)
            def _(n):
                cols = tile_of(n, 512)
                part[:, cols] = jnp.dot(h[0], wd[:, cols], preferred_element_type=F32)

            put_part(k).start()

        put_x(N_SRC - 1).wait()
        put_part(N_SRC - 1).wait()

        def get_x(k, slot):
            return pltpu.make_async_copy(xs_hbm.at[k], xs.at[slot], lsem.at[3 + slot])

        def put_h(k, slot):
            return pltpu.make_async_copy(h.at[slot], h_hbm.at[k], lsem.at[5 + slot])

        up_copy().wait_recv()
        load_f = pltpu.make_async_copy(wuf, wu, lsem.at[1])
        load_f.start()
        get_x(0, 0).start()
        load_f.wait()

        @pl.loop(0, N_SRC)
        def _(k):
            slot = lax.rem(k, 2)
            get_x(k, slot).wait()

            @pl.when(k < N_SRC - 1)
            def _():
                get_x(k + 1, 1 - slot).start()

            @pl.when(k >= 2)
            def _():
                put_h(k - 2, slot).wait()

            @pl.loop(0, ffn // 256)
            def _(n):
                cols = tile_of(n, 256)
                h[slot, :, cols] = gelu(jnp.dot(xs[slot], wu[:, cols], preferred_element_type=F32)).astype(BF16)

            put_h(k, slot).start()

        for k in (N_SRC - 2, N_SRC - 1):
            put_h(k, k % 2).wait()

    pl.run_scoped(up_phase,
                  pltpu.VMEM((n_tok, hidden), BF16), pltpu.VMEM((cap, n_tok), BF16), pltpu.VMEM((2, cap, hidden), BF16),
                  pltpu.VMEM((hidden, ffn), BF16), pltpu.VMEM((ffn, hidden), BF16), pltpu.VMEM((2, cap, ffn), BF16),
                  pltpu.VMEM((cap, hidden), F32))

    wide = CUTS[1]

    def mid_phase(wd, hc, part):
        for c in range(2):
            down_copy(c).wait_recv()
            load_w = pltpu.make_async_copy(wdf.at[pl.ds(c * wide, wide)], wd, lsem.at[0])
            load_w.start()

            def get_h(k, slot):
                return pltpu.make_async_copy(h_hbm.at[k, :, pl.ds(c * wide, wide)], hc.at[slot], lsem.at[1 + slot])

            def get_p(k, slot):
                return pltpu.make_async_copy(part_hbm.at[k], part.at[slot], lsem.at[3 + slot])

            def put_p(k, slot):
                return pltpu.make_async_copy(part.at[slot], part_hbm.at[k], lsem.at[5 + slot])

            get_h(0, 0).start()
            get_p(0, 0).start()
            load_w.wait()

            @pl.loop(0, N_SRC)
            def _(k):
                slot = lax.rem(k, 2)
                get_h(k, slot).wait()
                get_p(k, slot).wait()

                @pl.when(k >= 1)
                def _():
                    put_p(k - 1, 1 - slot).wait()

                @pl.when(k < N_SRC - 1)
                def _():
                    get_h(k + 1, 1 - slot).start()
                    get_p(k + 1, 1 - slot).start()

                @pl.loop(0, hidden // 512)
                def _(n):
                    cols = tile_of(n, 512)
                    part[slot, :, cols] = part[slot, :, cols] + jnp.dot(hc[slot], wd[:, cols], preferred_element_type=F32)

                put_p(k, slot).start()

            put_p(N_SRC - 1, (N_SRC - 1) % 2).wait()

    pl.run_scoped(mid_phase, pltpu.VMEM((wide, hidden), BF16), pltpu.VMEM((2, cap, wide), BF16),
                  pltpu.VMEM((2, cap, hidden), F32))

    last_rows = ffn - CUTS[2]
    head = 512

    def end_phase(res):
        def ret_copies(k):
            j = (k + 6) % 8
            spans = [(0, cap)] if k != XYC else [(0, head), (head, cap - head)]
            return [rcopy(res.at[j, pl.ds(a, n)], ret.at[k, pl.ds(a, n)], ret_s.at[k + i], ret_r.at[k + i], k)
                    for i, (a, n) in enumerate(spans)]

        def finish(wd, hc, part):
            def get_h(k, slot):
                return pltpu.make_async_copy(h_hbm.at[k, :, pl.ds(CUTS[2], last_rows)], hc.at[slot], lsem.at[1 + slot])

            def get_p(k, slot):
                return pltpu.make_async_copy(part_hbm.at[k], part.at[slot], lsem.at[3 + slot])

            get_h(2, 0).start()
            get_p(2, 0).start()
            down_copy(2).wait_recv()
            down_copy(3).wait_recv()
            load_w = pltpu.make_async_copy(wdf.at[pl.ds(CUTS[2], last_rows)], wd, lsem.at[0])
            load_w.start()
            load_w.wait()

            @pl.loop(0, N_SRC)
            def _(j):
                k = lax.rem(j + 2, N_SRC)
                slot = lax.rem(j, 2)
                get_h(k, slot).wait()
                get_p(k, slot).wait()

                @pl.when(j < N_SRC - 1)
                def _():
                    after = lax.rem(j + 3, N_SRC)
                    get_h(after, 1 - slot).start()
                    get_p(after, 1 - slot).start()

                @pl.loop(0, hidden // 512)
                def _(n):
                    cols = tile_of(n, 512)
                    total = part[slot, :, cols] + jnp.dot(hc[slot], wd[:, cols], preferred_element_type=F32)
                    res[j, :, cols] = total.astype(BF16)

                for kk in range(1, N_SRC):
                    @pl.when(k == kk)
                    def _():
                        for copy in ret_copies(kk):
                            copy.start()

        pl.run_scoped(finish, pltpu.VMEM((last_rows, hidden), BF16), pltpu.VMEM((2, cap, last_rows), BF16),
                      pltpu.VMEM((2, cap, hidden), F32))

        def combine(acc, rbuf, obuf):
            rows = 256

            def add(k, a, n, block, first=False, last=False):
                def put(i, slot):
                    return pltpu.make_async_copy(obuf.at[slot], out.at[tile_of(i, rows)], lsem.at[1 + slot])

                @pl.loop(0, n_tok // rows)
                def _(i):
                    r = tile_of(i, rows)
                    want = (lax.broadcasted_iota(I32, (rows, n), 1) + a).astype(F32)
                    pick = jnp.where(jnp.broadcast_to(slot_t[r, k:k + 1], want.shape) == want, 1.0, 0.0).astype(BF16)
                    got = jnp.broadcast_to(gate_t[r, k:k + 1], (rows, hidden)) * jnp.dot(pick, block[...], preferred_element_type=F32)
                    if first:
                        acc[r, :] = got
                    elif last:
                        slot = lax.rem(i, 2)

                        @pl.when(i >= 2)
                        def _():
                            put(i - 2, slot).wait()

                        obuf[slot] = (acc[r, :] + got).astype(BF16)
                        put(i, slot).start()
                    else:
                        acc[r, :] = acc[r, :] + got

                if last:
                    for i in (n_tok // rows - 2, n_tok // rows - 1):
                        put(i, i % 2).wait()

            add(OWN, 0, cap, res.at[6], first=True)
            for k in range(1, N_SRC):
                for copy, (a, n) in zip(ret_copies(k), [(0, cap)] if k != XYC else [(0, head), (head, cap - head)]):
                    copy.wait_recv()
                    get = pltpu.make_async_copy(ret.at[k, pl.ds(a, n)], rbuf.at[pl.ds(0, n)], lsem.at[0])
                    get.start()
                    get.wait()
                    add(k, a, n, rbuf.at[pl.ds(0, n)], last=a + n == cap and k == XYC)

        pl.run_scoped(combine, pltpu.VMEM((n_tok, hidden), F32), pltpu.VMEM((cap, hidden), BF16),
                      pltpu.VMEM((2, 256, hidden), BF16))
        for k in range(1, N_SRC):
            for copy in ret_copies(k):
                copy.wait_send()

    pl.run_scoped(end_phase, pltpu.VMEM((N_SRC, cap, hidden), BF16))

    for k in range(1, N_SRC):
        ids_copy(k).wait_send()
        tok_copy(k).wait_send()
    up_copy().wait_send()
    for i in range(len(CUTS) - 1):
        down_copy(i).wait_send()


def solution(mesh):
    row_spec = P(('dp', 'ep', 'tp'), None)
    n_exp = 2 * mesh.shape['ep']

    def local_moe(tokens, expert_ids, gate_vals, w_up, w_down):
        n_tok, hidden = tokens.shape
        ffn = w_up.shape[2]
        cap = capacity(n_tok, expert_ids.shape[1], n_exp)
        any_spec = pl.BlockSpec(memory_space=pl.ANY)
        shapes = [((n_tok, hidden), BF16), ((N_SRC, n_tok, hidden), BF16), ((hidden, ffn), BF16), ((ffn, hidden), BF16),
                  ((N_SRC, cap, hidden), BF16), ((N_SRC, cap, ffn), BF16), ((N_SRC, cap, hidden), F32), ((N_SRC, cap, hidden), BF16)]
        outs = pl.pallas_call(
            functools.partial(moe_kernel, cap),
            out_shape=[jax.ShapeDtypeStruct(s, d) for s, d in shapes],
            in_specs=[any_spec, pl.BlockSpec(memory_space=pltpu.VMEM), any_spec, any_spec, any_spec],
            out_specs=[any_spec] * len(shapes),
            scratch_shapes=[
                pltpu.VMEM((N_SRC, 2, n_tok), I32), pltpu.VMEM((128, n_tok), F32),
                pltpu.VMEM((n_tok, 128), F32), pltpu.VMEM((n_tok, 128), F32),
                pltpu.SemaphoreType.DMA((N_SRC,)), pltpu.SemaphoreType.DMA((N_SRC,)),
                pltpu.SemaphoreType.DMA((N_SRC,)), pltpu.SemaphoreType.DMA((N_SRC,)),
                pltpu.SemaphoreType.DMA((len(CUTS),)), pltpu.SemaphoreType.DMA((len(CUTS),)),
                pltpu.SemaphoreType.DMA((N_SRC + 1,)), pltpu.SemaphoreType.DMA((N_SRC + 1,)),
                pltpu.SemaphoreType.DMA((7,)),
            ],
            compiler_params=pltpu.CompilerParams(collective_id=0, has_side_effects=True, vmem_limit_bytes=65_000_000),
            name='moe',
        )(expert_ids.T, gate_vals.T, tokens, w_up, w_down)
        return outs[0]

    return jax.shard_map(local_moe, mesh=mesh,
                         in_specs=(row_spec, row_spec, row_spec, P('ep', None, 'tp'), P('ep', 'tp', None)),
                         out_specs=row_spec, check_vma=False)
```

```python
import functools
import math

import jax
import jax.numpy as jnp
from jax import lax
from jax.experimental import pallas as pl
from jax.experimental.pallas import tpu as pltpu
from jax.sharding import PartitionSpec as P

MESH = pl.DeviceIdType.MESH
F32, BF16, I32 = jnp.float32, jnp.bfloat16, jnp.int32
OWN, C, X, XC, Y, YC, XY, XYC = range(8)
N_SRC, N_SIDE = 8, 4
BLK = 128


def capacity(tok_count, n_top, n_exp):
    return ((5 * tok_count * n_top) // (4 * n_exp) + 7) // 8 * 8


def gelu(x):
    c = math.sqrt(2.0 / math.pi)
    return x * (0.5 * (1.0 + jnp.tanh(c * (x + 0.044715 * (x * x * x)))))


def tile_of(i, size):
    return pl.ds(pl.multiple_of(i * size, size), size)


def spread(row, shape):
    return jnp.broadcast_to(row, shape)


def slots_of(ids, experts, cap):
    shape = experts.shape
    hit = (spread(ids[0:1], shape) == experts) | (spread(ids[1:2], shape) == experts)
    hits = jnp.where(hit, 1, 0)
    lane = lax.broadcasted_iota(I32, shape, 1)
    count, step = hits, 1
    while step < shape[1]:
        count = count + jnp.where(lane >= step, pltpu.roll(count, step, 1), 0)
        step *= 2
    rank = count - hits
    return jnp.where(hit & (rank < cap), rank, -1)


def gates_of(ids, gates, experts):
    shape = experts.shape
    return (jnp.where(spread(ids[0:1], shape) == experts, spread(gates[0:1], shape), 0.0)
            + jnp.where(spread(ids[1:2], shape) == experts, spread(gates[1:2], shape), 0.0))


def moe_kernel(cap, cuts, ids_hbm, gates_hbm, tokens, w_up, w_down,
               out, tok, st_up, st_down, wuf, wdf, xs_hbm, h_hbm, part_hbm, rp, rh, rows_hbm,
               idsg, gatesg, pad, tab_h, tab_p,
               ids_s, ids_r, tok_s, tok_r, st_s, st_r, wo_s, wo_r, wm_s, wm_r, row_s, row_r, y_s, y_r, lsem, loc):
    n_tok, hidden = tokens.shape
    ffn = w_up.shape[2]
    n_cut = len(cuts) - 1
    n_blk, n_rnd = n_tok // BLK, cap // BLK
    tp, ep = lax.axis_index('tp'), lax.axis_index('ep')
    core = lax.rem(ep, 2)

    def place(k):
        e = ep + (1 - 2 * core) if k & 1 else ep
        e = lax.rem(e + 2, 4) if k & 2 else e
        return (1 - tp if k & 4 else tp), e

    def rcopy(src, dst, send, recv, k):
        t, e = place(k)
        return pltpu.make_async_remote_copy(src_ref=src, dst_ref=dst, send_sem=send, recv_sem=recv,
                                            device_id={'tp': t, 'ep': e}, device_id_type=MESH)

    hops = {Y: (OWN, Y), X: (OWN, X), C: (OWN, C), XY: (Y, X), YC: (Y, C), XC: (X, C), XYC: (XY, C)}

    def tok_copy(k):
        frm, to = hops[k]
        return rcopy(tokens if frm == OWN else tok.at[frm], tok.at[k], tok_s.at[k], tok_r.at[k], to)

    def ids_copy(k):
        frm, to = hops[k]
        return rcopy(ids_hbm if frm == OWN else idsg.at[frm], idsg.at[k], ids_s.at[k], ids_r.at[k], to)

    def gate_copy():
        return rcopy(gates_hbm, gatesg.at[1], ids_s.at[OWN], ids_r.at[OWN], Y)

    def spans(i):
        lo, hi = (0, hidden) if i == 0 else (cuts[i - 1], cuts[i])
        mid = (lo + hi) // 2
        return pl.ds(lo, mid - lo), pl.ds(mid, hi - mid)

    def stage_copy(i):
        rows = spans(i)[1]
        src, dst = (w_up, st_up) if i == 0 else (w_down, st_down)
        at = pl.ds(0, rows.size) if i == 0 else pl.ds(cuts[i - 1] // 2, rows.size)
        return rcopy(src.at[1 - tp, rows], dst.at[at], st_s.at[i], st_r.at[i], C)

    def own_copy(i):
        rows = spans(i)[0]
        src, dst = (w_up, wuf) if i == 0 else (w_down, wdf)
        return rcopy(src.at[1 - tp, rows], dst.at[rows], wo_s.at[i], wo_r.at[i], Y)

    def mate_copy(i):
        rows = spans(i)[1]
        src, dst = (st_up, wuf) if i == 0 else (st_down, wdf)
        at = pl.ds(0, rows.size) if i == 0 else pl.ds(cuts[i - 1] // 2, rows.size)
        return rcopy(src.at[at], dst.at[rows], wm_s.at[i], wm_r.at[i], YC)

    pieces = range(n_cut + 1)

    def wait_piece(i):
        own_copy(i).wait_recv()
        mate_copy(i).wait_recv()

    barrier = pltpu.get_barrier_semaphore()
    for k in range(1, N_SRC):
        t, e = place(k)
        pl.semaphore_signal(barrier, inc=1, device_id={'tp': t, 'ep': e}, device_id_type=MESH)
    pl.semaphore_wait(barrier, N_SRC - 1)

    gate_copy().start()
    for k in (Y, X, C):
        ids_copy(k).start()
        tok_copy(k).start()
    for i in pieces:
        stage_copy(i).start()

    def send_weights():
        for i in pieces:
            stage_copy(i).wait_recv()

        def first_own(group):
            for i in group:
                own_copy(i).start()

        def first_mate(group):
            for i in group:
                mate_copy(i).start()

        for group in ((0,), range(1, n_cut + 1)):
            @pl.when(core == 0)
            def _():
                first_own(group)
                first_mate(group)

            @pl.when(core == 1)
            def _():
                first_mate(group)
                first_own(group)

    def exp_rows(side, rels):
        row = lax.broadcasted_iota(I32, (8, n_tok), 0)
        experts = jnp.zeros((8, n_tok), I32)
        for i, k in enumerate(rels):
            t, e = place(k)
            experts = jnp.where(row == i, 2 * e + t, experts)
        return experts

    def turn(table):
        @pl.loop(0, n_tok // 128)
        def _(i):
            table[tile_of(i, 128), :] = jnp.transpose(pad[:, tile_of(i, 128)])

    own_ids = pltpu.make_async_copy(ids_hbm, idsg.at[OWN], lsem.at[0])
    own_gates = pltpu.make_async_copy(gates_hbm, gatesg.at[0], lsem.at[1])
    own_ids.start()
    own_gates.start()
    own_ids.wait()
    own_gates.wait()
    pad[...] = jnp.zeros_like(pad)

    def home_table():
        experts = exp_rows(0, range(N_SRC))
        slots = slots_of(idsg[OWN], experts, cap)
        gates = gates_of(idsg[OWN], gatesg[0], experts)
        far = (slots >= 0) & (lax.broadcasted_iota(I32, slots.shape, 0) >= N_SIDE)
        count = jnp.sum(jnp.where(far, 1.0, 0.0), axis=0, keepdims=True)
        gate = jnp.sum(jnp.where(far, gates, 0.0), axis=0, keepdims=True)
        pad[0:8, :] = slots.astype(F32)
        pad[8:16, :] = gates
        pad[16:24, :] = spread(jnp.where(count > 1.5, 1.0, gate), (8, n_tok))
        turn(tab_h)

    def proxy_table():
        experts = exp_rows(0, range(N_SIDE))
        slots = slots_of(idsg[Y], experts, cap)
        near = (slots >= 0) & (lax.broadcasted_iota(I32, slots.shape, 0) < N_SIDE)
        gates = gates_of(idsg[Y], gatesg[1], experts)
        count = jnp.sum(jnp.where(near, 1.0, 0.0), axis=0, keepdims=True)
        pad[0:8, :] = slots.astype(F32)
        pad[8:16, :] = jnp.where(spread(count, gates.shape) > 1.5, gates, 1.0)
        turn(tab_p)

    home_table()
    my_exp = 2 * ep + tp

    def up_phase(tokbuf, pick, xs, wu, wd, h, part, pre_a, pre_b):
        load_d = pltpu.make_async_copy(w_down.at[tp], wd, lsem.at[2])
        load_d.start()

        def load(k):
            return pltpu.make_async_copy(tokens if k == OWN else tok.at[k], tokbuf, lsem.at[0])

        def put_x(k):
            return pltpu.make_async_copy(xs.at[0], xs_hbm.at[k], lsem.at[3])

        def put_part(k):
            return pltpu.make_async_copy(part, part_hbm.at[k], lsem.at[4])

        def arrive(k):
            if k != OWN:
                ids_copy(k).wait_recv()
                tok_copy(k).wait_recv()
                for j, (frm, _) in hops.items():
                    if frm == k:
                        ids_copy(j).start()
                        tok_copy(j).start()

        def at_top(k):
            if k == X:
                send_weights()
                arrive(Y)
                arrive(X)
                gate_copy().wait_recv()
                proxy_table()
            elif k in (OWN, XY, XYC):
                arrive(k)
            if k in (OWN, X, XY, XYC):
                load(k).start()

        def after_pick(k):
            if k in (C, XC, Y, YC):
                if k != Y:
                    arrive(k)
                load(k).start()

        def up_tiles(x_slot, h_slot):
            def pre(n):
                return jnp.dot(xs[x_slot], wu[:, tile_of(n, 256)], preferred_element_type=F32)

            def post(n, buf):
                h[h_slot, :, tile_of(n, 256)] = gelu(buf[...]).astype(BF16)

            n_t = ffn // 256
            pre_a[...] = pre(0)

            @pl.loop(0, (n_t - 1) // 2)
            def _(i):
                pre_b[...] = pre(2 * i + 1)
                post(2 * i, pre_a)
                pre_a[...] = pre(2 * i + 2)
                post(2 * i + 1, pre_b)

            post(n_t - 1, pre_a)

        def near(k, lo):
            for kk in range(N_SRC):
                pl.when(k == kk)(functools.partial(at_top, kk))
            slots = slots_of(idsg[k], jnp.full((8, n_tok), my_exp, I32), cap)[0:1]

            @pl.loop(0, cap // 80)
            def _(i):
                want = lax.broadcasted_iota(I32, (80, n_tok), 0) + i * 80
                pick[tile_of(i, 80), :] = jnp.where(spread(slots, want.shape) == want, 1.0, 0.0).astype(BF16)

            load(0).wait()

            @pl.when(k > lo)
            def _():
                put_x(k - 1).wait()

            @pl.loop(0, hidden // 512)
            def _(n):
                cols = tile_of(n, 512)
                xs[0, :, cols] = jnp.dot(pick[...], tokbuf[:, cols], preferred_element_type=F32).astype(BF16)

            put_x(k).start()
            for kk in range(N_SRC - 1):
                pl.when(k == kk)(functools.partial(after_pick, kk + 1))
            up_tiles(0, 0)

            @pl.when(k > lo)
            def _():
                put_part(k - 1).wait()

            @pl.loop(0, hidden // 512)
            def _(n):
                cols = tile_of(n, 512)
                part[:, cols] = jnp.dot(h[0], wd[:, cols], preferred_element_type=F32)

            put_part(k).start()

        def get_x(k, slot):
            return pltpu.make_async_copy(xs_hbm.at[k], xs.at[slot], lsem.at[3 + slot])

        def put_h(k, slot):
            return pltpu.make_async_copy(h.at[slot], h_hbm.at[k], lsem.at[5 + slot])

        @pl.loop(0, 2)
        def _(rnd):
            lo = rnd * (6 + 2 * core)
            hi = 8 - 2 * (1 - core) * (1 - rnd)

            @pl.when(lo < hi)
            def _():
                load_u = pltpu.make_async_copy(w_up.at[tp], wu, lsem.at[1])
                load_u.start()
                load_u.wait()

                @pl.when(rnd == 0)
                def _():
                    load_d.wait()

                @pl.loop(lo, hi)
                def _(k):
                    near(k, lo)

                put_x(hi - 1).wait()
                put_part(hi - 1).wait()

                @pl.when(rnd == 0)
                def _():
                    wait_piece(0)

                load_f = pltpu.make_async_copy(wuf, wu, lsem.at[1])
                load_f.start()
                get_x(lo, 0).start()
                load_f.wait()

                @pl.loop(lo, hi)
                def _(k):
                    slot = lax.rem(k, 2)
                    get_x(k, slot).wait()

                    @pl.when(k < hi - 1)
                    def _():
                        get_x(k + 1, 1 - slot).start()

                    @pl.when(k >= lo + 2)
                    def _():
                        put_h(k - 2, slot).wait()

                    up_tiles(slot, slot)
                    put_h(k, slot).start()

                put_h(hi - 2, 0).wait()
                put_h(hi - 1, 1).wait()

    pl.run_scoped(up_phase,
                  pltpu.VMEM((n_tok, hidden), BF16), pltpu.VMEM((cap, n_tok), BF16), pltpu.VMEM((2, cap, hidden), BF16),
                  pltpu.VMEM((hidden, ffn), BF16), pltpu.VMEM((ffn, hidden), BF16), pltpu.VMEM((2, cap, ffn), BF16),
                  pltpu.VMEM((cap, hidden), F32), pltpu.VMEM((cap, 256), F32), pltpu.VMEM((cap, 256), F32))

    wide = cuts[1]

    def mid_phase(wd, hc, p_in, p_out):
        for c in range(2):
            wait_piece(1 + c)
            load_w = pltpu.make_async_copy(wdf.at[pl.ds(c * wide, wide)], wd, lsem.at[0])
            load_w.start()

            def src(i):
                return lax.rem(i + N_SIDE, N_SRC)

            def get_h(i, slot):
                return pltpu.make_async_copy(h_hbm.at[src(i), :, pl.ds(c * wide, wide)], hc.at[slot], lsem.at[1 + slot])

            def get_p(i, slot):
                return pltpu.make_async_copy(part_hbm.at[src(i)], p_in.at[slot], lsem.at[3 + slot])

            def put_p(i, slot):
                return pltpu.make_async_copy(p_out.at[slot], part_hbm.at[src(i)], lsem.at[5 + slot])

            get_h(0, 0).start()
            get_p(0, 0).start()
            load_w.wait()

            @pl.loop(0, N_SRC)
            def _(i):
                slot = lax.rem(i, 2)
                get_h(i, slot).wait()
                get_p(i, slot).wait()

                @pl.when(i < N_SRC - 1)
                def _():
                    get_h(i + 1, 1 - slot).start()
                    get_p(i + 1, 1 - slot).start()

                @pl.when(i >= 2)
                def _():
                    put_p(i - 2, slot).wait()

                @pl.loop(0, hidden // 512)
                def _(n):
                    cols = tile_of(n, 512)
                    p_out[slot, :, cols] = p_in[slot, :, cols] + jnp.dot(hc[slot], wd[:, cols], preferred_element_type=F32)

                put_p(i, slot).start()

            for i in (N_SRC - 2, N_SRC - 1):
                put_p(i, i % 2).wait()

    pl.run_scoped(mid_phase, pltpu.VMEM((wide, hidden), BF16), pltpu.VMEM((2, cap, wide), BF16),
                  pltpu.VMEM((2, cap, hidden), F32), pltpu.VMEM((2, cap, hidden), F32))

    def row_copy(block, k, r):
        dst = (rp if k >= N_SIDE else rh).at[k % N_SIDE, tile_of(r, BLK)]
        i = k * n_rnd + r
        if k == OWN:
            return pltpu.make_async_copy(block, dst, row_s.at[i])
        return rcopy(block, dst, row_s.at[i], row_r.at[i], k % N_SIDE)

    def y_copy(block, b):
        return rcopy(block, rows_hbm.at[tile_of(b, BLK)], y_s.at[b], y_r.at[b], Y)

    last_rows = ffn - cuts[2]
    order = (X, XC, OWN, C)

    def end_phase(merged):
        def rounds(res, wd, hc, p_in, rpv, tot):
            def gets(s, slot):
                side = jnp.where(s < n_rnd, N_SIDE, 0)
                r = tile_of(lax.rem(s, n_rnd), BLK)
                copies = []
                for q in range(N_SIDE):
                    k = side + order[q]
                    copies.append(pltpu.make_async_copy(h_hbm.at[k, r, pl.ds(cuts[2], last_rows)], hc.at[slot, q], loc.at[slot, 0, q]))
                    copies.append(pltpu.make_async_copy(part_hbm.at[k, r], p_in.at[slot, q], loc.at[slot, 1, q]))
                return copies

            rpv[...] = jnp.zeros_like(rpv)
            for copy in gets(0, 0):
                copy.start()
            for i in range(3, n_cut + 1):
                wait_piece(i)
            load_w = pltpu.make_async_copy(wdf.at[pl.ds(cuts[2], last_rows)], wd, lsem.at[4])
            load_w.start()
            load_w.wait()
            lead = 1 + (2 * n_rnd - 1) * (1 - core)

            def finish(s):
                slot = lax.rem(s, 2)
                for copy in gets(s, slot):
                    copy.wait()

                @pl.when(s < 2 * n_rnd - 1)
                def _():
                    for copy in gets(s + 1, 1 - slot):
                        copy.start()

                r = lax.rem(s, n_rnd)
                for q in range(N_SIDE):
                    block = res.at[r, q]
                    if order[q] != OWN:
                        @pl.when(s >= n_rnd)
                        def _():
                            row_copy(block, N_SIDE + order[q], r).wait_send()

                    block[...] = (p_in[slot, q] + jnp.dot(hc[slot, q], wd[...], preferred_element_type=F32)).astype(BF16)

                    @pl.when(s < n_rnd)
                    def _():
                        if order[q] == OWN:
                            rpv[0, tile_of(r, BLK)] = block[...]
                        else:
                            row_copy(block, N_SIDE + order[q], r).start()

                    @pl.when(s >= n_rnd)
                    def _():
                        row_copy(block, order[q], r).start()

            def merge(b):
                @pl.when(b < n_rnd)
                def _():
                    block = tile_of(b, BLK)
                    copies = [pltpu.make_async_copy(rp.at[e, block], rpv.at[e, block], lsem.at[e]) for e in range(1, N_SIDE)]
                    for e in range(1, N_SIDE):
                        row_copy(res.at[0, 0], N_SIDE + e, b).wait_recv()
                        copies[e - 1].start()
                    for copy in copies:
                        copy.wait()

                r = tile_of(b, BLK)
                for e in range(N_SIDE):
                    want = lax.broadcasted_iota(I32, (BLK, cap), 1).astype(F32)
                    p = jnp.where(spread(tab_p[r, e:e + 1], want.shape) == want, 1.0, 0.0).astype(BF16)
                    got = spread(tab_p[r, 8 + e:9 + e], (BLK, hidden)) * jnp.dot(p, rpv[e], preferred_element_type=F32)
                    tot[...] = tot[...] + got if e else got
                merged[b] = tot[...].astype(BF16)
                y_copy(merged.at[b], b).start()

            @pl.loop(0, 2 * n_rnd + n_blk)
            def _(s):
                pl.when(s < 2 * n_rnd)(functools.partial(finish, s))
                b = s - lead
                pl.when((b >= 0) & (b < n_blk))(functools.partial(merge, b))

            for k in range(N_SIDE):
                for r in range(n_rnd):
                    copy = row_copy(res.at[r, order.index(k)], k, r)
                    copy.wait() if k == OWN else copy.wait_send()

        pl.run_scoped(rounds, pltpu.VMEM((n_rnd, N_SIDE, BLK, hidden), BF16), pltpu.VMEM((last_rows, hidden), BF16),
                      pltpu.VMEM((2, N_SIDE, BLK, last_rows), BF16), pltpu.VMEM((2, N_SIDE, BLK, hidden), F32),
                      pltpu.VMEM((N_SIDE, cap, hidden), BF16), pltpu.VMEM((BLK, hidden), F32))

        def home(acc, rbuf, ybuf, obuf):
            rows = 256
            for e in range(N_SIDE):
                if e != OWN:
                    for r in range(n_rnd):
                        row_copy(rbuf.at[pl.ds(0, BLK)], e, r).wait_recv()
                get = pltpu.make_async_copy(rh.at[e], rbuf, lsem.at[0])
                get.start()
                get.wait()

                @pl.loop(0, n_tok // rows)
                def _(i):
                    r = tile_of(i, rows)
                    want = lax.broadcasted_iota(I32, (rows, cap), 1).astype(F32)
                    p = jnp.where(spread(tab_h[r, e:e + 1], want.shape) == want, 1.0, 0.0).astype(BF16)
                    got = spread(tab_h[r, 8 + e:9 + e], (rows, hidden)) * jnp.dot(p, rbuf[...], preferred_element_type=F32)
                    acc[r, :] = acc[r, :] + got if e else got

            def put(b, slot):
                return pltpu.make_async_copy(obuf.at[slot], out.at[tile_of(b, BLK)], lsem.at[1 + slot])

            @pl.loop(0, n_blk)
            def _(b):
                slot = lax.rem(b, 2)
                r = tile_of(b, BLK)
                y_copy(merged.at[b], b).wait_recv()
                get = pltpu.make_async_copy(rows_hbm.at[r], ybuf, lsem.at[0])
                get.start()

                @pl.when(b >= 2)
                def _():
                    put(b - 2, slot).wait()

                get.wait()
                obuf[slot] = (acc[r, :] + spread(tab_h[r, 16:17], (BLK, hidden)) * ybuf[...].astype(F32)).astype(BF16)
                put(b, slot).start()

            for b in (n_blk - 2, n_blk - 1):
                put(b, b % 2).wait()

        pl.run_scoped(home, pltpu.VMEM((n_tok, hidden), F32), pltpu.VMEM((cap, hidden), BF16),
                      pltpu.VMEM((BLK, hidden), BF16), pltpu.VMEM((2, BLK, hidden), BF16))

        @pl.loop(0, n_blk)
        def _(b):
            y_copy(merged.at[b], b).wait_send()

    pl.run_scoped(end_phase, pltpu.VMEM((n_blk, BLK, hidden), BF16))

    gate_copy().wait_send()
    for k in range(1, N_SRC):
        ids_copy(k).wait_send()
        tok_copy(k).wait_send()
    for i in pieces:
        stage_copy(i).wait_send()
        own_copy(i).wait_send()
        mate_copy(i).wait_send()


def solution(mesh):
    row_spec = P(('dp', 'ep', 'tp'), None)
    n_exp = 2 * mesh.shape['ep']

    def local_moe(tokens, expert_ids, gate_vals, w_up, w_down):
        n_tok, hidden = tokens.shape
        ffn = w_up.shape[2]
        cap = capacity(n_tok, expert_ids.shape[1], n_exp)
        cuts = (0, 1024, 2048, 2560, ffn)
        n_piece = len(cuts)
        any_spec = pl.BlockSpec(memory_space=pl.ANY)
        dma = pltpu.SemaphoreType.DMA
        shapes = [((n_tok, hidden), BF16), ((N_SRC, n_tok, hidden), BF16), ((hidden // 2, ffn), BF16), ((ffn // 2, hidden), BF16),
                  ((hidden, ffn), BF16), ((ffn, hidden), BF16), ((N_SRC, cap, hidden), BF16), ((N_SRC, cap, ffn), BF16),
                  ((N_SRC, cap, hidden), F32), ((N_SIDE, cap, hidden), BF16), ((N_SIDE, cap, hidden), BF16), ((n_tok, hidden), BF16)]
        n_row = N_SRC * (cap // BLK)
        outs = pl.pallas_call(
            functools.partial(moe_kernel, cap, cuts),
            out_shape=[jax.ShapeDtypeStruct(s, d) for s, d in shapes],
            in_specs=[any_spec] * 5,
            out_specs=[any_spec] * len(shapes),
            scratch_shapes=[
                pltpu.VMEM((N_SRC, 2, n_tok), I32), pltpu.VMEM((2, 2, n_tok), F32), pltpu.VMEM((128, n_tok), F32),
                pltpu.VMEM((n_tok, 128), F32), pltpu.VMEM((n_tok, 128), F32),
                dma((N_SRC,)), dma((N_SRC,)), dma((N_SRC,)), dma((N_SRC,)),
                dma((n_piece,)), dma((n_piece,)), dma((n_piece,)), dma((n_piece,)), dma((n_piece,)), dma((n_piece,)),
                dma((n_row,)), dma((n_row,)), dma((n_tok // BLK,)), dma((n_tok // BLK,)),
                dma((8,)), dma((2, 2, N_SIDE)),
            ],
            compiler_params=pltpu.CompilerParams(collective_id=0, has_side_effects=True, vmem_limit_bytes=66_000_000),
            name='moe',
        )(expert_ids.T, gate_vals.T, tokens, w_up, w_down)
        return outs[0]

    return jax.shard_map(local_moe, mesh=mesh,
                         in_specs=(row_spec, row_spec, row_spec, P('ep', None, 'tp'), P('ep', 'tp', None)),
                         out_specs=row_spec, check_vma=False)
```

```python
import functools
import math

import jax
import jax.numpy as jnp
from jax import lax
from jax.experimental import pallas as pl
from jax.experimental.pallas import tpu as pltpu
from jax.sharding import PartitionSpec as P

MESH = pl.DeviceIdType.MESH
F32, BF16, I32 = jnp.float32, jnp.bfloat16, jnp.int32
OWN, C, X, XC, Y, YC, XY, XYC = range(8)
N_SRC, N_SIDE = 8, 4
BLK = 128


def capacity(tok_count, n_top, n_exp):
    return ((5 * tok_count * n_top) // (4 * n_exp) + 7) // 8 * 8


def gelu(x):
    c = math.sqrt(2.0 / math.pi)
    return x * (0.5 * (1.0 + jnp.tanh(c * (x + 0.044715 * (x * x * x)))))


def tile_of(i, size):
    return pl.ds(pl.multiple_of(i * size, size), size)


def spread(row, shape):
    return jnp.broadcast_to(row, shape)


def prefix(count):
    lane, step = lax.broadcasted_iota(I32, count.shape, 1), 1
    while step < count.shape[1]:
        count = count + jnp.where(lane >= step, pltpu.roll(count, step, 1), 0)
        step *= 2
    return count


def slots_of(ids, experts, cap):
    shape = experts.shape
    hit = (spread(ids[0:1], shape) == experts) | (spread(ids[1:2], shape) == experts)
    hits = jnp.where(hit, 1, 0)
    rank = prefix(hits) - hits
    return jnp.where(hit & (rank < cap), rank, -1)


def gates_of(ids, gates, experts):
    shape = experts.shape
    return (jnp.where(spread(ids[0:1], shape) == experts, spread(gates[0:1], shape), 0.0)
            + jnp.where(spread(ids[1:2], shape) == experts, spread(gates[1:2], shape), 0.0))


def moe_kernel(cap, n_c, ids_hbm, gates_hbm, tokens, w_up, w_down,
               out, flag, tok, tokc, st_up, st_down, wuf, wdf, xs_hbm, h_hbm, part_hbm, rp, rh, rows_hbm,
               idsg, own_gates, meta, cur, pad, tab_h, tab_p,
               ids_s, ids_r, meta_s, meta_r, tok_s, tok_r, pk_s, pk_r, st_s, st_r, wo_s, wo_r, wm_s, wm_r, row_s, row_r, y_s, y_r, lsem):
    n_tok, hidden = tokens.shape
    ffn = w_up.shape[2]
    n_blk = n_c // BLK
    tp, ep = lax.axis_index('tp'), lax.axis_index('ep')
    core = lax.rem(ep, 2)

    def place(k):
        e = ep + (1 - 2 * core) if k & 1 else ep
        e = lax.rem(e + 2, 4) if k & 2 else e
        return (1 - tp if k & 4 else tp), e

    def rcopy(src, dst, send, recv, k):
        t, e = place(k)
        return pltpu.make_async_remote_copy(src_ref=src, dst_ref=dst, send_sem=send, recv_sem=recv,
                                            device_id={'tp': t, 'ep': e}, device_id_type=MESH)

    hops = {Y: (OWN, Y), X: (OWN, X), C: (OWN, C), XY: (Y, X), YC: (Y, C), XC: (X, C), XYC: (XY, C)}
    n_part = 4
    c_part = n_c // n_part

    def tok_copy(k):
        frm, to = hops[k]
        if k < N_SIDE:
            return rcopy(tokens if frm == OWN else tok.at[frm], tok.at[k], tok_s.at[k], tok_r.at[k], to)
        rows = pl.ds(0, n_c)
        return rcopy(tok.at[frm, rows], tok.at[k, rows], tok_s.at[k], tok_r.at[k], to)

    def pack_copy(i):
        rows = pl.ds(i * c_part, c_part)
        return rcopy(tokc.at[rows], tok.at[Y, rows], pk_s.at[i], pk_r.at[i], Y)

    def ids_copy(k):
        frm, to = hops[k]
        return rcopy(ids_hbm if frm == OWN else idsg.at[frm], idsg.at[k], ids_s.at[k], ids_r.at[k], to)

    def meta_copy(k):
        frm, to = hops[k]
        return rcopy(meta.at[frm], meta.at[k], meta_s.at[k], meta_r.at[k], to)

    u0 = 256
    um = u0 + (hidden - u0) // 2
    half = hidden // 2

    def piece(i, mate, w):
        if i < 2:
            rows = pl.ds(um, hidden - um) if mate else pl.ds(0, u0) if i == 0 else pl.ds(u0, um - u0)
            return w.at[rows]
        rows = pl.ds(ffn // 2 if mate else 0, ffn // 2)
        return w.at[rows, pl.ds((i - 2) * half, half)] if w.shape[-1] == hidden else w.at[i - 2, rows]

    def staged(i):
        return st_up.at[pl.ds(0, hidden - um)] if i == 1 else st_down.at[i - 2]

    def stage_copy(i):
        return rcopy(piece(i, True, (w_up if i < 2 else w_down).at[1 - tp]), staged(i), st_s.at[i], st_r.at[i], C)

    def own_copy(i):
        src, dst = (w_up, wuf) if i < 2 else (w_down, wdf)
        return rcopy(piece(i, False, src.at[1 - tp]), piece(i, False, dst), wo_s.at[i], wo_r.at[i], Y)

    def mate_copy(i):
        return rcopy(staged(i), piece(i, True, wuf if i < 2 else wdf), wm_s.at[i], wm_r.at[i], YC)

    pieces = (1, 2, 3)

    def wait_piece(i):
        own_copy(i).wait_recv()
        mate_copy(i).wait_recv()

    barrier = pltpu.get_barrier_semaphore()
    for k in range(1, N_SRC):
        t, e = place(k)
        pl.semaphore_signal(barrier, inc=1, device_id={'tp': t, 'ep': e}, device_id_type=MESH)
    pl.semaphore_wait(barrier, N_SRC - 1)

    own_copy(0).start()
    for k in (X, C):
        ids_copy(k).start()
        tok_copy(k).start()
    for i in pieces:
        stage_copy(i).start()

    def send_weights():
        for i in pieces:
            stage_copy(i).wait_recv()
        for group in ((1,), (2, 3)):
            @pl.when(core == 0)
            def _():
                for i in group:
                    own_copy(i).start()
                for i in group:
                    mate_copy(i).start()

            @pl.when(core == 1)
            def _():
                for i in group:
                    mate_copy(i).start()
                for i in group:
                    own_copy(i).start()

    def exp_rows(rels):
        row = lax.broadcasted_iota(I32, (8, n_tok), 0)
        experts = jnp.zeros((8, n_tok), I32)
        for i, k in enumerate(rels):
            t, e = place(k)
            experts = jnp.where(row == i, 2 * e + t, experts)
        return experts

    def turn(table):
        @pl.loop(0, n_tok // 128)
        def _(i):
            table[tile_of(i, 128), :] = jnp.transpose(pad[:, tile_of(i, 128)])

    def pack_phase(tokbuf, comp, cbuf, crow):
        get_i = pltpu.make_async_copy(ids_hbm, idsg.at[OWN], lsem.at[0])
        get_g = pltpu.make_async_copy(gates_hbm, own_gates, lsem.at[1])
        get_t = pltpu.make_async_copy(tokens, tokbuf, lsem.at[2])
        for get in (get_i, get_g, get_t):
            get.start()
        pad[...] = jnp.zeros_like(pad)
        get_i.wait()
        get_g.wait()
        experts = exp_rows(range(N_SRC))
        slots = slots_of(idsg[OWN], experts, cap)
        gates = gates_of(idsg[OWN], own_gates[...], experts)
        far = (slots >= 0) & (lax.broadcasted_iota(I32, slots.shape, 0) >= N_SIDE)
        count = jnp.sum(jnp.where(far, 1.0, 0.0), axis=0, keepdims=True)
        gate = jnp.sum(jnp.where(far, gates, 0.0), axis=0, keepdims=True)
        cross = spread(jnp.where(count > 0.5, 1, 0), (8, n_tok))
        seen = prefix(cross)
        crow[...] = jnp.where(cross > 0, seen - 1, -1)
        over = jnp.where(jnp.max(seen.astype(F32), axis=1, keepdims=True) > n_c, 1.0, 0.0)
        pad[0:8, :] = slots.astype(F32)
        pad[8:16, :] = gates
        pad[16:24, :] = spread(jnp.where(count > 1.5, 1.0, gate), (8, n_tok))
        pad[24:32, :] = crow[...].astype(F32)
        turn(tab_h)
        get_t.wait()

        def put_c(i):
            return pltpu.make_async_copy(cbuf.at[i], tokc.at[pl.ds(i * c_part, c_part)], lsem.at[3 + i])

        def send_part(i):
            put_c(i).wait()
            pack_copy(i).start()

        @pl.loop(0, n_part)
        def _(i):
            @pl.loop(0, c_part // 32)
            def _(j):
                want = lax.broadcasted_iota(I32, (32, n_tok), 0) + (i * c_part + j * 32)
                comp[tile_of(j, 32), :] = jnp.where(spread(crow[0:1, :], want.shape) == want, 1.0, 0.0).astype(BF16)

            @pl.loop(0, hidden // 512)
            def _(n):
                cols = tile_of(n, 512)
                cbuf[i, :, cols] = jnp.dot(comp[...], tokbuf[:, cols], preferred_element_type=F32).astype(BF16)

            for ii in range(n_part):
                @pl.when(i == ii)
                def _():
                    put_c(ii).start()
                    if ii:
                        send_part(ii - 1)

        @pl.loop(0, n_tok // 128)
        def _(j):
            mask = spread(crow[0:1, :], (128, n_tok)) == lax.broadcasted_iota(I32, (128, n_tok), 0) + j * 128
            lane = lax.broadcasted_iota(I32, (128, 128), 1)
            block = jnp.zeros((128, 128), F32)
            for q in range(4):
                row = idsg[OWN][q:q + 1].astype(F32) + 1.0 if q < 2 else own_gates[q - 2:q - 1, :]
                col = jnp.sum(jnp.where(mask, spread(row, mask.shape), 0.0), axis=1, keepdims=True)
                block = jnp.where(lane == q, spread(col, (128, 128)), block)
            block = jnp.transpose(block)[0:8]
            row = lax.broadcasted_iota(I32, (8, 128), 0)
            block = jnp.where(row < 2, block - 1.0, jnp.where(row == 4, spread(over, (8, 128)), block))
            meta[OWN, :, tile_of(j, 128)] = block

        send_part(n_part - 1)

    pl.run_scoped(pack_phase, pltpu.VMEM((n_tok, hidden), BF16), pltpu.VMEM((c_part, n_tok), BF16),
                  pltpu.VMEM((n_part, c_part, hidden), BF16), pltpu.VMEM((8, n_tok), I32))
    for k in (Y, X, C):
        meta_copy(k).start()

    def proxy_table():
        experts = exp_rows(range(N_SIDE))
        ids = meta[Y, 0:2, :].astype(I32)
        slots = slots_of(ids, experts, cap)
        near = (slots >= 0) & (lax.broadcasted_iota(I32, slots.shape, 0) < N_SIDE)
        gates = gates_of(ids, meta[Y, 2:4, :], experts)
        count = jnp.sum(jnp.where(near, 1.0, 0.0), axis=0, keepdims=True)
        pad[0:8, :] = slots.astype(F32)
        pad[8:16, :] = jnp.where(spread(count, gates.shape) > 1.5, gates, 1.0)
        turn(tab_p)

    my_exp = 2 * ep + tp

    def up_phase(tokbuf, pick, xs, wu, wd, h, part):
        load_d = pltpu.make_async_copy(w_down.at[tp], wd, lsem.at[2])
        load_d.start()

        def load(k):
            if k >= N_SIDE:
                rows = pl.ds(0, n_c)
                return pltpu.make_async_copy(tok.at[k, rows], tokbuf.at[rows], lsem.at[0])
            return pltpu.make_async_copy(tokens if k == OWN else tok.at[k], tokbuf, lsem.at[0])

        def put_x(k):
            return pltpu.make_async_copy(xs.at[0], xs_hbm.at[k], lsem.at[3])

        def put_part(k):
            return pltpu.make_async_copy(part, part_hbm.at[k], lsem.at[4])

        def arrive(k):
            if k == OWN:
                return
            if k < N_SIDE:
                ids_copy(k).wait_recv()
            else:
                meta_copy(k).wait_recv()
            if k == Y:
                for i in range(n_part):
                    pack_copy(i).wait_recv()
            else:
                tok_copy(k).wait_recv()
            for j, (frm, _) in hops.items():
                if frm == k:
                    (ids_copy if j < N_SIDE else meta_copy)(j).start()
                    tok_copy(j).start()

        def at_top(k):
            if k == X:
                send_weights()
                arrive(Y)
                arrive(X)
                meta_copy(X).wait_recv()
                meta_copy(XC).start()
                meta_copy(C).wait_recv()
                proxy_table()
            elif k in (OWN, XY, XYC):
                arrive(k)
            if k in (OWN, X, XY, XYC):
                load(k).start()

        def after_pick(k):
            if k in (C, XC, Y, YC):
                if k != Y:
                    arrive(k)
                load(k).start()

        def up_tiles(x_slot, h_slot):
            @pl.loop(0, ffn // 256)
            def _(n):
                cols = tile_of(n, 256)
                h[h_slot, :, cols] = gelu(jnp.dot(xs[x_slot], wu[:, cols], preferred_element_type=F32)).astype(BF16)

        def near(k, lo):
            for kk in range(N_SRC):
                @pl.when(k == kk)
                def _():
                    at_top(kk)
                    cur[0:2, :] = idsg[kk] if kk < N_SIDE else meta[kk, 0:2, :].astype(I32)
            slots = slots_of(cur[0:2, :], jnp.full((8, n_tok), my_exp, I32), cap)[0:1]

            @pl.loop(0, cap // 80)
            def _(i):
                want = lax.broadcasted_iota(I32, (80, n_tok), 0) + i * 80
                pick[tile_of(i, 80), :] = jnp.where(spread(slots, want.shape) == want, 1.0, 0.0).astype(BF16)

            for kk in (OWN, Y):
                @pl.when((k >= N_SIDE) if kk else (k < N_SIDE))
                def _():
                    load(kk).wait()

            @pl.when(k > lo)
            def _():
                put_x(k - 1).wait()

            @pl.loop(0, hidden // 512)
            def _(n):
                cols = tile_of(n, 512)
                xs[0, :, cols] = jnp.dot(pick[...], tokbuf[:, cols], preferred_element_type=F32).astype(BF16)

            put_x(k).start()
            for kk in range(N_SRC - 1):
                pl.when(k == kk)(functools.partial(after_pick, kk + 1))
            up_tiles(0, 0)

            @pl.when(k > lo)
            def _():
                put_part(k - 1).wait()

            @pl.loop(0, hidden // 512)
            def _(n):
                cols = tile_of(n, 512)
                part[:, cols] = jnp.dot(h[0], wd[:, cols], preferred_element_type=F32)

            put_part(k).start()

        def get_x(k, slot):
            return pltpu.make_async_copy(xs_hbm.at[k], xs.at[slot], lsem.at[3 + slot])

        def put_h(k, slot):
            return pltpu.make_async_copy(h.at[slot], h_hbm.at[k], lsem.at[5 + slot])

        @pl.loop(0, 2)
        def _(rnd):
            lo = rnd * (6 + 2 * core)
            hi = 8 - 2 * (1 - core) * (1 - rnd)

            @pl.when(lo < hi)
            def _():
                load_u = pltpu.make_async_copy(w_up.at[tp], wu, lsem.at[1])
                load_u.start()
                load_u.wait()

                @pl.when(rnd == 0)
                def _():
                    load_d.wait()

                @pl.loop(lo, hi)
                def _(k):
                    near(k, lo)

                put_x(hi - 1).wait()
                put_part(hi - 1).wait()

                @pl.when(rnd == 0)
                def _():
                    own_copy(0).wait_recv()
                    wait_piece(1)

                load_f = pltpu.make_async_copy(wuf, wu, lsem.at[1])
                load_f.start()
                get_x(lo, 0).start()
                load_f.wait()

                @pl.loop(lo, hi)
                def _(k):
                    slot = lax.rem(k, 2)
                    get_x(k, slot).wait()

                    @pl.when(k < hi - 1)
                    def _():
                        get_x(k + 1, 1 - slot).start()

                    @pl.when(k >= lo + 2)
                    def _():
                        put_h(k - 2, slot).wait()

                    up_tiles(slot, slot)
                    put_h(k, slot).start()

                put_h(hi - 2, 0).wait()
                put_h(hi - 1, 1).wait()

    pl.run_scoped(up_phase,
                  pltpu.VMEM((n_tok, hidden), BF16), pltpu.VMEM((cap, n_tok), BF16), pltpu.VMEM((2, cap, hidden), BF16),
                  pltpu.VMEM((hidden, ffn), BF16), pltpu.VMEM((ffn, hidden), BF16), pltpu.VMEM((2, cap, ffn), BF16),
                  pltpu.VMEM((cap, hidden), F32))

    order = (X, XC, OWN, C)

    def row_copy(block, k, c):
        dst = (rp if k >= N_SIDE else rh).at[c, k % N_SIDE]
        i = k * 2 + c
        if k == OWN:
            return pltpu.make_async_copy(block, dst, row_s.at[i])
        return rcopy(block, dst, row_s.at[i], row_r.at[i], k % N_SIDE)

    def y_copy(merged, c, b):
        rows = tile_of(b, BLK)
        i = c * n_blk + b
        return rcopy(merged.at[c, rows], rows_hbm.at[c, rows], y_s.at[i], y_r.at[i], Y)

    def end_phase(merged):
        def finish_and_merge(res, wd, hb, p_in, rpv, selfv, tot):
            def src(i):
                return jnp.where(i < N_SIDE, N_SIDE, 0) + lax.rem(i + 2, N_SIDE)

            def gets(i, c, slot):
                return (pltpu.make_async_copy(h_hbm.at[src(i)], hb.at[slot], lsem.at[slot]),
                        pltpu.make_async_copy(part_hbm.at[src(i), :, tile_of(c, half)], p_in.at[slot], lsem.at[2 + slot]))

            def finish(c):
                for get in gets(0, c, 0):
                    get.start()
                for cc in range(2):
                    pl.when(c == cc)(lambda: wait_piece(2 + cc))
                load_w = pltpu.make_async_copy(wdf.at[c], wd, lsem.at[4])
                load_w.start()
                load_w.wait()

                @pl.loop(0, N_SRC)
                def _(i):
                    slot = lax.rem(i, 2)
                    for get in gets(i, c, slot):
                        get.wait()

                    @pl.when(i < N_SRC - 1)
                    def _():
                        for get in gets(i + 1, c, 1 - slot):
                            get.start()

                    keys = [N_SIDE + k for k in order] + list(order)
                    for j, k in enumerate(keys):
                        if k % N_SIDE:
                            @pl.when((i == j) & (c > 0))
                            def _():
                                row_copy(res.at[j], k, 0).wait_send()

                    @pl.loop(0, half // 512)
                    def _(n):
                        cols = tile_of(n, 512)
                        value = p_in[slot, :, cols] + jnp.dot(hb[slot], wd[:, cols], preferred_element_type=F32)
                        res[i, :, cols] = value.astype(BF16)

                    for j, k in enumerate(keys):
                        @pl.when(i == j)
                        def _():
                            if k == Y:
                                selfv[c] = res[j]
                            elif k == OWN:
                                put = row_copy(res.at[j], k, c)
                                put.start()
                                put.wait()
                            else:
                                row_copy(res.at[j], k, c).start()

            def merge(c):
                fetch = [pltpu.make_async_copy(rp.at[c, e], rpv.at[e - 1], lsem.at[4 + e]) for e in range(1, N_SIDE)]
                for e in range(1, N_SIDE):
                    row_copy(res.at[0], N_SIDE + e, c).wait_recv()
                    fetch[e - 1].start()
                for get in fetch:
                    get.wait()

                @pl.loop(0, n_blk)
                def _(b):
                    rows = tile_of(b, BLK)
                    for e in range(N_SIDE):
                        want = lax.broadcasted_iota(I32, (BLK, cap), 1).astype(F32)
                        p = jnp.where(spread(tab_p[rows, e:e + 1], want.shape) == want, 1.0, 0.0).astype(BF16)
                        got = jnp.dot(p, rpv[e - 1] if e else selfv[c], preferred_element_type=F32)
                        got = spread(tab_p[rows, 8 + e:9 + e], got.shape) * got
                        tot[...] = tot[...] + got if e else got
                    merged[c, rows] = tot[...].astype(BF16)
                    y_copy(merged, c, b).start()

            @pl.loop(0, 4)
            def _(s):
                early = core == 0
                turn_f = jnp.where(early, s < 2, lax.rem(s, 2) == 0)
                pl.when(turn_f)(lambda: finish(jnp.where(early, s, s // 2)))
                pl.when(jnp.logical_not(turn_f))(lambda: merge(jnp.where(early, s - 2, s // 2)))

            for j, k in enumerate([N_SIDE + k for k in order] + list(order)):
                if k % N_SIDE:
                    row_copy(res.at[j], k, 1).wait_send()

        rows_t = pltpu.VMEM((2, cap, half), BF16)
        pl.run_scoped(finish_and_merge, pltpu.VMEM((N_SRC, cap, half), BF16), pltpu.VMEM((ffn, half), BF16),
                      pltpu.VMEM((2, cap, ffn), BF16), pltpu.VMEM((2, cap, half), F32),
                      pltpu.VMEM((N_SIDE - 1, cap, half), BF16), rows_t, pltpu.VMEM((BLK, half), F32))

        def home(acc, rbuf, ybuf, obuf):
            wide = 256
            n_wide = n_tok // wide
            n_pair = n_c // wide
            rest = n_c - n_pair * wide

            @pl.loop(0, 2)
            def _(c):
                fetch = [pltpu.make_async_copy(rh.at[c, e], rbuf.at[e], lsem.at[4 + e]) for e in range(N_SIDE)]
                for e in range(N_SIDE):
                    if e != OWN:
                        row_copy(rbuf.at[e], e, c).wait_recv()
                    fetch[e].start()
                for get in fetch:
                    get.wait()

                @pl.loop(0, n_wide)
                def _(i):
                    r = tile_of(i, wide)
                    for e in range(N_SIDE):
                        want = lax.broadcasted_iota(I32, (wide, cap), 1).astype(F32)
                        p = jnp.where(spread(tab_h[r, e:e + 1], want.shape) == want, 1.0, 0.0).astype(BF16)
                        got = jnp.dot(p, rbuf[e], preferred_element_type=F32)
                        got = spread(tab_h[r, 8 + e:9 + e], got.shape) * got
                        acc[r, :] = acc[r, :] + got if e else got

                def put(i, slot):
                    return pltpu.make_async_copy(obuf.at[slot], out.at[tile_of(i, wide), tile_of(c, half)], lsem.at[1 + slot])

                def emit(i, value):
                    slot = lax.rem(i, 2)

                    @pl.when(i >= 2)
                    def _():
                        put(i - 2, slot).wait()

                    obuf[slot] = value.astype(BF16)
                    put(i, slot).start()

                def returned(i, first, n):
                    r = tile_of(i, wide)
                    want = (lax.broadcasted_iota(I32, (wide, n), 1) + first).astype(F32)
                    p = jnp.where(spread(tab_h[r, 24:25], want.shape) == want, 1.0, 0.0).astype(BF16)
                    got = jnp.dot(p, ybuf[0:n, :], preferred_element_type=F32)
                    return acc[r, :] + spread(tab_h[r, 16:17], got.shape) * got

                def fetch_y(first, n):
                    get = pltpu.make_async_copy(rows_hbm.at[c, pl.ds(first, n)], ybuf.at[pl.ds(0, n)], lsem.at[0])
                    get.start()
                    get.wait()

                @pl.loop(0, n_pair)
                def _(i):
                    y_copy(merged, c, 2 * i).wait_recv()
                    y_copy(merged, c, 2 * i + 1).wait_recv()
                    fetch_y(pl.multiple_of(i * wide, wide), wide)
                    emit(i, returned(i, i * wide, wide))

                    @pl.loop(i + 1, n_wide)
                    def _(j):
                        acc[tile_of(j, wide), :] = returned(j, i * wide, wide)

                if rest:
                    y_copy(merged, c, n_blk - 1).wait_recv()
                    fetch_y(n_pair * wide, rest)
                if n_pair < n_wide:
                    @pl.loop(n_pair, n_wide)
                    def _(i):
                        emit(i, returned(i, n_pair * wide, rest) if rest else acc[tile_of(i, wide), :])

                for i in (n_wide - 2, n_wide - 1):
                    put(i, i % 2).wait()

        pl.run_scoped(home, pltpu.VMEM((n_tok, half), F32), pltpu.VMEM((N_SIDE, cap, half), BF16),
                      pltpu.VMEM((256, half), BF16), pltpu.VMEM((2, 256, half), BF16))

        for c in range(2):
            @pl.loop(0, n_blk)
            def _(b):
                y_copy(merged, c, b).wait_send()

    pl.run_scoped(end_phase, pltpu.VMEM((2, n_c, half), BF16))

    meta_copy(XC).wait_recv()
    top = meta[OWN, :, 0:128]
    for k in range(1, N_SRC):
        top = jnp.maximum(top, meta[k, :, 0:128])
    flag[...] = top
    for k in range(1, N_SRC):
        if k < N_SIDE:
            ids_copy(k).wait_send()
        meta_copy(k).wait_send()
        if k != Y:
            tok_copy(k).wait_send()
    for i in range(n_part):
        pack_copy(i).wait_send()
    own_copy(0).wait_send()
    for i in pieces:
        stage_copy(i).wait_send()
        own_copy(i).wait_send()
        mate_copy(i).wait_send()


def solution(mesh):
    row_spec = P(('dp', 'ep', 'tp'), None)
    n_exp = 2 * mesh.shape['ep']

    def local_moe(tokens, expert_ids, gate_vals, w_up, w_down):
        n_tok, hidden = tokens.shape
        ffn = w_up.shape[2]
        cap = capacity(n_tok, expert_ids.shape[1], n_exp)
        n_piece, half = 4, hidden // 2
        any_spec = pl.BlockSpec(memory_space=pl.ANY)
        dma = pltpu.SemaphoreType.DMA

        def run(n_c, collective_id):
            shapes = [((n_tok, hidden), BF16), ((8, 128), F32), ((N_SRC, n_tok, hidden), BF16), ((n_c, hidden), BF16),
                      ((half, ffn), BF16), ((2, ffn // 2, half), BF16), ((hidden, ffn), BF16), ((2, ffn, half), BF16),
                      ((N_SRC, cap, hidden), BF16), ((N_SRC, cap, ffn), BF16), ((N_SRC, cap, hidden), F32),
                      ((2, N_SIDE, cap, half), BF16), ((2, N_SIDE, cap, half), BF16), ((2, n_c, half), BF16)]
            outs = pl.pallas_call(
                functools.partial(moe_kernel, cap, n_c),
                out_shape=[jax.ShapeDtypeStruct(s, d) for s, d in shapes],
                in_specs=[any_spec] * 5,
                out_specs=[any_spec, pl.BlockSpec(memory_space=pltpu.VMEM)] + [any_spec] * (len(shapes) - 2),
                scratch_shapes=[
                    pltpu.VMEM((N_SIDE, 2, n_tok), I32), pltpu.VMEM((2, n_tok), F32), pltpu.VMEM((N_SRC, 8, n_tok), F32),
                    pltpu.VMEM((8, n_tok), I32), pltpu.VMEM((128, n_tok), F32),
                    pltpu.VMEM((n_tok, 128), F32), pltpu.VMEM((n_tok, 128), F32),
                    dma((N_SIDE,)), dma((N_SIDE,)), dma((N_SRC,)), dma((N_SRC,)), dma((N_SRC,)), dma((N_SRC,)), dma((4,)), dma((4,)),
                    dma((n_piece,)), dma((n_piece,)), dma((n_piece,)), dma((n_piece,)), dma((n_piece,)), dma((n_piece,)),
                    dma((N_SRC * 2,)), dma((N_SRC * 2,)), dma((2 * (n_c // BLK),)), dma((2 * (n_c // BLK),)),
                    dma((8,)),
                ],
                compiler_params=pltpu.CompilerParams(collective_id=collective_id, has_side_effects=True,
                                                     vmem_limit_bytes=66_000_000),
                name=f'moe_{n_c}',
            )(expert_ids.T, gate_vals.T, tokens, w_up, w_down)
            return outs[0], outs[1]

        fast, flag = run(n_tok * 13 // 16, 0)
        return lax.cond(flag[4, 0] > 0.5, lambda: run(n_tok, 1)[0], lambda: fast)

    return jax.shard_map(local_moe, mesh=mesh,
                         in_specs=(row_spec, row_spec, row_spec, P('ep', None, 'tp'), P('ep', 'tp', None)),
                         out_specs=row_spec, check_vma=False)
```

```python
import functools
import math

import jax
import jax.numpy as jnp
from jax import lax
from jax.experimental import pallas as pl
from jax.experimental.pallas import tpu as pltpu
from jax.sharding import PartitionSpec as P

MESH = pl.DeviceIdType.MESH
F32, BF16, I32 = jnp.float32, jnp.bfloat16, jnp.int32
OWN, C, X, XC, Y, YC, XY, XYC = range(8)
N_SRC, N_SIDE = 8, 4
BLK = 128


def capacity(tok_count, n_top, n_exp):
    return ((5 * tok_count * n_top) // (4 * n_exp) + 7) // 8 * 8


def gelu(x):
    c = math.sqrt(2.0 / math.pi)
    return x * (0.5 * (1.0 + jnp.tanh(c * (x + 0.044715 * (x * x * x)))))


def tile_of(i, size):
    return pl.ds(pl.multiple_of(i * size, size), size)


def spread(row, shape):
    return jnp.broadcast_to(row, shape)


def prefix(count):
    lane, step = lax.broadcasted_iota(I32, count.shape, 1), 1
    while step < count.shape[1]:
        count = count + jnp.where(lane >= step, pltpu.roll(count, step, 1), 0)
        step *= 2
    return count


def slots_of(ids, experts, cap):
    shape = experts.shape
    hit = (spread(ids[0:1], shape) == experts) | (spread(ids[1:2], shape) == experts)
    hits = jnp.where(hit, 1, 0)
    rank = prefix(hits) - hits
    return jnp.where(hit & (rank < cap), rank, -1)


def gates_of(ids, gates, experts):
    shape = experts.shape
    return (jnp.where(spread(ids[0:1], shape) == experts, spread(gates[0:1], shape), 0.0)
            + jnp.where(spread(ids[1:2], shape) == experts, spread(gates[1:2], shape), 0.0))


def last_block(n_c, wide):
    size = n_c % wide or wide
    return size, (n_c - size) // wide


def last_kernel(first_t, n_c, x_hbm, acc_ref, tab_ref, rows_hbm, o_hbm, buf, rows, sem_i, sem_o, sem_r):
    n_tile, wide, hidden = buf.shape
    n, half = rows.shape

    def get(i):
        return pltpu.make_async_copy(x_hbm.at[pl.ds(i * wide, wide)], buf.at[i], sem_i.at[i])

    def put(i):
        return pltpu.make_async_copy(buf.at[i], o_hbm.at[pl.ds(i * wide, wide)], sem_o.at[i])

    get_r = pltpu.make_async_copy(rows_hbm.at[1, pl.ds(n_c - n, n)], rows, sem_r)
    get_r.start()
    tiles = list(range(first_t, n_tile)) + list(range(first_t))
    for i in tiles:
        get(i).start()
    get_r.wait()
    for i in tiles:
        get(i).wait()
        if i >= first_t:
            r = pl.ds((i - first_t) * wide, wide)
            want = (lax.broadcasted_iota(I32, (wide, n), 1) + (n_c - n)).astype(F32)
            p = jnp.where(spread(tab_ref[r, 24:25], want.shape) == want, 1.0, 0.0).astype(BF16)
            got = jnp.dot(p, rows[...], preferred_element_type=F32)
            buf[i, :, half:] = (acc_ref[r, :] + spread(tab_ref[r, 16:17], got.shape) * got).astype(BF16)
        put(i).start()
    for i in tiles:
        put(i).wait()


def moe_kernel(cap, n_c, ids_hbm, gates_hbm, tokens, w_up, w_down,
               out, acc_t, tab_t, flag, tok, tokc, st_up, st_down, wuf, wdf, xs_hbm, h_hbm, part_hbm, rp, rh, rows_hbm,
               idsg, own_gates, meta, cur, pad, tab_h, tab_p,
               ids_s, ids_r, meta_s, meta_r, tok_s, tok_r, pk_s, pk_r, st_s, st_r, wo_s, wo_r, wm_s, wm_r, row_s, row_r, y_s, y_r, lsem):
    n_tok, hidden = tokens.shape
    ffn = w_up.shape[2]
    n_blk = n_c // BLK
    tp, ep = lax.axis_index('tp'), lax.axis_index('ep')
    core = lax.rem(ep, 2)

    def place(k):
        e = ep + (1 - 2 * core) if k & 1 else ep
        e = lax.rem(e + 2, 4) if k & 2 else e
        return (1 - tp if k & 4 else tp), e

    def rcopy(src, dst, send, recv, k):
        t, e = place(k)
        return pltpu.make_async_remote_copy(src_ref=src, dst_ref=dst, send_sem=send, recv_sem=recv,
                                            device_id={'tp': t, 'ep': e}, device_id_type=MESH)

    hops = {Y: (OWN, Y), X: (OWN, X), C: (OWN, C), XY: (Y, X), YC: (Y, C), XC: (X, C), XYC: (XY, C)}
    n_part = 4
    c_part = n_c // n_part

    def tok_copy(k):
        frm, to = hops[k]
        if k < N_SIDE:
            return rcopy(tokens if frm == OWN else tok.at[frm], tok.at[k], tok_s.at[k], tok_r.at[k], to)
        rows = pl.ds(0, n_c)
        return rcopy(tok.at[frm, rows], tok.at[k, rows], tok_s.at[k], tok_r.at[k], to)

    def pack_copy(i):
        rows = pl.ds(i * c_part, c_part)
        return rcopy(tokc.at[rows], tok.at[Y, rows], pk_s.at[i], pk_r.at[i], Y)

    def ids_copy(k):
        frm, to = hops[k]
        return rcopy(ids_hbm if frm == OWN else idsg.at[frm], idsg.at[k], ids_s.at[k], ids_r.at[k], to)

    def meta_copy(k):
        frm, to = hops[k]
        return rcopy(meta.at[frm], meta.at[k], meta_s.at[k], meta_r.at[k], to)

    u0 = 256
    um = u0 + (hidden - u0) // 2
    half = hidden // 2

    def piece(i, mate, w):
        if i < 2:
            rows = pl.ds(um, hidden - um) if mate else pl.ds(0, u0) if i == 0 else pl.ds(u0, um - u0)
            return w.at[rows]
        rows = pl.ds(ffn // 2 if mate else 0, ffn // 2)
        return w.at[rows, pl.ds((i - 2) * half, half)] if w.shape[-1] == hidden else w.at[i - 2, rows]

    def staged(i):
        return st_up.at[pl.ds(0, hidden - um)] if i == 1 else st_down.at[i - 2]

    def stage_copy(i):
        return rcopy(piece(i, True, (w_up if i < 2 else w_down).at[1 - tp]), staged(i), st_s.at[i], st_r.at[i], C)

    def own_copy(i):
        src, dst = (w_up, wuf) if i < 2 else (w_down, wdf)
        return rcopy(piece(i, False, src.at[1 - tp]), piece(i, False, dst), wo_s.at[i], wo_r.at[i], Y)

    def mate_copy(i):
        return rcopy(staged(i), piece(i, True, wuf if i < 2 else wdf), wm_s.at[i], wm_r.at[i], YC)

    pieces = (1, 2, 3)

    def wait_piece(i):
        own_copy(i).wait_recv()
        mate_copy(i).wait_recv()

    barrier = pltpu.get_barrier_semaphore()
    for k in range(1, N_SRC):
        t, e = place(k)
        pl.semaphore_signal(barrier, inc=1, device_id={'tp': t, 'ep': e}, device_id_type=MESH)
    pl.semaphore_wait(barrier, N_SRC - 1)

    own_copy(0).start()
    for k in (X, C):
        ids_copy(k).start()
        tok_copy(k).start()
    for i in pieces:
        stage_copy(i).start()

    def send_weights():
        for i in pieces:
            stage_copy(i).wait_recv()
        for group in ((1,), (2, 3)):
            @pl.when(core == 0)
            def _():
                for i in group:
                    own_copy(i).start()
                for i in group:
                    mate_copy(i).start()

            @pl.when(core == 1)
            def _():
                for i in group:
                    mate_copy(i).start()
                for i in group:
                    own_copy(i).start()

    def exp_rows(rels):
        row = lax.broadcasted_iota(I32, (8, n_tok), 0)
        experts = jnp.zeros((8, n_tok), I32)
        for i, k in enumerate(rels):
            t, e = place(k)
            experts = jnp.where(row == i, 2 * e + t, experts)
        return experts

    def turn(table):
        @pl.loop(0, n_tok // 128)
        def _(i):
            table[tile_of(i, 128), :] = jnp.transpose(pad[:, tile_of(i, 128)])

    def pack_phase(tokbuf, comp, cbuf, crow):
        get_i = pltpu.make_async_copy(ids_hbm, idsg.at[OWN], lsem.at[0])
        get_g = pltpu.make_async_copy(gates_hbm, own_gates, lsem.at[1])
        get_t = pltpu.make_async_copy(tokens, tokbuf, lsem.at[2])
        for get in (get_i, get_g, get_t):
            get.start()
        pad[...] = jnp.zeros_like(pad)
        get_i.wait()
        get_g.wait()
        experts = exp_rows(range(N_SRC))
        slots = slots_of(idsg[OWN], experts, cap)
        gates = gates_of(idsg[OWN], own_gates[...], experts)
        far = (slots >= 0) & (lax.broadcasted_iota(I32, slots.shape, 0) >= N_SIDE)
        count = jnp.sum(jnp.where(far, 1.0, 0.0), axis=0, keepdims=True)
        gate = jnp.sum(jnp.where(far, gates, 0.0), axis=0, keepdims=True)
        cross = spread(jnp.where(count > 0.5, 1, 0), (8, n_tok))
        seen = prefix(cross)
        crow[...] = jnp.where(cross > 0, seen - 1, -1)
        over = jnp.where(jnp.max(seen.astype(F32), axis=1, keepdims=True) > n_c, 1.0, 0.0)
        pad[0:8, :] = slots.astype(F32)
        pad[8:16, :] = gates
        pad[16:24, :] = spread(jnp.where(count > 1.5, 1.0, gate), (8, n_tok))
        pad[24:32, :] = crow[...].astype(F32)
        turn(tab_h)
        get_t.wait()

        def put_c(i):
            return pltpu.make_async_copy(cbuf.at[i], tokc.at[pl.ds(i * c_part, c_part)], lsem.at[3 + i])

        def send_part(i):
            put_c(i).wait()
            pack_copy(i).start()

        @pl.loop(0, n_part)
        def _(i):
            @pl.loop(0, c_part // 32)
            def _(j):
                want = lax.broadcasted_iota(I32, (32, n_tok), 0) + (i * c_part + j * 32)
                comp[tile_of(j, 32), :] = jnp.where(spread(crow[0:1, :], want.shape) == want, 1.0, 0.0).astype(BF16)

            @pl.loop(0, hidden // 512)
            def _(n):
                cols = tile_of(n, 512)
                cbuf[i, :, cols] = jnp.dot(comp[...], tokbuf[:, cols], preferred_element_type=F32).astype(BF16)

            for ii in range(n_part):
                @pl.when(i == ii)
                def _():
                    put_c(ii).start()
                    if ii:
                        send_part(ii - 1)

        @pl.loop(0, n_tok // 128)
        def _(j):
            mask = spread(crow[0:1, :], (128, n_tok)) == lax.broadcasted_iota(I32, (128, n_tok), 0) + j * 128
            lane = lax.broadcasted_iota(I32, (128, 128), 1)
            block = jnp.zeros((128, 128), F32)
            for q in range(4):
                row = idsg[OWN][q:q + 1].astype(F32) + 1.0 if q < 2 else own_gates[q - 2:q - 1, :]
                col = jnp.sum(jnp.where(mask, spread(row, mask.shape), 0.0), axis=1, keepdims=True)
                block = jnp.where(lane == q, spread(col, (128, 128)), block)
            block = jnp.transpose(block)[0:8]
            row = lax.broadcasted_iota(I32, (8, 128), 0)
            block = jnp.where(row < 2, block - 1.0, jnp.where(row == 4, spread(over, (8, 128)), block))
            meta[OWN, :, tile_of(j, 128)] = block

        send_part(n_part - 1)

    pl.run_scoped(pack_phase, pltpu.VMEM((n_tok, hidden), BF16), pltpu.VMEM((c_part, n_tok), BF16),
                  pltpu.VMEM((n_part, c_part, hidden), BF16), pltpu.VMEM((8, n_tok), I32))
    for k in (Y, X, C):
        meta_copy(k).start()

    def proxy_table():
        experts = exp_rows(range(N_SIDE))
        ids = meta[Y, 0:2, :].astype(I32)
        slots = slots_of(ids, experts, cap)
        near = (slots >= 0) & (lax.broadcasted_iota(I32, slots.shape, 0) < N_SIDE)
        gates = gates_of(ids, meta[Y, 2:4, :], experts)
        count = jnp.sum(jnp.where(near, 1.0, 0.0), axis=0, keepdims=True)
        pad[0:8, :] = slots.astype(F32)
        pad[8:16, :] = jnp.where(spread(count, gates.shape) > 1.5, gates, 1.0)
        turn(tab_p)

    my_exp = 2 * ep + tp

    def up_phase(tokbuf, xs, wu, wd, h, part):
        pick = h.at[1, :, pl.ds(0, n_tok)]
        load_d = pltpu.make_async_copy(w_down.at[tp], wd, lsem.at[2])
        load_d.start()

        def load(k):
            if k >= N_SIDE:
                rows = pl.ds(0, n_c)
                return pltpu.make_async_copy(tok.at[k, rows], tokbuf.at[rows], lsem.at[0])
            return pltpu.make_async_copy(tokens if k == OWN else tok.at[k], tokbuf, lsem.at[0])

        def put_x(k):
            return pltpu.make_async_copy(xs.at[0], xs_hbm.at[k], lsem.at[3])

        def put_part(k):
            return pltpu.make_async_copy(part, part_hbm.at[k], lsem.at[4])

        def arrive(k):
            if k == OWN:
                return
            if k < N_SIDE:
                ids_copy(k).wait_recv()
            else:
                meta_copy(k).wait_recv()
            if k == Y:
                for i in range(n_part):
                    pack_copy(i).wait_recv()
            else:
                tok_copy(k).wait_recv()
            for j, (frm, _) in hops.items():
                if frm == k:
                    (ids_copy if j < N_SIDE else meta_copy)(j).start()
                    tok_copy(j).start()

        def at_top(k):
            if k == X:
                send_weights()
                arrive(Y)
                arrive(X)
                meta_copy(X).wait_recv()
                meta_copy(XC).start()
                meta_copy(C).wait_recv()
                proxy_table()
            elif k in (OWN, XY, XYC):
                arrive(k)
            if k in (OWN, X, XY, XYC):
                load(k).start()

        def after_pick(k):
            if k in (C, XC, Y, YC):
                if k != Y:
                    arrive(k)
                load(k).start()

        def up_tiles(x_slot, h_slot):
            @pl.loop(0, ffn // 256)
            def _(n):
                cols = tile_of(n, 256)
                h[h_slot, :, cols] = gelu(jnp.dot(xs[x_slot], wu[:, cols], preferred_element_type=F32)).astype(BF16)

        def near(k, lo):
            for kk in range(N_SRC):
                @pl.when(k == kk)
                def _():
                    at_top(kk)
                    cur[0:2, :] = idsg[kk] if kk < N_SIDE else meta[kk, 0:2, :].astype(I32)
            slots = slots_of(cur[0:2, :], jnp.full((8, n_tok), my_exp, I32), cap)[0:1]

            @pl.loop(0, cap // 80)
            def _(i):
                want = lax.broadcasted_iota(I32, (80, n_tok), 0) + i * 80
                pick[tile_of(i, 80), :] = jnp.where(spread(slots, want.shape) == want, 1.0, 0.0).astype(BF16)

            for kk in (OWN, Y):
                @pl.when((k >= N_SIDE) if kk else (k < N_SIDE))
                def _():
                    load(kk).wait()

            @pl.when(k > lo)
            def _():
                put_x(k - 1).wait()

            @pl.loop(0, hidden // 512)
            def _(n):
                cols = tile_of(n, 512)
                xs[0, :, cols] = jnp.dot(pick[...], tokbuf[:, cols], preferred_element_type=F32).astype(BF16)

            put_x(k).start()
            for kk in range(N_SRC - 1):
                pl.when(k == kk)(functools.partial(after_pick, kk + 1))
            up_tiles(0, 0)

            @pl.when(k > lo)
            def _():
                put_part(k - 1).wait()

            @pl.loop(0, hidden // 512)
            def _(n):
                cols = tile_of(n, 512)
                part[:, cols] = jnp.dot(h[0], wd[:, cols], preferred_element_type=F32)

            put_part(k).start()

        def get_x(k, slot):
            return pltpu.make_async_copy(xs_hbm.at[k], xs.at[slot], lsem.at[3 + slot])

        def put_h(k, slot):
            return pltpu.make_async_copy(h.at[slot], h_hbm.at[k], lsem.at[5 + slot])

        @pl.loop(0, 2)
        def _(rnd):
            lo = rnd * (6 + 2 * core)
            hi = 8 - 2 * (1 - core) * (1 - rnd)

            @pl.when(lo < hi)
            def _():
                load_u = pltpu.make_async_copy(w_up.at[tp], wu, lsem.at[1])
                load_u.start()
                load_u.wait()

                @pl.when(rnd == 0)
                def _():
                    load_d.wait()

                @pl.loop(lo, hi)
                def _(k):
                    near(k, lo)

                put_x(hi - 1).wait()
                put_part(hi - 1).wait()

                @pl.when(rnd == 0)
                def _():
                    own_copy(0).wait_recv()
                    wait_piece(1)

                load_f = pltpu.make_async_copy(wuf, wu, lsem.at[1])
                load_f.start()
                get_x(lo, 0).start()
                load_f.wait()

                @pl.loop(lo, hi)
                def _(k):
                    slot = lax.rem(k, 2)
                    get_x(k, slot).wait()

                    @pl.when(k < hi - 1)
                    def _():
                        get_x(k + 1, 1 - slot).start()

                    @pl.when(k >= lo + 2)
                    def _():
                        put_h(k - 2, slot).wait()

                    up_tiles(slot, slot)
                    put_h(k, slot).start()

                put_h(hi - 2, 0).wait()
                put_h(hi - 1, 1).wait()

    pl.run_scoped(up_phase,
                  pltpu.VMEM((n_tok, hidden), BF16), pltpu.VMEM((2, cap, hidden), BF16),
                  pltpu.VMEM((hidden, ffn), BF16), pltpu.VMEM((ffn, hidden), BF16), pltpu.VMEM((2, cap, ffn), BF16),
                  pltpu.VMEM((cap, hidden), F32))

    meta_copy(XC).wait_recv()
    over = meta[OWN, 4:5, 0:128]
    for k in range(1, N_SRC):
        over = jnp.maximum(over, meta[k, 4:5, 0:128])
    flag[0, 0] = jnp.max(over).astype(I32)

    order = (X, XC, OWN, C)

    def row_copy(block, k, c):
        dst = (rp if k >= N_SIDE else rh).at[c, k % N_SIDE]
        i = k * 2 + c
        if k == OWN:
            return pltpu.make_async_copy(block, dst, row_s.at[i])
        return rcopy(block, dst, row_s.at[i], row_r.at[i], k % N_SIDE)

    def y_copy(merged, c, b):
        rows = tile_of(b, BLK)
        i = c * n_blk + b
        return rcopy(merged.at[c, rows], rows_hbm.at[c, rows], y_s.at[i], y_r.at[i], Y)

    def end_phase(merged):
        def finish_and_merge(res, wd, hb, p_in, rpv, selfv, tot):
            def src(i):
                return jnp.where(i < N_SIDE, N_SIDE, 0) + lax.rem(i + 2, N_SIDE)

            def gets(i, c, slot):
                return (pltpu.make_async_copy(h_hbm.at[src(i)], hb.at[slot], lsem.at[slot]),
                        pltpu.make_async_copy(part_hbm.at[src(i), :, tile_of(c, half)], p_in.at[slot], lsem.at[2 + slot]))

            def finish(c):
                for get in gets(0, c, 0):
                    get.start()
                for cc in range(2):
                    pl.when(c == cc)(lambda: wait_piece(2 + cc))
                load_w = pltpu.make_async_copy(wdf.at[c], wd, lsem.at[4])
                load_w.start()
                load_w.wait()

                @pl.loop(0, N_SRC)
                def _(i):
                    slot = lax.rem(i, 2)
                    for get in gets(i, c, slot):
                        get.wait()

                    @pl.when(i < N_SRC - 1)
                    def _():
                        for get in gets(i + 1, c, 1 - slot):
                            get.start()

                    keys = [N_SIDE + k for k in order] + list(order)
                    for j, k in enumerate(keys):
                        if k % N_SIDE:
                            @pl.when((i == j) & (c > 0))
                            def _():
                                row_copy(res.at[j], k, 0).wait_send()

                    @pl.loop(0, half // 512)
                    def _(n):
                        cols = tile_of(n, 512)
                        value = p_in[slot, :, cols] + jnp.dot(hb[slot], wd[:, cols], preferred_element_type=F32)
                        res[i, :, cols] = value.astype(BF16)

                    for j, k in enumerate(keys):
                        @pl.when(i == j)
                        def _():
                            if k == Y:
                                selfv[c] = res[j]
                            elif k == OWN:
                                put = row_copy(res.at[j], k, c)
                                put.start()
                                put.wait()
                            else:
                                row_copy(res.at[j], k, c).start()

            def merge(c):
                fetch = [pltpu.make_async_copy(rp.at[c, e], rpv.at[e - 1], lsem.at[4 + e]) for e in range(1, N_SIDE)]
                for e in range(1, N_SIDE):
                    row_copy(res.at[0], N_SIDE + e, c).wait_recv()
                    fetch[e - 1].start()
                for get in fetch:
                    get.wait()

                @pl.loop(0, n_blk)
                def _(b):
                    rows = tile_of(b, BLK)
                    for e in range(N_SIDE):
                        want = lax.broadcasted_iota(I32, (BLK, cap), 1).astype(F32)
                        p = jnp.where(spread(tab_p[rows, e:e + 1], want.shape) == want, 1.0, 0.0).astype(BF16)
                        got = jnp.dot(p, rpv[e - 1] if e else selfv[c], preferred_element_type=F32)
                        got = spread(tab_p[rows, 8 + e:9 + e], got.shape) * got
                        tot[...] = tot[...] + got if e else got
                    merged[c, rows] = tot[...].astype(BF16)
                    y_copy(merged, c, b).start()

            @pl.loop(0, 4)
            def _(s):
                early = core == 0
                turn_f = jnp.where(early, s < 2, lax.rem(s, 2) == 0)
                pl.when(turn_f)(lambda: finish(jnp.where(early, s, s // 2)))
                pl.when(jnp.logical_not(turn_f))(lambda: merge(jnp.where(early, s - 2, s // 2)))

            for j, k in enumerate([N_SIDE + k for k in order] + list(order)):
                if k % N_SIDE:
                    row_copy(res.at[j], k, 1).wait_send()

        rows_t = pltpu.VMEM((2, cap, half), BF16)
        pl.run_scoped(finish_and_merge, pltpu.VMEM((N_SRC, cap, half), BF16), pltpu.VMEM((ffn, half), BF16),
                      pltpu.VMEM((2, cap, ffn), BF16), pltpu.VMEM((2, cap, half), F32),
                      pltpu.VMEM((N_SIDE - 1, cap, half), BF16), rows_t, pltpu.VMEM((BLK, half), F32))

        def home(acc, rbuf, ybuf, obuf):
            wide = 256
            n_wide = n_tok // wide
            n_last, first_t = last_block(n_c, wide)

            @pl.loop(0, 2)
            def _(c):
                fetch = [pltpu.make_async_copy(rh.at[c, e], rbuf.at[e], lsem.at[4 + e]) for e in range(N_SIDE)]
                for e in range(N_SIDE):
                    if e != OWN:
                        row_copy(rbuf.at[e], e, c).wait_recv()
                    fetch[e].start()
                for get in fetch:
                    get.wait()

                @pl.loop(0, n_wide)
                def _(i):
                    r = tile_of(i, wide)
                    for e in range(N_SIDE):
                        want = lax.broadcasted_iota(I32, (wide, cap), 1).astype(F32)
                        p = jnp.where(spread(tab_h[r, e:e + 1], want.shape) == want, 1.0, 0.0).astype(BF16)
                        got = jnp.dot(p, rbuf[e], preferred_element_type=F32)
                        got = spread(tab_h[r, 8 + e:9 + e], got.shape) * got
                        acc[r, :] = acc[r, :] + got if e else got

                def put(i, slot):
                    return pltpu.make_async_copy(obuf.at[slot], out.at[tile_of(i, wide), tile_of(c, half)], lsem.at[1 + slot])

                def emit(i, value):
                    slot = lax.rem(i, 2)

                    @pl.when(i >= 2)
                    def _():
                        put(i - 2, slot).wait()

                    obuf[slot] = value.astype(BF16)
                    put(i, slot).start()

                def returned(i, first, n):
                    r = tile_of(i, wide)
                    want = (lax.broadcasted_iota(I32, (wide, n), 1) + first).astype(F32)
                    p = jnp.where(spread(tab_h[r, 24:25], want.shape) == want, 1.0, 0.0).astype(BF16)
                    got = jnp.dot(p, ybuf[0:n, :], preferred_element_type=F32)
                    return acc[r, :] + spread(tab_h[r, 16:17], got.shape) * got

                def fetch_y(first, n):
                    get = pltpu.make_async_copy(rows_hbm.at[c, pl.ds(first, n)], ybuf.at[pl.ds(0, n)], lsem.at[0])
                    get.start()
                    get.wait()

                @pl.loop(0, (n_c - n_last) // wide)
                def _(i):
                    y_copy(merged, c, 2 * i).wait_recv()
                    y_copy(merged, c, 2 * i + 1).wait_recv()
                    fetch_y(pl.multiple_of(i * wide, wide), wide)
                    emit(i, returned(i, i * wide, wide))

                    @pl.loop(i + 1, n_wide)
                    def _(j):
                        acc[tile_of(j, wide), :] = returned(j, i * wide, wide)

                tail = pl.ds(first_t * wide, (n_wide - first_t) * wide)
                put_a = pltpu.make_async_copy(acc.at[tail], acc_t, lsem.at[3])
                put_t = pltpu.make_async_copy(tab_h.at[tail], tab_t, lsem.at[4])

                @pl.when(c == 1)
                def _():
                    put_a.start()
                    put_t.start()

                for b in range((n_c - n_last) // BLK, n_blk):
                    y_copy(merged, c, b).wait_recv()

                @pl.when(c == 0)
                def _():
                    fetch_y(n_c - n_last, n_last)

                    @pl.loop(first_t, n_wide)
                    def _(i):
                        emit(i, returned(i, n_c - n_last, n_last))

                    for i in (n_wide - 2, n_wide - 1):
                        put(i, i % 2).wait()

                @pl.when(c == 1)
                def _():
                    for i in (first_t - 2, first_t - 1):
                        put(i, i % 2).wait()
                    put_a.wait()
                    put_t.wait()

        pl.run_scoped(home, pltpu.VMEM((n_tok, half), F32), pltpu.VMEM((N_SIDE, cap, half), BF16),
                      pltpu.VMEM((256, half), BF16), pltpu.VMEM((2, 256, half), BF16))

        for c in range(2):
            @pl.loop(0, n_blk)
            def _(b):
                y_copy(merged, c, b).wait_send()

    pl.run_scoped(end_phase, pltpu.VMEM((2, n_c, half), BF16))

    for k in range(1, N_SRC):
        if k < N_SIDE:
            ids_copy(k).wait_send()
        meta_copy(k).wait_send()
        if k != Y:
            tok_copy(k).wait_send()
    for i in range(n_part):
        pack_copy(i).wait_send()
    own_copy(0).wait_send()
    for i in pieces:
        stage_copy(i).wait_send()
        own_copy(i).wait_send()
        mate_copy(i).wait_send()


def solution(mesh):
    row_spec = P(('dp', 'ep', 'tp'), None)
    n_exp = 2 * mesh.shape['ep']

    def local_moe(tokens, expert_ids, gate_vals, w_up, w_down):
        n_tok, hidden = tokens.shape
        ffn = w_up.shape[2]
        cap = capacity(n_tok, expert_ids.shape[1], n_exp)
        n_piece, half = 4, hidden // 2
        any_spec = pl.BlockSpec(memory_space=pl.ANY)
        dma = pltpu.SemaphoreType.DMA

        def run(n_c, collective_id):
            wide = 256
            n_last, first_t = last_block(n_c, wide)
            n_tail = n_tok - first_t * wide
            shapes = [((n_tok, hidden), BF16), ((n_tail, half), F32), ((n_tail, 128), F32), ((1, 1), I32), ((N_SRC, n_tok, hidden), BF16), ((n_c, hidden), BF16),
                      ((half, ffn), BF16), ((2, ffn // 2, half), BF16), ((hidden, ffn), BF16), ((2, ffn, half), BF16),
                      ((N_SRC, cap, hidden), BF16), ((N_SRC, cap, ffn), BF16), ((N_SRC, cap, hidden), F32),
                      ((2, N_SIDE, cap, half), BF16), ((2, N_SIDE, cap, half), BF16), ((2, n_c, half), BF16)]
            outs = pl.pallas_call(
                functools.partial(moe_kernel, cap, n_c),
                out_shape=[jax.ShapeDtypeStruct(s, d) for s, d in shapes],
                in_specs=[any_spec] * 5,
                out_specs=[any_spec] * 3 + [pl.BlockSpec(memory_space=pltpu.SMEM)] + [any_spec] * (len(shapes) - 4),
                scratch_shapes=[
                    pltpu.VMEM((N_SIDE, 2, n_tok), I32), pltpu.VMEM((2, n_tok), F32), pltpu.VMEM((N_SRC, 8, n_tok), F32),
                    pltpu.VMEM((8, n_tok), I32), pltpu.VMEM((128, n_tok), F32),
                    pltpu.VMEM((n_tok, 128), F32), pltpu.VMEM((n_tok, 128), F32),
                    dma((N_SIDE,)), dma((N_SIDE,)), dma((N_SRC,)), dma((N_SRC,)), dma((N_SRC,)), dma((N_SRC,)), dma((4,)), dma((4,)),
                    dma((n_piece,)), dma((n_piece,)), dma((n_piece,)), dma((n_piece,)), dma((n_piece,)), dma((n_piece,)),
                    dma((N_SRC * 2,)), dma((N_SRC * 2,)), dma((2 * (n_c // BLK),)), dma((2 * (n_c // BLK),)),
                    dma((8,)),
                ],
                compiler_params=pltpu.CompilerParams(collective_id=collective_id, has_side_effects=True,
                                                     vmem_limit_bytes=56 * 1024 * 1024),
                name=f'moe_{n_c}',
            )(expert_ids.T, gate_vals.T, tokens, w_up, w_down)

            def last():
                vmem = pl.BlockSpec(memory_space=pltpu.VMEM)
                return pl.pallas_call(
                    functools.partial(last_kernel, first_t, n_c),
                    out_shape=jax.ShapeDtypeStruct((n_tok, hidden), BF16),
                    in_specs=[any_spec, vmem, vmem, any_spec],
                    out_specs=any_spec,
                    scratch_shapes=[pltpu.VMEM((n_tok // wide, wide, hidden), BF16), pltpu.VMEM((n_last, half), BF16),
                                    dma((n_tok // wide,)), dma((n_tok // wide,)), dma(())],
                    compiler_params=pltpu.CompilerParams(vmem_limit_bytes=24 * 1024 * 1024),
                    name=f'last_{n_c}',
                )(outs[0], outs[1], outs[2], outs[-1])

            return last, outs[3]

        last, flag = run(n_tok * 13 // 16, 0)
        return lax.cond(flag[0, 0] > 0, lambda: run(n_tok, 1)[0](), last)

    return jax.shard_map(local_moe, mesh=mesh,
                         in_specs=(row_spec, row_spec, row_spec, P('ep', None, 'tp'), P('ep', 'tp', None)),
                         out_specs=row_spec, check_vma=False)
```

```python
import functools
import math

import jax
import jax.numpy as jnp
from jax import lax
from jax.experimental import pallas as pl
from jax.experimental.pallas import tpu as pltpu
from jax.sharding import PartitionSpec as P

MESH = pl.DeviceIdType.MESH
F32, BF16, I32 = jnp.float32, jnp.bfloat16, jnp.int32
OWN, C, X, XC, Y, YC, XY, XYC = range(8)
N_SRC, N_SIDE = 8, 4
BLK = 128


def capacity(tok_count, n_top, n_exp):
    return ((5 * tok_count * n_top) // (4 * n_exp) + 7) // 8 * 8


def gelu(x):
    c = math.sqrt(2.0 / math.pi)
    return x * (0.5 * (1.0 + jnp.tanh(c * (x + 0.044715 * (x * x * x)))))


def tile_of(i, size):
    return pl.ds(pl.multiple_of(i * size, size), size)


def spread(row, shape):
    return jnp.broadcast_to(row, shape)


def prefix(count):
    lane, step = lax.broadcasted_iota(I32, count.shape, 1), 1
    while step < count.shape[1]:
        count = count + jnp.where(lane >= step, pltpu.roll(count, step, 1), 0)
        step *= 2
    return count


def slots_of(ids, experts, cap):
    shape = experts.shape
    hit = (spread(ids[0:1], shape) == experts) | (spread(ids[1:2], shape) == experts)
    hits = jnp.where(hit, 1, 0)
    rank = prefix(hits) - hits
    return jnp.where(hit & (rank < cap), rank, -1)


def gates_of(ids, gates, experts):
    shape = experts.shape
    return (jnp.where(spread(ids[0:1], shape) == experts, spread(gates[0:1], shape), 0.0)
            + jnp.where(spread(ids[1:2], shape) == experts, spread(gates[1:2], shape), 0.0))


def pack_parts(n_c):
    return 3 if n_c % 96 == 0 else 4


def last_block(n_c, wide):
    size = n_c % wide or wide
    return size, (n_c - size) // wide


def last_kernel(first_t, n_c, a_ref, b_ref, acc_ref, tab_ref, rows_hbm, o_hbm, buf, rows, sem, sem_r):
    n_t, wide, half = buf.shape
    n = rows.shape[0]
    get_r = pltpu.make_async_copy(rows_hbm.at[1, pl.ds(n_c - n, n)], rows, sem_r)
    get_r.start()
    lo = pl.ds(0, first_t * wide)
    puts = [pltpu.make_async_copy(a_ref, o_hbm.at[:, pl.ds(0, half)], sem.at[0]),
            pltpu.make_async_copy(b_ref.at[lo], o_hbm.at[lo, pl.ds(half, half)], sem.at[1])]
    for put in puts:
        put.start()
    get_r.wait()
    for i in range(n_t):
        r = pl.ds(i * wide, wide)
        want = (lax.broadcasted_iota(I32, (wide, n), 1) + (n_c - n)).astype(F32)
        p = jnp.where(spread(tab_ref[r, 24:25], want.shape) == want, 1.0, 0.0).astype(BF16)
        got = jnp.dot(p, rows[...], preferred_element_type=F32)
        buf[i] = (acc_ref[r, :] + spread(tab_ref[r, 16:17], got.shape) * got).astype(BF16)
        puts.append(pltpu.make_async_copy(buf.at[i], o_hbm.at[pl.ds((first_t + i) * wide, wide), pl.ds(half, half)], sem.at[2 + i]))
        puts[-1].start()
    for put in puts:
        put.wait()


def moe_kernel(cap, n_c, ids_hbm, gates_hbm, tokens, w_up, w_down,
               out_a, out_b, acc_t, tab_t, flag, tok, tokc, st_up, st_down, wuf, wdf, xs_hbm, h_hbm, part_hbm, rp, rh, rows_hbm,
               idsg, own_gates, meta, cur, pad, tab_h, tab_p,
               ids_s, ids_r, meta_s, meta_r, tok_s, tok_r, pk_s, pk_r, st_s, st_r, wo_s, wo_r, wm_s, wm_r, row_s, row_r, y_s, y_r, lsem):
    n_tok, hidden = tokens.shape
    ffn = w_up.shape[2]
    n_blk = -(-n_c // BLK)
    tp, ep = lax.axis_index('tp'), lax.axis_index('ep')
    core = lax.rem(ep, 2)

    def place(k):
        e = ep + (1 - 2 * core) if k & 1 else ep
        e = lax.rem(e + 2, 4) if k & 2 else e
        return (1 - tp if k & 4 else tp), e

    def rcopy(src, dst, send, recv, k):
        t, e = place(k)
        return pltpu.make_async_remote_copy(src_ref=src, dst_ref=dst, send_sem=send, recv_sem=recv,
                                            device_id={'tp': t, 'ep': e}, device_id_type=MESH)

    hops = {Y: (OWN, Y), X: (OWN, X), C: (OWN, C), XY: (Y, X), YC: (Y, C), XC: (X, C), XYC: (XY, C)}
    n_part = pack_parts(n_c)
    c_part = n_c // n_part

    def tok_copy(k):
        frm, to = hops[k]
        if k < N_SIDE:
            return rcopy(tokens if frm == OWN else tok.at[frm], tok.at[k], tok_s.at[k], tok_r.at[k], to)
        rows = pl.ds(0, n_c)
        return rcopy(tok.at[frm, rows], tok.at[k, rows], tok_s.at[k], tok_r.at[k], to)

    def pack_copy(i):
        rows = pl.ds(i * c_part, c_part)
        return rcopy(tokc.at[rows], tok.at[Y, rows], pk_s.at[i], pk_r.at[i], Y)

    def ids_copy(k):
        frm, to = hops[k]
        return rcopy(ids_hbm if frm == OWN else idsg.at[frm], idsg.at[k], ids_s.at[k], ids_r.at[k], to)

    def meta_copy(k):
        frm, to = hops[k]
        return rcopy(meta.at[frm], meta.at[k], meta_s.at[k], meta_r.at[k], to)

    u0 = 256
    um = u0 + (hidden - u0) // 2
    half = hidden // 2

    def piece(i, mate, w):
        if i < 2:
            rows = pl.ds(um, hidden - um) if mate else pl.ds(0, u0) if i == 0 else pl.ds(u0, um - u0)
            return w.at[rows]
        rows = pl.ds(ffn // 2 if mate else 0, ffn // 2)
        return w.at[rows, pl.ds((i - 2) * half, half)] if w.shape[-1] == hidden else w.at[i - 2, rows]

    def staged(i):
        return st_up.at[pl.ds(0, hidden - um)] if i == 1 else st_down.at[i - 2]

    def stage_copy(i):
        return rcopy(piece(i, True, (w_up if i < 2 else w_down).at[1 - tp]), staged(i), st_s.at[i], st_r.at[i], C)

    def own_copy(i):
        src, dst = (w_up, wuf) if i < 2 else (w_down, wdf)
        return rcopy(piece(i, False, src.at[1 - tp]), piece(i, False, dst), wo_s.at[i], wo_r.at[i], Y)

    def mate_copy(i):
        return rcopy(staged(i), piece(i, True, wuf if i < 2 else wdf), wm_s.at[i], wm_r.at[i], YC)

    pieces = (1, 2, 3)

    def wait_piece(i):
        own_copy(i).wait_recv()
        mate_copy(i).wait_recv()

    barrier = pltpu.get_barrier_semaphore()
    for k in range(1, N_SRC):
        t, e = place(k)
        pl.semaphore_signal(barrier, inc=1, device_id={'tp': t, 'ep': e}, device_id_type=MESH)
    pl.semaphore_wait(barrier, N_SRC - 1)

    own_copy(0).start()
    for k in (X, C):
        ids_copy(k).start()
        tok_copy(k).start()
    for i in pieces:
        stage_copy(i).start()

    def send_weights():
        for i in pieces:
            stage_copy(i).wait_recv()
        for group in ((1,), (2, 3)):
            @pl.when(core == 0)
            def _():
                for i in group:
                    own_copy(i).start()
                for i in group:
                    mate_copy(i).start()

            @pl.when(core == 1)
            def _():
                for i in group:
                    mate_copy(i).start()
                for i in group:
                    own_copy(i).start()

    def exp_rows(rels):
        row = lax.broadcasted_iota(I32, (8, n_tok), 0)
        experts = jnp.zeros((8, n_tok), I32)
        for i, k in enumerate(rels):
            t, e = place(k)
            experts = jnp.where(row == i, 2 * e + t, experts)
        return experts

    def turn(table):
        @pl.loop(0, n_tok // 128)
        def _(i):
            table[tile_of(i, 128), :] = jnp.transpose(pad[:, tile_of(i, 128)])

    def pack_phase(tokbuf, comp, cbuf, crow):
        get_i = pltpu.make_async_copy(ids_hbm, idsg.at[OWN], lsem.at[0])
        get_g = pltpu.make_async_copy(gates_hbm, own_gates, lsem.at[1])
        get_t = pltpu.make_async_copy(tokens, tokbuf, lsem.at[2])
        for get in (get_i, get_g, get_t):
            get.start()
        pad[...] = jnp.zeros_like(pad)
        get_i.wait()
        get_g.wait()
        experts = exp_rows(range(N_SRC))
        slots = slots_of(idsg[OWN], experts, cap)
        gates = gates_of(idsg[OWN], own_gates[...], experts)
        far = (slots >= 0) & (lax.broadcasted_iota(I32, slots.shape, 0) >= N_SIDE)
        count = jnp.sum(jnp.where(far, 1.0, 0.0), axis=0, keepdims=True)
        gate = jnp.sum(jnp.where(far, gates, 0.0), axis=0, keepdims=True)
        cross = spread(jnp.where(count > 0.5, 1, 0), (8, n_tok))
        seen = prefix(cross)
        crow[...] = jnp.where(cross > 0, seen - 1, -1)
        over = jnp.where(jnp.max(seen.astype(F32), axis=1, keepdims=True) > n_c, 1.0, 0.0)
        pad[0:8, :] = slots.astype(F32)
        pad[8:16, :] = gates
        pad[16:24, :] = spread(jnp.where(count > 1.5, 1.0, gate), (8, n_tok))
        pad[24:32, :] = crow[...].astype(F32)
        turn(tab_h)
        get_t.wait()

        def put_c(i):
            return pltpu.make_async_copy(cbuf.at[i], tokc.at[pl.ds(i * c_part, c_part)], lsem.at[3 + i])

        def send_part(i):
            put_c(i).wait()
            pack_copy(i).start()

        @pl.loop(0, n_part)
        def _(i):
            @pl.loop(0, c_part // 32)
            def _(j):
                want = lax.broadcasted_iota(I32, (32, n_tok), 0) + (i * c_part + j * 32)
                comp[tile_of(j, 32), :] = jnp.where(spread(crow[0:1, :], want.shape) == want, 1.0, 0.0).astype(BF16)

            @pl.loop(0, hidden // 512)
            def _(n):
                cols = tile_of(n, 512)
                cbuf[i, :, cols] = jnp.dot(comp[...], tokbuf[:, cols], preferred_element_type=F32).astype(BF16)

            for ii in range(n_part):
                @pl.when(i == ii)
                def _():
                    put_c(ii).start()
                    if ii:
                        send_part(ii - 1)

        @pl.loop(0, n_tok // 128)
        def _(j):
            mask = spread(crow[0:1, :], (128, n_tok)) == lax.broadcasted_iota(I32, (128, n_tok), 0) + j * 128
            lane = lax.broadcasted_iota(I32, (128, 128), 1)
            block = jnp.zeros((128, 128), F32)
            for q in range(4):
                row = idsg[OWN][q:q + 1].astype(F32) + 1.0 if q < 2 else own_gates[q - 2:q - 1, :]
                col = jnp.sum(jnp.where(mask, spread(row, mask.shape), 0.0), axis=1, keepdims=True)
                block = jnp.where(lane == q, spread(col, (128, 128)), block)
            block = jnp.transpose(block)[0:8]
            row = lax.broadcasted_iota(I32, (8, 128), 0)
            block = jnp.where(row < 2, block - 1.0, jnp.where(row == 4, spread(over, (8, 128)), block))
            meta[OWN, :, tile_of(j, 128)] = block

        send_part(n_part - 1)

    pl.run_scoped(pack_phase, pltpu.VMEM((n_tok, hidden), BF16), pltpu.VMEM((c_part, n_tok), BF16),
                  pltpu.VMEM((n_part, c_part, hidden), BF16), pltpu.VMEM((8, n_tok), I32))
    for k in (Y, X, C):
        meta_copy(k).start()

    def proxy_table():
        experts = exp_rows(range(N_SIDE))
        ids = meta[Y, 0:2, :].astype(I32)
        slots = slots_of(ids, experts, cap)
        near = (slots >= 0) & (lax.broadcasted_iota(I32, slots.shape, 0) < N_SIDE)
        gates = gates_of(ids, meta[Y, 2:4, :], experts)
        count = jnp.sum(jnp.where(near, 1.0, 0.0), axis=0, keepdims=True)
        pad[0:8, :] = slots.astype(F32)
        pad[8:16, :] = jnp.where(spread(count, gates.shape) > 1.5, gates, 1.0)
        turn(tab_p)

    my_exp = 2 * ep + tp

    def up_phase(tokbuf, xs, wu, wd, h, part):
        pick = h.at[1, :, pl.ds(0, n_tok)]
        load_d = pltpu.make_async_copy(w_down.at[tp], wd, lsem.at[2])
        load_d.start()

        def load(k):
            if k >= N_SIDE:
                rows = pl.ds(0, n_c)
                return pltpu.make_async_copy(tok.at[k, rows], tokbuf.at[rows], lsem.at[0])
            return pltpu.make_async_copy(tokens if k == OWN else tok.at[k], tokbuf, lsem.at[0])

        def put_x(k):
            return pltpu.make_async_copy(xs.at[0], xs_hbm.at[k], lsem.at[3])

        def put_part(k):
            return pltpu.make_async_copy(part, part_hbm.at[k], lsem.at[4])

        def arrive(k):
            if k == OWN:
                return
            if k < N_SIDE:
                ids_copy(k).wait_recv()
            else:
                meta_copy(k).wait_recv()
            if k == Y:
                for i in range(n_part):
                    pack_copy(i).wait_recv()
            else:
                tok_copy(k).wait_recv()
            for j, (frm, _) in hops.items():
                if frm == k:
                    (ids_copy if j < N_SIDE else meta_copy)(j).start()
                    tok_copy(j).start()

        def at_top(k):
            if k == X:
                send_weights()
                arrive(Y)
                arrive(X)
                meta_copy(X).wait_recv()
                meta_copy(XC).start()
                meta_copy(C).wait_recv()
                proxy_table()
            elif k in (OWN, XY, XYC):
                arrive(k)
            if k in (OWN, X, XY, XYC):
                load(k).start()

        def after_pick(k):
            if k in (C, XC, Y, YC):
                if k != Y:
                    arrive(k)
                load(k).start()

        def up_tiles(x_slot, h_slot):
            @pl.loop(0, ffn // 256)
            def _(n):
                cols = tile_of(n, 256)
                h[h_slot, :, cols] = gelu(jnp.dot(xs[x_slot], wu[:, cols], preferred_element_type=F32)).astype(BF16)

        def near(k, lo):
            for kk in range(N_SRC):
                @pl.when(k == kk)
                def _():
                    at_top(kk)
                    cur[0:2, :] = idsg[kk] if kk < N_SIDE else meta[kk, 0:2, :].astype(I32)
            slots = slots_of(cur[0:2, :], jnp.full((8, n_tok), my_exp, I32), cap)[0:1]

            @pl.loop(0, cap // 80)
            def _(i):
                want = lax.broadcasted_iota(I32, (80, n_tok), 0) + i * 80
                pick[tile_of(i, 80), :] = jnp.where(spread(slots, want.shape) == want, 1.0, 0.0).astype(BF16)

            for kk in (OWN, Y):
                @pl.when((k >= N_SIDE) if kk else (k < N_SIDE))
                def _():
                    load(kk).wait()

            @pl.when(k > lo)
            def _():
                put_x(k - 1).wait()

            @pl.loop(0, hidden // 512)
            def _(n):
                cols = tile_of(n, 512)
                xs[0, :, cols] = jnp.dot(pick[...], tokbuf[:, cols], preferred_element_type=F32).astype(BF16)

            put_x(k).start()
            for kk in range(N_SRC - 1):
                pl.when(k == kk)(functools.partial(after_pick, kk + 1))
            up_tiles(0, 0)

            @pl.when(k > lo)
            def _():
                put_part(k - 1).wait()

            @pl.loop(0, hidden // 512)
            def _(n):
                cols = tile_of(n, 512)
                part[:, cols] = jnp.dot(h[0], wd[:, cols], preferred_element_type=F32)

            put_part(k).start()

        def get_x(k, slot):
            return pltpu.make_async_copy(xs_hbm.at[k], xs.at[slot], lsem.at[3 + slot])

        def put_h(k, slot):
            return pltpu.make_async_copy(h.at[slot], h_hbm.at[k], lsem.at[5 + slot])

        @pl.loop(0, 2)
        def _(rnd):
            lo = rnd * (6 + 2 * core)
            hi = 8 - 2 * (1 - core) * (1 - rnd)

            @pl.when(lo < hi)
            def _():
                load_u = pltpu.make_async_copy(w_up.at[tp], wu, lsem.at[1])
                load_u.start()
                load_u.wait()

                @pl.when(rnd == 0)
                def _():
                    load_d.wait()

                @pl.loop(lo, hi)
                def _(k):
                    near(k, lo)

                put_x(hi - 1).wait()
                put_part(hi - 1).wait()

                @pl.when(rnd == 0)
                def _():
                    own_copy(0).wait_recv()
                    wait_piece(1)

                load_f = pltpu.make_async_copy(wuf, wu, lsem.at[1])
                load_f.start()
                get_x(lo, 0).start()
                load_f.wait()

                @pl.loop(lo, hi)
                def _(k):
                    slot = lax.rem(k, 2)
                    get_x(k, slot).wait()

                    @pl.when(k < hi - 1)
                    def _():
                        get_x(k + 1, 1 - slot).start()

                    @pl.when(k >= lo + 2)
                    def _():
                        put_h(k - 2, slot).wait()

                    up_tiles(slot, slot)
                    put_h(k, slot).start()

                put_h(hi - 2, 0).wait()
                put_h(hi - 1, 1).wait()

    pl.run_scoped(up_phase,
                  pltpu.VMEM((n_tok, hidden), BF16), pltpu.VMEM((2, cap, hidden), BF16),
                  pltpu.VMEM((hidden, ffn), BF16), pltpu.VMEM((ffn, hidden), BF16), pltpu.VMEM((2, cap, ffn), BF16),
                  pltpu.VMEM((cap, hidden), F32))

    meta_copy(XC).wait_recv()
    over = meta[OWN, 4:5, 0:128]
    for k in range(1, N_SRC):
        over = jnp.maximum(over, meta[k, 4:5, 0:128])
    flag[0, 0] = jnp.max(over).astype(I32)

    order = (X, XC, OWN, C)

    def row_copy(block, k, c):
        dst = (rp if k >= N_SIDE else rh).at[c, k % N_SIDE]
        i = k * 2 + c
        if k == OWN:
            return pltpu.make_async_copy(block, dst, row_s.at[i])
        return rcopy(block, dst, row_s.at[i], row_r.at[i], k % N_SIDE)

    def y_copy(merged, c, b, n=BLK):
        rows = pl.ds(b * BLK if isinstance(b, int) else pl.multiple_of(b * BLK, BLK), n)
        i = c * n_blk + b
        return rcopy(merged.at[c, rows], rows_hbm.at[c, rows], y_s.at[i], y_r.at[i], Y)

    end = n_c - (n_blk - 1) * BLK

    def end_phase(merged):
        def finish_and_merge(res, wd, hb, p_in, rpv, selfv, tot):
            def src(i):
                return jnp.where(i < N_SIDE, N_SIDE, 0) + lax.rem(i + 2, N_SIDE)

            def gets(i, c, slot):
                return (pltpu.make_async_copy(h_hbm.at[src(i)], hb.at[slot], lsem.at[slot]),
                        pltpu.make_async_copy(part_hbm.at[src(i), :, tile_of(c, half)], p_in.at[slot], lsem.at[2 + slot]))

            def finish(c):
                for get in gets(0, c, 0):
                    get.start()
                for cc in range(2):
                    pl.when(c == cc)(lambda: wait_piece(2 + cc))
                load_w = pltpu.make_async_copy(wdf.at[c], wd, lsem.at[4])
                load_w.start()
                load_w.wait()

                @pl.loop(0, N_SRC)
                def _(i):
                    slot = lax.rem(i, 2)
                    for get in gets(i, c, slot):
                        get.wait()

                    @pl.when(i < N_SRC - 1)
                    def _():
                        for get in gets(i + 1, c, 1 - slot):
                            get.start()

                    keys = [N_SIDE + k for k in order] + list(order)
                    for j, k in enumerate(keys):
                        if k % N_SIDE:
                            @pl.when((i == j) & (c > 0))
                            def _():
                                row_copy(res.at[j], k, 0).wait_send()

                    @pl.loop(0, half // 512)
                    def _(n):
                        cols = tile_of(n, 512)
                        value = p_in[slot, :, cols] + jnp.dot(hb[slot], wd[:, cols], preferred_element_type=F32)
                        res[i, :, cols] = value.astype(BF16)

                    for j, k in enumerate(keys):
                        @pl.when(i == j)
                        def _():
                            if k == Y:
                                selfv[c] = res[j]
                            elif k == OWN:
                                put = row_copy(res.at[j], k, c)
                                put.start()
                                put.wait()
                            else:
                                row_copy(res.at[j], k, c).start()

            def merge(c):
                fetch = [pltpu.make_async_copy(rp.at[c, e], rpv.at[e - 1], lsem.at[4 + e]) for e in range(1, N_SIDE)]
                for e in range(1, N_SIDE):
                    row_copy(res.at[0], N_SIDE + e, c).wait_recv()
                    fetch[e - 1].start()
                for get in fetch:
                    get.wait()

                @pl.loop(0, n_blk)
                def _(b):
                    rows = tile_of(b, BLK)
                    for e in range(N_SIDE):
                        want = lax.broadcasted_iota(I32, (BLK, cap), 1).astype(F32)
                        p = jnp.where(spread(tab_p[rows, e:e + 1], want.shape) == want, 1.0, 0.0).astype(BF16)
                        got = jnp.dot(p, rpv[e - 1] if e else selfv[c], preferred_element_type=F32)
                        got = spread(tab_p[rows, 8 + e:9 + e], got.shape) * got
                        tot[...] = tot[...] + got if e else got
                    merged[c, rows] = tot[...].astype(BF16)
                    pl.when(b < n_blk - 1)(lambda: y_copy(merged, c, b).start())
                    pl.when(b == n_blk - 1)(lambda: y_copy(merged, c, n_blk - 1, end).start())

            @pl.loop(0, 4)
            def _(s):
                early = core == 0
                turn_f = jnp.where(early, s < 2, lax.rem(s, 2) == 0)
                pl.when(turn_f)(lambda: finish(jnp.where(early, s, s // 2)))
                pl.when(jnp.logical_not(turn_f))(lambda: merge(jnp.where(early, s - 2, s // 2)))

            for j, k in enumerate([N_SIDE + k for k in order] + list(order)):
                if k % N_SIDE:
                    row_copy(res.at[j], k, 1).wait_send()

        rows_t = pltpu.VMEM((2, cap, half), BF16)
        pl.run_scoped(finish_and_merge, pltpu.VMEM((N_SRC, cap, half), BF16), pltpu.VMEM((ffn, half), BF16),
                      pltpu.VMEM((2, cap, ffn), BF16), pltpu.VMEM((2, cap, half), F32),
                      pltpu.VMEM((N_SIDE - 1, cap, half), BF16), rows_t, pltpu.VMEM((BLK, half), F32))

        def home(acc, rbuf, ybuf):
            wide = 256
            n_wide = n_tok // wide
            n_last, first_t = last_block(n_c, wide)

            @pl.loop(0, 2)
            def _(c):
                fetch = [pltpu.make_async_copy(rh.at[c, e], rbuf.at[e], lsem.at[4 + e]) for e in range(N_SIDE)]
                for e in range(N_SIDE):
                    if e != OWN:
                        row_copy(rbuf.at[e], e, c).wait_recv()
                    fetch[e].start()
                for get in fetch:
                    get.wait()

                @pl.loop(0, n_wide)
                def _(i):
                    r = tile_of(i, wide)
                    for e in range(N_SIDE):
                        want = lax.broadcasted_iota(I32, (wide, cap), 1).astype(F32)
                        p = jnp.where(spread(tab_h[r, e:e + 1], want.shape) == want, 1.0, 0.0).astype(BF16)
                        got = jnp.dot(p, rbuf[e], preferred_element_type=F32)
                        got = spread(tab_h[r, 8 + e:9 + e], got.shape) * got
                        acc[r, :] = acc[r, :] + got if e else got

                def emit(i, value):
                    for cc, out in enumerate((out_a, out_b)):
                        @pl.when(c == cc)
                        def _():
                            out[tile_of(i, wide), :] = value().astype(BF16)

                def returned(i, first, n):
                    r = tile_of(i, wide)
                    want = (lax.broadcasted_iota(I32, (wide, n), 1) + first).astype(F32)
                    p = jnp.where(spread(tab_h[r, 24:25], want.shape) == want, 1.0, 0.0).astype(BF16)
                    got = jnp.dot(p, ybuf[0:n, :], preferred_element_type=F32)
                    return acc[r, :] + spread(tab_h[r, 16:17], got.shape) * got

                def fetch_y(first, n):
                    get = pltpu.make_async_copy(rows_hbm.at[c, pl.ds(first, n)], ybuf.at[pl.ds(0, n)], lsem.at[0])
                    get.start()
                    get.wait()

                @pl.loop(0, (n_c - n_last) // wide)
                def _(i):
                    y_copy(merged, c, 2 * i).wait_recv()
                    y_copy(merged, c, 2 * i + 1).wait_recv()
                    fetch_y(pl.multiple_of(i * wide, wide), wide)
                    emit(i, lambda: returned(i, i * wide, wide))

                    @pl.loop(i + 1, n_wide)
                    def _(j):
                        acc[tile_of(j, wide), :] = returned(j, i * wide, wide)

                tail = pl.ds(first_t * wide, (n_wide - first_t) * wide)

                @pl.when(c == 1)
                def _():
                    acc_t[...] = acc[tail, :]
                    tab_t[...] = tab_h[tail, :]

                for b in range((n_c - n_last) // BLK, n_blk):
                    y_copy(merged, c, b, end if b == n_blk - 1 else BLK).wait_recv()

                @pl.when(c == 0)
                def _():
                    fetch_y(n_c - n_last, n_last)

                    @pl.loop(first_t, n_wide)
                    def _(i):
                        emit(i, lambda: returned(i, n_c - n_last, n_last))

        pl.run_scoped(home, pltpu.VMEM((n_tok, half), F32), pltpu.VMEM((N_SIDE, cap, half), BF16),
                      pltpu.VMEM((256, half), BF16))

        for c in range(2):
            @pl.loop(0, n_blk - 1)
            def _(b):
                y_copy(merged, c, b).wait_send()

            y_copy(merged, c, n_blk - 1, end).wait_send()

    pl.run_scoped(end_phase, pltpu.VMEM((2, n_blk * BLK, half), BF16))

    for k in range(1, N_SRC):
        if k < N_SIDE:
            ids_copy(k).wait_send()
        meta_copy(k).wait_send()
        if k != Y:
            tok_copy(k).wait_send()
    for i in range(n_part):
        pack_copy(i).wait_send()
    own_copy(0).wait_send()
    for i in pieces:
        stage_copy(i).wait_send()
        own_copy(i).wait_send()
        mate_copy(i).wait_send()


def solution(mesh):
    row_spec = P(('dp', 'ep', 'tp'), None)
    n_exp = 2 * mesh.shape['ep']

    def local_moe(tokens, expert_ids, gate_vals, w_up, w_down):
        n_tok, hidden = tokens.shape
        ffn = w_up.shape[2]
        cap = capacity(n_tok, expert_ids.shape[1], n_exp)
        n_piece, half = 4, hidden // 2
        any_spec = pl.BlockSpec(memory_space=pl.ANY)
        dma = pltpu.SemaphoreType.DMA

        def run(n_c, collective_id):
            vmem = pl.BlockSpec(memory_space=pltpu.VMEM)
            wide = 256
            n_last, first_t = last_block(n_c, wide)
            n_tail = n_tok - first_t * wide
            shapes = [((1, 1), I32), ((N_SRC, n_tok, hidden), BF16), ((n_c, hidden), BF16),
                      ((half, ffn), BF16), ((2, ffn // 2, half), BF16), ((hidden, ffn), BF16), ((2, ffn, half), BF16),
                      ((N_SRC, cap, hidden), BF16), ((N_SRC, cap, ffn), BF16), ((N_SRC, cap, hidden), F32),
                      ((2, N_SIDE, cap, half), BF16), ((2, N_SIDE, cap, half), BF16), ((2, n_c, half), BF16)]
            outs = pl.pallas_call(
                functools.partial(moe_kernel, cap, n_c),
                out_shape=[pltpu.VMEM((n_tok, half), BF16)] * 2 + [pltpu.VMEM((n_tail, n), F32) for n in (half, 128)] + [jax.ShapeDtypeStruct(s, d) for s, d in shapes],
                in_specs=[any_spec] * 5,
                out_specs=[vmem] * 4 + [pl.BlockSpec(memory_space=pltpu.SMEM)] + [any_spec] * (len(shapes) - 1),
                scratch_shapes=[
                    pltpu.VMEM((N_SIDE, 2, n_tok), I32), pltpu.VMEM((2, n_tok), F32), pltpu.VMEM((N_SRC, 8, n_tok), F32),
                    pltpu.VMEM((8, n_tok), I32), pltpu.VMEM((128, n_tok), F32),
                    pltpu.VMEM((n_tok, 128), F32), pltpu.VMEM((n_tok, 128), F32),
                    dma((N_SIDE,)), dma((N_SIDE,)), dma((N_SRC,)), dma((N_SRC,)), dma((N_SRC,)), dma((N_SRC,)), dma((4,)), dma((4,)),
                    dma((n_piece,)), dma((n_piece,)), dma((n_piece,)), dma((n_piece,)), dma((n_piece,)), dma((n_piece,)),
                    dma((N_SRC * 2,)), dma((N_SRC * 2,)), dma((2 * -(-n_c // BLK),)), dma((2 * -(-n_c // BLK),)),
                    dma((8,)),
                ],
                compiler_params=pltpu.CompilerParams(collective_id=collective_id, has_side_effects=True,
                                                     vmem_limit_bytes=53 * 1024 * 1024),
                name=f'moe_{n_c}',
            )(expert_ids.T, gate_vals.T, tokens, w_up, w_down)

            def last():
                return pl.pallas_call(
                    functools.partial(last_kernel, first_t, n_c),
                    out_shape=jax.ShapeDtypeStruct((n_tok, hidden), BF16),
                    in_specs=[vmem] * 4 + [any_spec],
                    out_specs=any_spec,
                    scratch_shapes=[pltpu.VMEM((n_tail // wide, wide, half), BF16), pltpu.VMEM((n_last, half), BF16),
                                    dma((n_tail // wide + 2,)), dma(())],
                    compiler_params=pltpu.CompilerParams(vmem_limit_bytes=10 * 1024 * 1024),
                    name=f'last_{n_c}',
                )(outs[0], outs[1], outs[2], outs[3], outs[-1])

            return last, outs[4]

        last, flag = run(n_tok * 51 // 64, 0)
        return lax.cond(flag[0, 0] > 0, lambda: run(n_tok, 1)[0](), last)

    return jax.shard_map(local_moe, mesh=mesh,
                         in_specs=(row_spec, row_spec, row_spec, P('ep', None, 'tp'), P('ep', 'tp', None)),
                         out_specs=row_spec, check_vma=False)
```

```python
import functools
import math

import jax
import jax.numpy as jnp
from jax import lax
from jax.experimental import pallas as pl
from jax.experimental.pallas import tpu as pltpu
from jax.sharding import PartitionSpec as P

MESH = pl.DeviceIdType.MESH
F32, BF16, I32 = jnp.float32, jnp.bfloat16, jnp.int32
OWN, C, X, XC, Y, YC, XY, XYC = range(8)
N_SRC, N_SIDE = 8, 4
BLK = 128


def capacity(tok_count, n_top, n_exp):
    return ((5 * tok_count * n_top) // (4 * n_exp) + 7) // 8 * 8


def gelu(x):
    c = math.sqrt(2.0 / math.pi)
    return x * (0.5 * (1.0 + jnp.tanh(c * (x + 0.044715 * (x * x * x)))))


def tile_of(i, size):
    return pl.ds(pl.multiple_of(i * size, size), size)


def spread(row, shape):
    return jnp.broadcast_to(row, shape)


def prefix(count):
    lane, step = lax.broadcasted_iota(I32, count.shape, 1), 1
    while step < count.shape[1]:
        count = count + jnp.where(lane >= step, pltpu.roll(count, step, 1), 0)
        step *= 2
    return count


def slots_of(ids, experts, cap):
    shape = experts.shape
    hit = (spread(ids[0:1], shape) == experts) | (spread(ids[1:2], shape) == experts)
    hits = jnp.where(hit, 1, 0)
    rank = prefix(hits) - hits
    return jnp.where(hit & (rank < cap), rank, -1)


def gates_of(ids, gates, experts):
    shape = experts.shape
    return (jnp.where(spread(ids[0:1], shape) == experts, spread(gates[0:1], shape), 0.0)
            + jnp.where(spread(ids[1:2], shape) == experts, spread(gates[1:2], shape), 0.0))


def pack_parts(n_c):
    n = 4 if n_c % 128 == 0 else 3
    return n, -(-n_c // (32 * n)) * 32


def last_block(n_c, wide):
    size = n_c % wide or wide
    return size, (n_c - size) // wide


def last_kernel(first_t, n_c, a_ref, b_ref, acc_ref, tab_ref, rows_hbm, o_hbm, buf, rows, sem, sem_r):
    n_t, wide, half = buf.shape
    n = rows.shape[0]
    get_r = pltpu.make_async_copy(rows_hbm.at[1, pl.ds(n_c - n, n)], rows, sem_r)
    get_r.start()
    lo = pl.ds(0, first_t * wide)
    puts = [pltpu.make_async_copy(a_ref, o_hbm.at[:, pl.ds(0, half)], sem.at[0]),
            pltpu.make_async_copy(b_ref.at[lo], o_hbm.at[lo, pl.ds(half, half)], sem.at[1])]
    for put in puts:
        put.start()
    get_r.wait()
    for i in range(n_t):
        r = pl.ds(i * wide, wide)
        want = (lax.broadcasted_iota(I32, (wide, n), 1) + (n_c - n)).astype(F32)
        p = jnp.where(spread(tab_ref[r, 24:25], want.shape) == want, 1.0, 0.0).astype(BF16)
        got = jnp.dot(p, rows[...], preferred_element_type=F32)
        buf[i] = (acc_ref[r, :] + spread(tab_ref[r, 16:17], got.shape) * got).astype(BF16)
        puts.append(pltpu.make_async_copy(buf.at[i], o_hbm.at[pl.ds((first_t + i) * wide, wide), pl.ds(half, half)], sem.at[2 + i]))
        puts[-1].start()
    for put in puts:
        put.wait()


def moe_kernel(cap, n_c, ids_hbm, gates_hbm, tokens, w_up, w_down,
               out_a, out_b, acc_t, tab_t, flag, tok, tokc, st_up, st_down, wuf, wdf, xs_hbm, h_hbm, part_hbm, rp, rh, rows_hbm,
               idsg, own_gates, meta, cur, pad, tab_h, tab_p,
               ids_s, ids_r, meta_s, meta_r, tok_s, tok_r, pk_s, pk_r, st_s, st_r, wo_s, wo_r, wm_s, wm_r, row_s, row_r, y_s, y_r, lsem):
    n_tok, hidden = tokens.shape
    ffn = w_up.shape[2]
    n_blk = -(-n_c // BLK)
    tp, ep = lax.axis_index('tp'), lax.axis_index('ep')
    core = lax.rem(ep, 2)

    def place(k):
        e = ep + (1 - 2 * core) if k & 1 else ep
        e = lax.rem(e + 2, 4) if k & 2 else e
        return (1 - tp if k & 4 else tp), e

    def rcopy(src, dst, send, recv, k):
        t, e = place(k)
        return pltpu.make_async_remote_copy(src_ref=src, dst_ref=dst, send_sem=send, recv_sem=recv,
                                            device_id={'tp': t, 'ep': e}, device_id_type=MESH)

    hops = {Y: (OWN, Y), X: (OWN, X), C: (OWN, C), XY: (Y, X), YC: (Y, C), XC: (X, C), XYC: (XY, C)}
    n_part, c_part = pack_parts(n_c)
    n_l = n_blk * BLK

    def tok_copy(k):
        frm, to = hops[k]
        if k < N_SIDE:
            return rcopy(tokens if frm == OWN else tok.at[frm], tok.at[k], tok_s.at[k], tok_r.at[k], to)
        rows = pl.ds(0, n_c)
        return rcopy(tok.at[frm, rows], tok.at[k, rows], tok_s.at[k], tok_r.at[k], to)

    def pack_copy(i):
        rows = pl.ds(i * c_part, min(c_part, n_c - i * c_part))
        return rcopy(tokc.at[rows], tok.at[Y, rows], pk_s.at[i], pk_r.at[i], Y)

    def ids_copy(k):
        frm, to = hops[k]
        return rcopy(ids_hbm if frm == OWN else idsg.at[frm], idsg.at[k], ids_s.at[k], ids_r.at[k], to)

    def meta_copy(k):
        frm, to = hops[k]
        lanes = pl.ds(0, n_l)
        return rcopy(meta.at[frm, :, lanes], meta.at[k, :, lanes], meta_s.at[k], meta_r.at[k], to)

    u0 = 256
    um = u0 + (hidden - u0) // 2
    half = hidden // 2

    def piece(i, mate, w):
        if i < 2:
            rows = pl.ds(um, hidden - um) if mate else pl.ds(0, u0) if i == 0 else pl.ds(u0, um - u0)
            return w.at[rows]
        rows = pl.ds(ffn // 2 if mate else 0, ffn // 2)
        return w.at[rows, pl.ds((i - 2) * half, half)] if w.shape[-1] == hidden else w.at[i - 2, rows]

    def staged(i):
        return st_up.at[pl.ds(0, hidden - um)] if i == 1 else st_down.at[i - 2]

    def stage_copy(i):
        return rcopy(piece(i, True, (w_up if i < 2 else w_down).at[1 - tp]), staged(i), st_s.at[i], st_r.at[i], C)

    def own_copy(i):
        src, dst = (w_up, wuf) if i < 2 else (w_down, wdf)
        return rcopy(piece(i, False, src.at[1 - tp]), piece(i, False, dst), wo_s.at[i], wo_r.at[i], Y)

    def mate_copy(i):
        return rcopy(staged(i), piece(i, True, wuf if i < 2 else wdf), wm_s.at[i], wm_r.at[i], YC)

    pieces = (1, 2, 3)

    def wait_piece(i):
        own_copy(i).wait_recv()
        mate_copy(i).wait_recv()

    barrier = pltpu.get_barrier_semaphore()
    partners = (Y, X, C, YC, XC)
    for k in partners:
        t, e = place(k)
        pl.semaphore_signal(barrier, inc=1, device_id={'tp': t, 'ep': e}, device_id_type=MESH)
    pl.semaphore_wait(barrier, len(partners))

    own_copy(0).start()
    for k in (X, C):
        ids_copy(k).start()
        tok_copy(k).start()
    for i in pieces:
        stage_copy(i).start()

    def send_weights():
        for i in pieces:
            stage_copy(i).wait_recv()
        for group in ((1,), (2, 3)):
            @pl.when(core == 0)
            def _():
                for i in group:
                    own_copy(i).start()
                for i in group:
                    mate_copy(i).start()

            @pl.when(core == 1)
            def _():
                for i in group:
                    mate_copy(i).start()
                for i in group:
                    own_copy(i).start()

    def exp_rows(rels):
        row = lax.broadcasted_iota(I32, (8, n_tok), 0)
        experts = jnp.zeros((8, n_tok), I32)
        for i, k in enumerate(rels):
            t, e = place(k)
            experts = jnp.where(row == i, 2 * e + t, experts)
        return experts

    def turn(table):
        @pl.loop(0, n_tok // 128)
        def _(i):
            table[tile_of(i, 128), :] = jnp.transpose(pad[:, tile_of(i, 128)])

    def pack_phase(tokbuf, comp, cbuf, crow):
        get_i = pltpu.make_async_copy(ids_hbm, idsg.at[OWN], lsem.at[0])
        get_g = pltpu.make_async_copy(gates_hbm, own_gates, lsem.at[1])
        get_t = pltpu.make_async_copy(tokens, tokbuf, lsem.at[2])
        for get in (get_i, get_g, get_t):
            get.start()
        pad[...] = jnp.zeros_like(pad)
        if n_l < n_tok:
            for k in range(1, N_SRC):
                meta[k, :, n_l:n_tok] = jnp.full((8, n_tok - n_l), -1.0, F32)
        get_i.wait()
        get_g.wait()
        experts = exp_rows(range(N_SRC))
        slots = slots_of(idsg[OWN], experts, cap)
        gates = gates_of(idsg[OWN], own_gates[...], experts)
        far = (slots >= 0) & (lax.broadcasted_iota(I32, slots.shape, 0) >= N_SIDE)
        count = jnp.sum(jnp.where(far, 1.0, 0.0), axis=0, keepdims=True)
        gate = jnp.sum(jnp.where(far, gates, 0.0), axis=0, keepdims=True)
        cross = spread(jnp.where(count > 0.5, 1, 0), (8, n_tok))
        seen = prefix(cross)
        crow[...] = jnp.where(cross > 0, seen - 1, -1)
        over = jnp.where(jnp.max(seen.astype(F32), axis=1, keepdims=True) > n_c, 1.0, 0.0)
        pad[0:8, :] = slots.astype(F32)
        pad[8:16, :] = gates
        pad[16:24, :] = spread(jnp.where(count > 1.5, 1.0, gate), (8, n_tok))
        pad[24:32, :] = crow[...].astype(F32)
        turn(tab_h)
        get_t.wait()

        def put_c(i):
            return pltpu.make_async_copy(cbuf.at[i], tokc.at[pl.ds(i * c_part, c_part)], lsem.at[3 + i])

        def send_part(i):
            put_c(i).wait()
            pack_copy(i).start()

        @pl.loop(0, n_part)
        def _(i):
            @pl.loop(0, c_part // 32)
            def _(j):
                want = lax.broadcasted_iota(I32, (32, n_tok), 0) + (i * c_part + j * 32)
                comp[tile_of(j, 32), :] = jnp.where(spread(crow[0:1, :], want.shape) == want, 1.0, 0.0).astype(BF16)

            @pl.loop(0, hidden // 512)
            def _(n):
                cols = tile_of(n, 512)
                cbuf[i, :, cols] = jnp.dot(comp[...], tokbuf[:, cols], preferred_element_type=F32).astype(BF16)

            for ii in range(n_part):
                @pl.when(i == ii)
                def _():
                    put_c(ii).start()
                    if ii:
                        send_part(ii - 1)

        @pl.loop(0, n_tok // 128)
        def _(j):
            mask = spread(crow[0:1, :], (128, n_tok)) == lax.broadcasted_iota(I32, (128, n_tok), 0) + j * 128
            lane = lax.broadcasted_iota(I32, (128, 128), 1)
            block = jnp.zeros((128, 128), F32)
            for q in range(4):
                row = idsg[OWN][q:q + 1].astype(F32) + 1.0 if q < 2 else own_gates[q - 2:q - 1, :]
                col = jnp.sum(jnp.where(mask, spread(row, mask.shape), 0.0), axis=1, keepdims=True)
                block = jnp.where(lane == q, spread(col, (128, 128)), block)
            block = jnp.transpose(block)[0:8]
            row = lax.broadcasted_iota(I32, (8, 128), 0)
            block = jnp.where(row < 2, block - 1.0, jnp.where(row == 4, spread(over, (8, 128)), block))
            meta[OWN, :, tile_of(j, 128)] = block

        send_part(n_part - 1)

    pl.run_scoped(pack_phase, pltpu.VMEM((n_tok, hidden), BF16), pltpu.VMEM((c_part, n_tok), BF16),
                  pltpu.VMEM((n_part, c_part, hidden), BF16), pltpu.VMEM((8, n_tok), I32))
    for k in (Y, X, C):
        meta_copy(k).start()

    def proxy_table():
        experts = exp_rows(range(N_SIDE))
        ids = meta[Y, 0:2, :].astype(I32)
        slots = slots_of(ids, experts, cap)
        near = (slots >= 0) & (lax.broadcasted_iota(I32, slots.shape, 0) < N_SIDE)
        gates = gates_of(ids, meta[Y, 2:4, :], experts)
        count = jnp.sum(jnp.where(near, 1.0, 0.0), axis=0, keepdims=True)
        pad[0:8, :] = slots.astype(F32)
        pad[8:16, :] = jnp.where(spread(count, gates.shape) > 1.5, gates, 1.0)
        turn(tab_p)

    my_exp = 2 * ep + tp

    def up_phase(tokbuf, xs, wu, wd, h, part):
        pick = h.at[1, :, pl.ds(0, n_tok)]
        load_d = pltpu.make_async_copy(w_down.at[tp], wd, lsem.at[2])
        load_d.start()

        def load(k):
            if k >= N_SIDE:
                rows = pl.ds(0, n_c)
                return pltpu.make_async_copy(tok.at[k, rows], tokbuf.at[rows], lsem.at[0])
            return pltpu.make_async_copy(tokens if k == OWN else tok.at[k], tokbuf, lsem.at[0])

        def put_x(k):
            return pltpu.make_async_copy(xs.at[0], xs_hbm.at[k], lsem.at[3])

        def put_part(k):
            return pltpu.make_async_copy(part, part_hbm.at[k], lsem.at[4])

        def arrive(k):
            if k == OWN:
                return
            if k < N_SIDE:
                ids_copy(k).wait_recv()
            else:
                meta_copy(k).wait_recv()
            if k == Y:
                for i in range(n_part):
                    pack_copy(i).wait_recv()
            else:
                tok_copy(k).wait_recv()
            for j, (frm, _) in hops.items():
                if frm == k:
                    (ids_copy if j < N_SIDE else meta_copy)(j).start()
                    tok_copy(j).start()

        def at_top(k):
            if k == X:
                send_weights()
                arrive(Y)
                arrive(X)
                meta_copy(X).wait_recv()
                meta_copy(XC).start()
                meta_copy(C).wait_recv()
                proxy_table()
            elif k in (OWN, XY, XYC):
                arrive(k)
            if k in (OWN, X, XY, XYC):
                load(k).start()

        def after_pick(k):
            if k in (C, XC, Y, YC):
                if k != Y:
                    arrive(k)
                load(k).start()

        def up_tiles(x_slot, h_slot):
            @pl.loop(0, ffn // 256)
            def _(n):
                cols = tile_of(n, 256)
                h[h_slot, :, cols] = gelu(jnp.dot(xs[x_slot], wu[:, cols], preferred_element_type=F32)).astype(BF16)

        def near(k, lo):
            for kk in range(N_SRC):
                @pl.when(k == kk)
                def _():
                    at_top(kk)
                    cur[0:2, :] = idsg[kk] if kk < N_SIDE else meta[kk, 0:2, :].astype(I32)
            slots = slots_of(cur[0:2, :], jnp.full((8, n_tok), my_exp, I32), cap)[0:1]

            @pl.loop(0, cap // 80)
            def _(i):
                want = lax.broadcasted_iota(I32, (80, n_tok), 0) + i * 80
                pick[tile_of(i, 80), :] = jnp.where(spread(slots, want.shape) == want, 1.0, 0.0).astype(BF16)

            for kk in (OWN, Y):
                @pl.when((k >= N_SIDE) if kk else (k < N_SIDE))
                def _():
                    load(kk).wait()

            @pl.when(k > lo)
            def _():
                put_x(k - 1).wait()

            @pl.loop(0, hidden // 512)
            def _(n):
                cols = tile_of(n, 512)
                xs[0, :, cols] = jnp.dot(pick[...], tokbuf[:, cols], preferred_element_type=F32).astype(BF16)

            put_x(k).start()
            for kk in range(N_SRC - 1):
                pl.when(k == kk)(functools.partial(after_pick, kk + 1))
            up_tiles(0, 0)

            @pl.when(k > lo)
            def _():
                put_part(k - 1).wait()

            @pl.loop(0, hidden // 512)
            def _(n):
                cols = tile_of(n, 512)
                part[:, cols] = jnp.dot(h[0], wd[:, cols], preferred_element_type=F32)

            put_part(k).start()

        def get_x(k, slot):
            return pltpu.make_async_copy(xs_hbm.at[k], xs.at[slot], lsem.at[3 + slot])

        def put_h(k, slot):
            return pltpu.make_async_copy(h.at[slot], h_hbm.at[k], lsem.at[5 + slot])

        @pl.loop(0, 2)
        def _(rnd):
            lo = rnd * (6 + 2 * core)
            hi = 8 - 2 * (1 - core) * (1 - rnd)

            @pl.when(lo < hi)
            def _():
                load_u = pltpu.make_async_copy(w_up.at[tp], wu, lsem.at[1])
                load_u.start()
                load_u.wait()

                @pl.when(rnd == 0)
                def _():
                    load_d.wait()

                @pl.loop(lo, hi)
                def _(k):
                    near(k, lo)

                put_x(hi - 1).wait()
                put_part(hi - 1).wait()

                @pl.when(rnd == 0)
                def _():
                    own_copy(0).wait_recv()
                    wait_piece(1)

                load_f = pltpu.make_async_copy(wuf, wu, lsem.at[1])
                load_f.start()
                get_x(lo, 0).start()
                load_f.wait()

                @pl.loop(lo, hi)
                def _(k):
                    slot = lax.rem(k, 2)
                    get_x(k, slot).wait()

                    @pl.when(k < hi - 1)
                    def _():
                        get_x(k + 1, 1 - slot).start()

                    @pl.when(k >= lo + 2)
                    def _():
                        put_h(k - 2, slot).wait()

                    up_tiles(slot, slot)
                    put_h(k, slot).start()

                put_h(hi - 2, 0).wait()
                put_h(hi - 1, 1).wait()

    pl.run_scoped(up_phase,
                  pltpu.VMEM((n_tok, hidden), BF16), pltpu.VMEM((2, cap, hidden), BF16),
                  pltpu.VMEM((hidden, ffn), BF16), pltpu.VMEM((ffn, hidden), BF16), pltpu.VMEM((2, cap, ffn), BF16),
                  pltpu.VMEM((cap, hidden), F32))

    meta_copy(XC).wait_recv()
    over = meta[OWN, 4:5, 0:128]
    for k in range(1, N_SRC):
        over = jnp.maximum(over, meta[k, 4:5, 0:128])
    flag[0, 0] = jnp.max(over).astype(I32)

    order = (X, XC, OWN, C)

    def row_copy(block, k, c):
        dst = (rp if k >= N_SIDE else rh).at[c, k % N_SIDE]
        i = k * 2 + c
        if k == OWN:
            return pltpu.make_async_copy(block, dst, row_s.at[i])
        return rcopy(block, dst, row_s.at[i], row_r.at[i], k % N_SIDE)

    def y_copy(merged, c, b, n=BLK):
        rows = pl.ds(b * BLK if isinstance(b, int) else pl.multiple_of(b * BLK, BLK), n)
        i = c * n_blk + b
        return rcopy(merged.at[c, rows], rows_hbm.at[c, rows], y_s.at[i], y_r.at[i], Y)

    end = n_c - (n_blk - 1) * BLK

    def end_phase(merged):
        def finish_and_merge(res, wd, hb, p_in, rpv, selfv, tot):
            def src(i):
                return jnp.where(i < N_SIDE, N_SIDE, 0) + lax.rem(i + 2, N_SIDE)

            def gets(i, c, slot):
                return (pltpu.make_async_copy(h_hbm.at[src(i)], hb.at[slot], lsem.at[slot]),
                        pltpu.make_async_copy(part_hbm.at[src(i), :, tile_of(c, half)], p_in.at[slot], lsem.at[2 + slot]))

            def finish(c):
                for get in gets(0, c, 0):
                    get.start()
                for cc in range(2):
                    pl.when(c == cc)(lambda: wait_piece(2 + cc))
                load_w = pltpu.make_async_copy(wdf.at[c], wd, lsem.at[4])
                load_w.start()
                load_w.wait()

                @pl.loop(0, N_SRC)
                def _(i):
                    slot = lax.rem(i, 2)
                    for get in gets(i, c, slot):
                        get.wait()

                    @pl.when(i < N_SRC - 1)
                    def _():
                        for get in gets(i + 1, c, 1 - slot):
                            get.start()

                    keys = [N_SIDE + k for k in order] + list(order)
                    for j, k in enumerate(keys):
                        if k % N_SIDE:
                            @pl.when((i == j) & (c > 0))
                            def _():
                                row_copy(res.at[j], k, 0).wait_send()

                    @pl.loop(0, half // 512)
                    def _(n):
                        cols = tile_of(n, 512)
                        value = p_in[slot, :, cols] + jnp.dot(hb[slot], wd[:, cols], preferred_element_type=F32)
                        res[i, :, cols] = value.astype(BF16)

                    for j, k in enumerate(keys):
                        @pl.when(i == j)
                        def _():
                            if k == Y:
                                selfv[c] = res[j]
                            elif k == OWN:
                                put = row_copy(res.at[j], k, c)
                                put.start()
                                put.wait()
                            else:
                                row_copy(res.at[j], k, c).start()

            def merge(c):
                fetch = [pltpu.make_async_copy(rp.at[c, e], rpv.at[e - 1], lsem.at[4 + e]) for e in range(1, N_SIDE)]
                for e in range(1, N_SIDE):
                    row_copy(res.at[0], N_SIDE + e, c).wait_recv()
                    fetch[e - 1].start()
                for get in fetch:
                    get.wait()

                @pl.loop(0, n_blk)
                def _(b):
                    rows = tile_of(b, BLK)
                    for e in range(N_SIDE):
                        want = lax.broadcasted_iota(I32, (BLK, cap), 1).astype(F32)
                        p = jnp.where(spread(tab_p[rows, e:e + 1], want.shape) == want, 1.0, 0.0).astype(BF16)
                        got = jnp.dot(p, rpv[e - 1] if e else selfv[c], preferred_element_type=F32)
                        got = spread(tab_p[rows, 8 + e:9 + e], got.shape) * got
                        tot[...] = tot[...] + got if e else got
                    merged[c, rows] = tot[...].astype(BF16)
                    pl.when(b < n_blk - 1)(lambda: y_copy(merged, c, b).start())
                    pl.when(b == n_blk - 1)(lambda: y_copy(merged, c, n_blk - 1, end).start())

            @pl.loop(0, 4)
            def _(s):
                early = core == 0
                turn_f = jnp.where(early, s < 2, lax.rem(s, 2) == 0)
                pl.when(turn_f)(lambda: finish(jnp.where(early, s, s // 2)))
                pl.when(jnp.logical_not(turn_f))(lambda: merge(jnp.where(early, s - 2, s // 2)))

            for j, k in enumerate([N_SIDE + k for k in order] + list(order)):
                if k % N_SIDE:
                    row_copy(res.at[j], k, 1).wait_send()

        rows_t = pltpu.VMEM((2, cap, half), BF16)
        pl.run_scoped(finish_and_merge, pltpu.VMEM((N_SRC, cap, half), BF16), pltpu.VMEM((ffn, half), BF16),
                      pltpu.VMEM((2, cap, ffn), BF16), pltpu.VMEM((2, cap, half), F32),
                      pltpu.VMEM((N_SIDE - 1, cap, half), BF16), rows_t, pltpu.VMEM((BLK, half), F32))

        def home(acc, rbuf, ybuf):
            wide = 256
            n_wide = n_tok // wide
            n_last, first_t = last_block(n_c, wide)

            @pl.loop(0, 2)
            def _(c):
                fetch = [pltpu.make_async_copy(rh.at[c, e], rbuf.at[e], lsem.at[4 + e]) for e in range(N_SIDE)]
                for e in range(N_SIDE):
                    if e != OWN:
                        row_copy(rbuf.at[e], e, c).wait_recv()
                    fetch[e].start()
                for get in fetch:
                    get.wait()

                @pl.loop(0, n_wide)
                def _(i):
                    r = tile_of(i, wide)
                    for e in range(N_SIDE):
                        want = lax.broadcasted_iota(I32, (wide, cap), 1).astype(F32)
                        p = jnp.where(spread(tab_h[r, e:e + 1], want.shape) == want, 1.0, 0.0).astype(BF16)
                        got = jnp.dot(p, rbuf[e], preferred_element_type=F32)
                        got = spread(tab_h[r, 8 + e:9 + e], got.shape) * got
                        acc[r, :] = acc[r, :] + got if e else got

                def emit(i, value):
                    for cc, out in enumerate((out_a, out_b)):
                        @pl.when(c == cc)
                        def _():
                            out[tile_of(i, wide), :] = value().astype(BF16)

                def returned(i, first, n):
                    r = tile_of(i, wide)
                    want = (lax.broadcasted_iota(I32, (wide, n), 1) + first).astype(F32)
                    p = jnp.where(spread(tab_h[r, 24:25], want.shape) == want, 1.0, 0.0).astype(BF16)
                    got = jnp.dot(p, ybuf[0:n, :], preferred_element_type=F32)
                    return acc[r, :] + spread(tab_h[r, 16:17], got.shape) * got

                def fetch_y(first, n):
                    get = pltpu.make_async_copy(rows_hbm.at[c, pl.ds(first, n)], ybuf.at[pl.ds(0, n)], lsem.at[0])
                    get.start()
                    get.wait()

                @pl.loop(0, (n_c - n_last) // wide)
                def _(i):
                    y_copy(merged, c, 2 * i).wait_recv()
                    y_copy(merged, c, 2 * i + 1).wait_recv()
                    fetch_y(pl.multiple_of(i * wide, wide), wide)
                    emit(i, lambda: returned(i, i * wide, wide))

                    @pl.loop(i + 1, n_wide)
                    def _(j):
                        acc[tile_of(j, wide), :] = returned(j, i * wide, wide)

                tail = pl.ds(first_t * wide, (n_wide - first_t) * wide)

                @pl.when(c == 1)
                def _():
                    acc_t[...] = acc[tail, :]
                    tab_t[...] = tab_h[tail, :]

                for b in range((n_c - n_last) // BLK, n_blk):
                    y_copy(merged, c, b, end if b == n_blk - 1 else BLK).wait_recv()

                @pl.when(c == 0)
                def _():
                    fetch_y(n_c - n_last, n_last)

                    @pl.loop(first_t, n_wide)
                    def _(i):
                        emit(i, lambda: returned(i, n_c - n_last, n_last))

        pl.run_scoped(home, pltpu.VMEM((n_tok, half), F32), pltpu.VMEM((N_SIDE, cap, half), BF16),
                      pltpu.VMEM((256, half), BF16))

        for c in range(2):
            @pl.loop(0, n_blk - 1)
            def _(b):
                y_copy(merged, c, b).wait_send()

            y_copy(merged, c, n_blk - 1, end).wait_send()

    pl.run_scoped(end_phase, pltpu.VMEM((2, n_blk * BLK, half), BF16))

    for k in range(1, N_SRC):
        if k < N_SIDE:
            ids_copy(k).wait_send()
        meta_copy(k).wait_send()
        if k != Y:
            tok_copy(k).wait_send()
    for i in range(n_part):
        pack_copy(i).wait_send()
    own_copy(0).wait_send()
    for i in pieces:
        stage_copy(i).wait_send()
        own_copy(i).wait_send()
        mate_copy(i).wait_send()


def solution(mesh):
    row_spec = P(('dp', 'ep', 'tp'), None)
    n_exp = 2 * mesh.shape['ep']

    def local_moe(tokens, expert_ids, gate_vals, w_up, w_down):
        n_tok, hidden = tokens.shape
        ffn = w_up.shape[2]
        cap = capacity(n_tok, expert_ids.shape[1], n_exp)
        n_piece, half = 4, hidden // 2
        any_spec = pl.BlockSpec(memory_space=pl.ANY)
        dma = pltpu.SemaphoreType.DMA

        def run(n_c, collective_id):
            vmem = pl.BlockSpec(memory_space=pltpu.VMEM)
            wide = 256
            n_last, first_t = last_block(n_c, wide)
            n_tail = n_tok - first_t * wide
            shapes = [((1, 1), I32), ((N_SRC, n_tok, hidden), BF16), ((math.prod(pack_parts(n_c)), hidden), BF16),
                      ((half, ffn), BF16), ((2, ffn // 2, half), BF16), ((hidden, ffn), BF16), ((2, ffn, half), BF16),
                      ((N_SRC, cap, hidden), BF16), ((N_SRC, cap, ffn), BF16), ((N_SRC, cap, hidden), F32),
                      ((2, N_SIDE, cap, half), BF16), ((2, N_SIDE, cap, half), BF16), ((2, n_c, half), BF16)]
            outs = pl.pallas_call(
                functools.partial(moe_kernel, cap, n_c),
                out_shape=[pltpu.VMEM((n_tok, half), BF16)] * 2 + [pltpu.VMEM((n_tail, n), F32) for n in (half, 128)] + [jax.ShapeDtypeStruct(s, d) for s, d in shapes],
                in_specs=[any_spec] * 5,
                out_specs=[vmem] * 4 + [pl.BlockSpec(memory_space=pltpu.SMEM)] + [any_spec] * (len(shapes) - 1),
                scratch_shapes=[
                    pltpu.VMEM((N_SIDE, 2, n_tok), I32), pltpu.VMEM((2, n_tok), F32), pltpu.VMEM((N_SRC, 8, n_tok), F32),
                    pltpu.VMEM((8, n_tok), I32), pltpu.VMEM((128, n_tok), F32),
                    pltpu.VMEM((n_tok, 128), F32), pltpu.VMEM((n_tok, 128), F32),
                    dma((N_SIDE,)), dma((N_SIDE,)), dma((N_SRC,)), dma((N_SRC,)), dma((N_SRC,)), dma((N_SRC,)), dma((4,)), dma((4,)),
                    dma((n_piece,)), dma((n_piece,)), dma((n_piece,)), dma((n_piece,)), dma((n_piece,)), dma((n_piece,)),
                    dma((N_SRC * 2,)), dma((N_SRC * 2,)), dma((2 * -(-n_c // BLK),)), dma((2 * -(-n_c // BLK),)),
                    dma((8,)),
                ],
                compiler_params=pltpu.CompilerParams(collective_id=collective_id, has_side_effects=True,
                                                     vmem_limit_bytes=53 * 1024 * 1024),
                name=f'moe_{n_c}',
            )(expert_ids.T, gate_vals.T, tokens, w_up, w_down)

            def last():
                return pl.pallas_call(
                    functools.partial(last_kernel, first_t, n_c),
                    out_shape=jax.ShapeDtypeStruct((n_tok, hidden), BF16),
                    in_specs=[vmem] * 4 + [any_spec],
                    out_specs=any_spec,
                    scratch_shapes=[pltpu.VMEM((n_tail // wide, wide, half), BF16), pltpu.VMEM((n_last, half), BF16),
                                    dma((n_tail // wide + 2,)), dma(())],
                    compiler_params=pltpu.CompilerParams(vmem_limit_bytes=10 * 1024 * 1024),
                    name=f'last_{n_c}',
                )(outs[0], outs[1], outs[2], outs[3], outs[-1])

            return last, outs[4]

        last, flag = run(n_tok * 101 // 128, 0)
        return lax.cond(flag[0, 0] > 0, lambda: run(n_tok, 1)[0](), last)

    return jax.shard_map(local_moe, mesh=mesh,
                         in_specs=(row_spec, row_spec, row_spec, P('ep', None, 'tp'), P('ep', 'tp', None)),
                         out_specs=row_spec, check_vma=False)
```

```python
import functools
import math

import jax
import jax.numpy as jnp
from jax import lax
from jax.experimental import pallas as pl
from jax.experimental.pallas import tpu as pltpu
from jax.sharding import PartitionSpec as P

MESH = pl.DeviceIdType.MESH
F32, BF16, I32 = jnp.float32, jnp.bfloat16, jnp.int32
OWN, C, X, XC, Y, YC, XY, XYC = range(8)
N_SRC, N_SIDE = 8, 4
BLK = 128


def capacity(tok_count, n_top, n_exp):
    return ((5 * tok_count * n_top) // (4 * n_exp) + 7) // 8 * 8


def gelu(x):
    c = math.sqrt(2.0 / math.pi)
    return x * (0.5 * (1.0 + jnp.tanh(c * (x + 0.044715 * (x * x * x)))))


def tile_of(i, size):
    return pl.ds(pl.multiple_of(i * size, size), size)


def spread(row, shape):
    return jnp.broadcast_to(row, shape)


def prefix(count):
    lane, step = lax.broadcasted_iota(I32, count.shape, 1), 1
    while step < count.shape[1]:
        count = count + jnp.where(lane >= step, pltpu.roll(count, step, 1), 0)
        step *= 2
    return count


def slots_of(ids, experts, cap):
    shape = experts.shape
    hit = (spread(ids[0:1], shape) == experts) | (spread(ids[1:2], shape) == experts)
    hits = jnp.where(hit, 1, 0)
    rank = prefix(hits) - hits
    return jnp.where(hit & (rank < cap), rank, -1)


def gates_of(ids, gates, experts):
    shape = experts.shape
    return (jnp.where(spread(ids[0:1], shape) == experts, spread(gates[0:1], shape), 0.0)
            + jnp.where(spread(ids[1:2], shape) == experts, spread(gates[1:2], shape), 0.0))


def pack_parts(n_c):
    n = 4 if n_c % 128 == 0 else 3
    return n, -(-n_c // (32 * n)) * 32


def last_block(n_c, wide):
    size = n_c % wide or wide
    return size, (n_c - size) // wide


def last_kernel(first_t, n_c, a_ref, b_ref, acc_ref, tab_ref, rows_hbm, o_hbm, buf, rows, sem, sem_r):
    n_t, wide, half = buf.shape
    n = rows.shape[0]
    get_r = pltpu.make_async_copy(rows_hbm.at[1, pl.ds(n_c - n, n)], rows, sem_r)
    get_r.start()
    lo = pl.ds(0, first_t * wide)
    puts = [pltpu.make_async_copy(a_ref, o_hbm.at[:, pl.ds(0, half)], sem.at[0]),
            pltpu.make_async_copy(b_ref.at[lo], o_hbm.at[lo, pl.ds(half, half)], sem.at[1])]
    for put in puts:
        put.start()
    get_r.wait()
    for i in range(n_t):
        r = pl.ds(i * wide, wide)
        want = (lax.broadcasted_iota(I32, (wide, n), 1) + (n_c - n)).astype(F32)
        p = jnp.where(spread(tab_ref[r, 24:25], want.shape) == want, 1.0, 0.0).astype(BF16)
        got = jnp.dot(p, rows[...], preferred_element_type=F32)
        buf[i] = (acc_ref[r, :] + spread(tab_ref[r, 16:17], got.shape) * got).astype(BF16)
        puts.append(pltpu.make_async_copy(buf.at[i], o_hbm.at[pl.ds((first_t + i) * wide, wide), pl.ds(half, half)], sem.at[2 + i]))
        puts[-1].start()
    for put in puts:
        put.wait()


def moe_kernel(cap, n_c, ids_hbm, gates_hbm, tokens, w_up, w_down,
               out_a, out_b, acc_t, tab_t, flag, tok, tokc, st_up, st_down, wuf, wdf, xs_hbm, h_hbm, part_hbm, rp, rh, rows_hbm,
               idsg, own_gates, meta, cur, pad, tab_h, tab_p,
               ids_s, ids_r, meta_s, meta_r, tok_s, tok_r, pk_s, pk_r, st_s, st_r, wo_s, wo_r, wm_s, wm_r, row_s, row_r, y_s, y_r, lsem):
    n_tok, hidden = tokens.shape
    ffn = w_up.shape[2]
    n_blk = -(-n_c // BLK)
    tp, ep = lax.axis_index('tp'), lax.axis_index('ep')
    core = lax.rem(ep, 2)

    def place(k):
        e = ep + (1 - 2 * core) if k & 1 else ep
        e = lax.rem(e + 2, 4) if k & 2 else e
        return (1 - tp if k & 4 else tp), e

    def rcopy(src, dst, send, recv, k):
        t, e = place(k)
        return pltpu.make_async_remote_copy(src_ref=src, dst_ref=dst, send_sem=send, recv_sem=recv,
                                            device_id={'tp': t, 'ep': e}, device_id_type=MESH)

    hops = {Y: (OWN, Y), X: (OWN, X), C: (OWN, C), XY: (Y, X), YC: (Y, C), XC: (X, C), XYC: (XY, C)}
    n_part, c_part = pack_parts(n_c)
    n_l = n_blk * BLK

    def tok_copy(k):
        frm, to = hops[k]
        if k < N_SIDE:
            return rcopy(tokens if frm == OWN else tok.at[frm], tok.at[k], tok_s.at[k], tok_r.at[k], to)
        rows = pl.ds(0, n_c)
        return rcopy(tok.at[frm, rows], tok.at[k, rows], tok_s.at[k], tok_r.at[k], to)

    def pack_copy(i):
        rows = pl.ds(i * c_part, min(c_part, n_c - i * c_part))
        return rcopy(tokc.at[rows], tok.at[Y, rows], pk_s.at[i], pk_r.at[i], Y)

    def ids_copy(k):
        frm, to = hops[k]
        return rcopy(ids_hbm if frm == OWN else idsg.at[frm], idsg.at[k], ids_s.at[k], ids_r.at[k], to)

    def meta_copy(k):
        frm, to = hops[k]
        lanes = pl.ds(0, n_l)
        return rcopy(meta.at[frm, :, lanes], meta.at[k, :, lanes], meta_s.at[k], meta_r.at[k], to)

    u0 = 256
    um = u0 + (hidden - u0) // 2
    half = hidden // 2

    def piece(i, mate, w):
        if i < 2:
            rows = pl.ds(um, hidden - um) if mate else pl.ds(0, u0) if i == 0 else pl.ds(u0, um - u0)
            return w.at[rows]
        rows = pl.ds(ffn // 2 if mate else 0, ffn // 2)
        return w.at[rows, pl.ds((i - 2) * half, half)] if w.shape[-1] == hidden else w.at[i - 2, rows]

    def staged(i):
        return st_up.at[pl.ds(0, hidden - um)] if i == 1 else st_down.at[i - 2]

    def stage_copy(i):
        return rcopy(piece(i, True, (w_up if i < 2 else w_down).at[1 - tp]), staged(i), st_s.at[i], st_r.at[i], C)

    def own_copy(i):
        src, dst = (w_up, wuf) if i < 2 else (w_down, wdf)
        return rcopy(piece(i, False, src.at[1 - tp]), piece(i, False, dst), wo_s.at[i], wo_r.at[i], Y)

    def mate_copy(i):
        return rcopy(staged(i), piece(i, True, wuf if i < 2 else wdf), wm_s.at[i], wm_r.at[i], YC)

    pieces = (1, 2, 3)

    def wait_piece(i):
        own_copy(i).wait_recv()
        mate_copy(i).wait_recv()

    def send_weights():
        for i in pieces:
            stage_copy(i).wait_recv()
        for group in ((1,), (2, 3)):
            @pl.when(core == 0)
            def _():
                for i in group:
                    own_copy(i).start()
                for i in group:
                    mate_copy(i).start()

            @pl.when(core == 1)
            def _():
                for i in group:
                    mate_copy(i).start()
                for i in group:
                    own_copy(i).start()

    def ids_of(k):
        code = meta[k, 0:1, :].astype(I32)
        return jnp.concatenate([code >> 3, jnp.where(code < 0, -1, code & 7)], axis=0)

    def exp_rows(rels):
        row = lax.broadcasted_iota(I32, (8, n_tok), 0)
        experts = jnp.zeros((8, n_tok), I32)
        for i, k in enumerate(rels):
            t, e = place(k)
            experts = jnp.where(row == i, 2 * e + t, experts)
        return experts

    def turn(table):
        @pl.loop(0, n_tok // 128)
        def _(i):
            table[tile_of(i, 128), :] = jnp.transpose(pad[:, tile_of(i, 128)])

    def first_copy(ubuf):
        return rcopy(ubuf, piece(0, False, wuf), wo_s.at[0], wo_r.at[0], Y)

    def pack_phase(tokbuf, comp, cbuf, crow, ubuf):
        get_u = pltpu.make_async_copy(piece(0, False, w_up.at[1 - tp]), ubuf, lsem.at[7])
        get_u.start()
        barrier = pltpu.get_barrier_semaphore()
        partners = (Y, X, C, YC, XC)
        for k in partners:
            t, e = place(k)
            pl.semaphore_signal(barrier, inc=1, device_id={'tp': t, 'ep': e}, device_id_type=MESH)
        pl.semaphore_wait(barrier, len(partners))

        get_u.wait()
        first_copy(ubuf).start()
        for k in (X, C):
            ids_copy(k).start()
            tok_copy(k).start()
        for i in pieces:
            stage_copy(i).start()

        get_i = pltpu.make_async_copy(ids_hbm, idsg.at[OWN], lsem.at[0])
        get_g = pltpu.make_async_copy(gates_hbm, own_gates, lsem.at[1])
        get_t = pltpu.make_async_copy(tokens, tokbuf, lsem.at[2])
        for get in (get_i, get_g, get_t):
            get.start()
        pad[...] = jnp.zeros_like(pad)
        if n_l < n_tok:
            for k in range(1, N_SRC):
                meta[k, :, n_l:n_tok] = jnp.full((4, n_tok - n_l), -1.0, F32)
        get_i.wait()
        get_g.wait()
        experts = exp_rows(range(N_SRC))
        slots = slots_of(idsg[OWN], experts, cap)
        gates = gates_of(idsg[OWN], own_gates[...], experts)
        far = (slots >= 0) & (lax.broadcasted_iota(I32, slots.shape, 0) >= N_SIDE)
        count = jnp.sum(jnp.where(far, 1.0, 0.0), axis=0, keepdims=True)
        gate = jnp.sum(jnp.where(far, gates, 0.0), axis=0, keepdims=True)
        cross = spread(jnp.where(count > 0.5, 1, 0), (8, n_tok))
        seen = prefix(cross)
        crow[...] = jnp.where(cross > 0, seen - 1, -1)
        over = jnp.where(jnp.max(seen.astype(F32), axis=1, keepdims=True) > n_c, 1.0, 0.0)
        pad[0:8, :] = slots.astype(F32)
        pad[8:16, :] = gates
        pad[16:24, :] = spread(jnp.where(count > 1.5, 1.0, gate), (8, n_tok))
        pad[24:32, :] = crow[...].astype(F32)
        turn(tab_h)
        get_t.wait()

        def put_c(i):
            return pltpu.make_async_copy(cbuf.at[i], tokc.at[pl.ds(i * c_part, c_part)], lsem.at[3 + i])

        def send_part(i):
            put_c(i).wait()
            pack_copy(i).start()

        @pl.loop(0, n_part)
        def _(i):
            @pl.loop(0, c_part // 32)
            def _(j):
                want = lax.broadcasted_iota(I32, (32, n_tok), 0) + (i * c_part + j * 32)
                comp[tile_of(j, 32), :] = jnp.where(spread(crow[0:1, :], want.shape) == want, 1.0, 0.0).astype(BF16)

            @pl.loop(0, hidden // 512)
            def _(n):
                cols = tile_of(n, 512)
                cbuf[i, :, cols] = jnp.dot(comp[...], tokbuf[:, cols], preferred_element_type=F32).astype(BF16)

            for ii in range(n_part):
                @pl.when(i == ii)
                def _():
                    put_c(ii).start()
                    if ii:
                        send_part(ii - 1)

        @pl.loop(0, n_tok // 128)
        def _(j):
            mask = spread(crow[0:1, :], (128, n_tok)) == lax.broadcasted_iota(I32, (128, n_tok), 0) + j * 128
            lane = lax.broadcasted_iota(I32, (128, 128), 1)
            block = jnp.zeros((128, 128), F32)
            for q in range(3):
                row = own_gates[q - 1:q, :] if q else (idsg[OWN][0:1] * 8 + idsg[OWN][1:2]).astype(F32) + 1.0
                col = jnp.sum(jnp.where(mask, spread(row, mask.shape), 0.0), axis=1, keepdims=True)
                block = jnp.where(lane == q, spread(col, (128, 128)), block)
            block = jnp.transpose(block)[0:8]
            row = lax.broadcasted_iota(I32, (8, 128), 0)
            block = jnp.where(row == 0, block - 1.0, jnp.where(row == 3, spread(over, (8, 128)), block))
            meta[OWN, :, tile_of(j, 128)] = block[0:4]

        send_part(n_part - 1)
        first_copy(ubuf).wait_send()

    pl.run_scoped(pack_phase, pltpu.VMEM((n_tok, hidden), BF16), pltpu.VMEM((c_part, n_tok), BF16),
                  pltpu.VMEM((n_part, c_part, hidden), BF16), pltpu.VMEM((8, n_tok), I32),
                  pltpu.VMEM((u0, ffn), BF16))
    for k in (Y, X, C):
        meta_copy(k).start()

    def proxy_table():
        experts = exp_rows(range(N_SIDE))
        ids = ids_of(Y)
        slots = slots_of(ids, experts, cap)
        near = (slots >= 0) & (lax.broadcasted_iota(I32, slots.shape, 0) < N_SIDE)
        gates = gates_of(ids, meta[Y, 1:3, :], experts)
        count = jnp.sum(jnp.where(near, 1.0, 0.0), axis=0, keepdims=True)
        pad[0:8, :] = slots.astype(F32)
        pad[8:16, :] = jnp.where(spread(count, gates.shape) > 1.5, gates, 1.0)
        turn(tab_p)

    my_exp = 2 * ep + tp

    def up_phase(tokbuf, xs, wu, wd, h, part):
        pick = h.at[1, :, pl.ds(0, n_tok)]
        load_d = pltpu.make_async_copy(w_down.at[tp], wd, lsem.at[2])
        load_d.start()

        def load(k):
            if k >= N_SIDE:
                rows = pl.ds(0, n_c)
                return pltpu.make_async_copy(tok.at[k, rows], tokbuf.at[rows], lsem.at[0])
            return pltpu.make_async_copy(tokens if k == OWN else tok.at[k], tokbuf, lsem.at[0])

        def put_x(k):
            return pltpu.make_async_copy(xs.at[0], xs_hbm.at[k], lsem.at[3])

        def put_part(k):
            return pltpu.make_async_copy(part, part_hbm.at[k], lsem.at[4])

        def arrive(k):
            if k == OWN:
                return
            if k < N_SIDE:
                ids_copy(k).wait_recv()
            else:
                meta_copy(k).wait_recv()
            if k == Y:
                for i in range(n_part):
                    pack_copy(i).wait_recv()
            else:
                tok_copy(k).wait_recv()
            for j, (frm, _) in hops.items():
                if frm == k:
                    (ids_copy if j < N_SIDE else meta_copy)(j).start()
                    tok_copy(j).start()

        def at_top(k):
            if k == X:
                send_weights()
                arrive(Y)
                arrive(X)
                meta_copy(X).wait_recv()
                meta_copy(XC).start()
                meta_copy(C).wait_recv()
                proxy_table()
            elif k in (OWN, XY, XYC):
                arrive(k)
            if k in (OWN, X, XY, XYC):
                load(k).start()

        def after_pick(k):
            if k in (C, XC, Y, YC):
                if k != Y:
                    arrive(k)
                load(k).start()

        def up_tiles(x_slot, h_slot):
            @pl.loop(0, ffn // 256)
            def _(n):
                cols = tile_of(n, 256)
                h[h_slot, :, cols] = gelu(jnp.dot(xs[x_slot], wu[:, cols], preferred_element_type=F32)).astype(BF16)

        def near(k, lo):
            for kk in range(N_SRC):
                @pl.when(k == kk)
                def _():
                    at_top(kk)
                    cur[0:2, :] = idsg[kk] if kk < N_SIDE else ids_of(kk)
            slots = slots_of(cur[0:2, :], jnp.full((8, n_tok), my_exp, I32), cap)[0:1]

            @pl.loop(0, cap // 80)
            def _(i):
                want = lax.broadcasted_iota(I32, (80, n_tok), 0) + i * 80
                pick[tile_of(i, 80), :] = jnp.where(spread(slots, want.shape) == want, 1.0, 0.0).astype(BF16)

            for kk in (OWN, Y):
                @pl.when((k >= N_SIDE) if kk else (k < N_SIDE))
                def _():
                    load(kk).wait()

            @pl.when(k > lo)
            def _():
                put_x(k - 1).wait()

            @pl.loop(0, hidden // 512)
            def _(n):
                cols = tile_of(n, 512)
                xs[0, :, cols] = jnp.dot(pick[...], tokbuf[:, cols], preferred_element_type=F32).astype(BF16)

            put_x(k).start()
            for kk in range(N_SRC - 1):
                pl.when(k == kk)(functools.partial(after_pick, kk + 1))
            up_tiles(0, 0)

            @pl.when(k > lo)
            def _():
                put_part(k - 1).wait()

            @pl.loop(0, hidden // 512)
            def _(n):
                cols = tile_of(n, 512)
                part[:, cols] = jnp.dot(h[0], wd[:, cols], preferred_element_type=F32)

            put_part(k).start()

        def get_x(k, slot):
            return pltpu.make_async_copy(xs_hbm.at[k], xs.at[slot], lsem.at[3 + slot])

        def put_h(k, slot):
            return pltpu.make_async_copy(h.at[slot], h_hbm.at[k], lsem.at[5 + slot])

        @pl.loop(0, 2)
        def _(rnd):
            lo = rnd * (6 + 2 * core)
            hi = 8 - 2 * (1 - core) * (1 - rnd)

            @pl.when(lo < hi)
            def _():
                load_u = pltpu.make_async_copy(w_up.at[tp], wu, lsem.at[1])
                load_u.start()
                load_u.wait()

                @pl.when(rnd == 0)
                def _():
                    load_d.wait()

                @pl.loop(lo, hi)
                def _(k):
                    near(k, lo)

                put_x(hi - 1).wait()
                put_part(hi - 1).wait()

                @pl.when(rnd == 0)
                def _():
                    own_copy(0).wait_recv()
                    wait_piece(1)

                load_f = pltpu.make_async_copy(wuf, wu, lsem.at[1])
                load_f.start()
                get_x(lo, 0).start()
                load_f.wait()

                @pl.loop(lo, hi)
                def _(k):
                    slot = lax.rem(k, 2)
                    get_x(k, slot).wait()

                    @pl.when(k < hi - 1)
                    def _():
                        get_x(k + 1, 1 - slot).start()

                    @pl.when(k >= lo + 2)
                    def _():
                        put_h(k - 2, slot).wait()

                    up_tiles(slot, slot)
                    put_h(k, slot).start()

                put_h(hi - 2, 0).wait()
                put_h(hi - 1, 1).wait()

    pl.run_scoped(up_phase,
                  pltpu.VMEM((n_tok, hidden), BF16), pltpu.VMEM((2, cap, hidden), BF16),
                  pltpu.VMEM((hidden, ffn), BF16), pltpu.VMEM((ffn, hidden), BF16), pltpu.VMEM((2, cap, ffn), BF16),
                  pltpu.VMEM((cap, hidden), F32))

    meta_copy(XC).wait_recv()
    over = meta[OWN, 3:4, 0:128]
    for k in range(1, N_SRC):
        over = jnp.maximum(over, meta[k, 3:4, 0:128])
    flag[0, 0] = jnp.max(over).astype(I32)

    order = (X, XC, OWN, C)

    def row_copy(block, k, c):
        dst = (rp if k >= N_SIDE else rh).at[c, k % N_SIDE]
        i = k * 2 + c
        if k == OWN:
            return pltpu.make_async_copy(block, dst, row_s.at[i])
        return rcopy(block, dst, row_s.at[i], row_r.at[i], k % N_SIDE)

    def y_copy(merged, c, b, n=BLK):
        rows = pl.ds(b * BLK if isinstance(b, int) else pl.multiple_of(b * BLK, BLK), n)
        i = c * n_blk + b
        return rcopy(merged.at[c, rows], rows_hbm.at[c, rows], y_s.at[i], y_r.at[i], Y)

    end = n_c - (n_blk - 1) * BLK

    def sent_all(merged):
        for k in range(1, N_SRC):
            if k < N_SIDE:
                ids_copy(k).wait_send()
            meta_copy(k).wait_send()
            if k != Y:
                tok_copy(k).wait_send()
        for i in range(n_part):
            pack_copy(i).wait_send()
        for i in pieces:
            stage_copy(i).wait_send()
            own_copy(i).wait_send()
            mate_copy(i).wait_send()
        for c in range(2):
            @pl.loop(0, n_blk - 1)
            def _(b):
                y_copy(merged, c, b).wait_send()

        y_copy(merged, 0, n_blk - 1, end).wait_send()

    def end_phase(merged):
        def finish_and_merge(res, wd, hb, p_in, rpv, selfv, tot):
            def src(i):
                return jnp.where(i < N_SIDE, N_SIDE, 0) + lax.rem(i + 2, N_SIDE)

            def gets(i, c, slot):
                return (pltpu.make_async_copy(h_hbm.at[src(i)], hb.at[slot], lsem.at[slot]),
                        pltpu.make_async_copy(part_hbm.at[src(i), :, tile_of(c, half)], p_in.at[slot], lsem.at[2 + slot]))

            def finish(c):
                for get in gets(0, c, 0):
                    get.start()
                for cc in range(2):
                    pl.when(c == cc)(lambda: wait_piece(2 + cc))
                load_w = pltpu.make_async_copy(wdf.at[c], wd, lsem.at[4])
                load_w.start()
                load_w.wait()

                @pl.loop(0, N_SRC)
                def _(i):
                    slot = lax.rem(i, 2)
                    for get in gets(i, c, slot):
                        get.wait()

                    @pl.when(i < N_SRC - 1)
                    def _():
                        for get in gets(i + 1, c, 1 - slot):
                            get.start()

                    keys = [N_SIDE + k for k in order] + list(order)
                    for j, k in enumerate(keys):
                        if k % N_SIDE:
                            @pl.when((i == j) & (c > 0))
                            def _():
                                row_copy(res.at[j], k, 0).wait_send()

                    @pl.loop(0, half // 512)
                    def _(n):
                        cols = tile_of(n, 512)
                        value = p_in[slot, :, cols] + jnp.dot(hb[slot], wd[:, cols], preferred_element_type=F32)
                        res[i, :, cols] = value.astype(BF16)

                    for j, k in enumerate(keys):
                        @pl.when(i == j)
                        def _():
                            if k == Y:
                                selfv[c] = res[j]
                            elif k == OWN:
                                put = row_copy(res.at[j], k, c)
                                put.start()
                                put.wait()
                            else:
                                row_copy(res.at[j], k, c).start()

            def merge(c):
                fetch = [pltpu.make_async_copy(rp.at[c, e], rpv.at[e - 1], lsem.at[4 + e]) for e in range(1, N_SIDE)]
                for e in range(1, N_SIDE):
                    row_copy(res.at[0], N_SIDE + e, c).wait_recv()
                    fetch[e - 1].start()
                for get in fetch:
                    get.wait()

                @pl.loop(0, n_blk)
                def _(b):
                    rows = tile_of(b, BLK)
                    for e in range(N_SIDE):
                        want = lax.broadcasted_iota(I32, (BLK, cap), 1).astype(F32)
                        p = jnp.where(spread(tab_p[rows, e:e + 1], want.shape) == want, 1.0, 0.0).astype(BF16)
                        got = jnp.dot(p, rpv[e - 1] if e else selfv[c], preferred_element_type=F32)
                        got = spread(tab_p[rows, 8 + e:9 + e], got.shape) * got
                        tot[...] = tot[...] + got if e else got
                    merged[c, rows] = tot[...].astype(BF16)
                    pl.when(b < n_blk - 1)(lambda: y_copy(merged, c, b).start())
                    pl.when(b == n_blk - 1)(lambda: y_copy(merged, c, n_blk - 1, end).start())

            @pl.loop(0, 4)
            def _(s):
                early = core == 0
                turn_f = jnp.where(early, s < 2, lax.rem(s, 2) == 0)
                pl.when(turn_f)(lambda: finish(jnp.where(early, s, s // 2)))
                pl.when(jnp.logical_not(turn_f))(lambda: merge(jnp.where(early, s - 2, s // 2)))

            for j, k in enumerate([N_SIDE + k for k in order] + list(order)):
                if k % N_SIDE:
                    row_copy(res.at[j], k, 1).wait_send()

        rows_t = pltpu.VMEM((2, cap, half), BF16)
        pl.run_scoped(finish_and_merge, pltpu.VMEM((N_SRC, cap, half), BF16), pltpu.VMEM((ffn, half), BF16),
                      pltpu.VMEM((2, cap, ffn), BF16), pltpu.VMEM((2, cap, half), F32),
                      pltpu.VMEM((N_SIDE - 1, cap, half), BF16), rows_t, pltpu.VMEM((BLK, half), F32))

        def home(acc, rbuf, ybuf):
            wide = 256
            n_wide = n_tok // wide
            n_last, first_t = last_block(n_c, wide)

            @pl.loop(0, 2)
            def _(c):
                fetch = [pltpu.make_async_copy(rh.at[c, e], rbuf.at[e], lsem.at[4 + e]) for e in range(N_SIDE)]
                for e in range(N_SIDE):
                    if e != OWN:
                        row_copy(rbuf.at[e], e, c).wait_recv()
                    fetch[e].start()
                for get in fetch:
                    get.wait()

                @pl.loop(0, n_wide)
                def _(i):
                    r = tile_of(i, wide)
                    for e in range(N_SIDE):
                        want = lax.broadcasted_iota(I32, (wide, cap), 1).astype(F32)
                        p = jnp.where(spread(tab_h[r, e:e + 1], want.shape) == want, 1.0, 0.0).astype(BF16)
                        got = jnp.dot(p, rbuf[e], preferred_element_type=F32)
                        got = spread(tab_h[r, 8 + e:9 + e], got.shape) * got
                        acc[r, :] = acc[r, :] + got if e else got

                def emit(i, value):
                    for cc, out in enumerate((out_a, out_b)):
                        @pl.when(c == cc)
                        def _():
                            out[tile_of(i, wide), :] = value().astype(BF16)

                def returned(i, first, n):
                    r = tile_of(i, wide)
                    want = (lax.broadcasted_iota(I32, (wide, n), 1) + first).astype(F32)
                    p = jnp.where(spread(tab_h[r, 24:25], want.shape) == want, 1.0, 0.0).astype(BF16)
                    got = jnp.dot(p, ybuf[0:n, :], preferred_element_type=F32)
                    return acc[r, :] + spread(tab_h[r, 16:17], got.shape) * got

                def fetch_y(first, n):
                    get = pltpu.make_async_copy(rows_hbm.at[c, pl.ds(first, n)], ybuf.at[pl.ds(0, n)], lsem.at[0])
                    get.start()
                    get.wait()

                @pl.loop(0, (n_c - n_last) // wide)
                def _(i):
                    y_copy(merged, c, 2 * i).wait_recv()
                    y_copy(merged, c, 2 * i + 1).wait_recv()
                    fetch_y(pl.multiple_of(i * wide, wide), wide)
                    emit(i, lambda: returned(i, i * wide, wide))

                    @pl.loop(i + 1, n_wide)
                    def _(j):
                        acc[tile_of(j, wide), :] = returned(j, i * wide, wide)

                tail = pl.ds(first_t * wide, (n_wide - first_t) * wide)

                @pl.when(c == 1)
                def _():
                    acc_t[...] = acc[tail, :]
                    tab_t[...] = tab_h[tail, :]

                @pl.when(c == 1)
                def _():
                    sent_all(merged)

                for b in range((n_c - n_last) // BLK, n_blk):
                    y_copy(merged, c, b, end if b == n_blk - 1 else BLK).wait_recv()

                @pl.when(c == 0)
                def _():
                    fetch_y(n_c - n_last, n_last)

                    @pl.loop(first_t, n_wide)
                    def _(i):
                        emit(i, lambda: returned(i, n_c - n_last, n_last))

        pl.run_scoped(home, pltpu.VMEM((n_tok, half), F32), pltpu.VMEM((N_SIDE, cap, half), BF16),
                      pltpu.VMEM((256, half), BF16))

        y_copy(merged, 1, n_blk - 1, end).wait_send()

    pl.run_scoped(end_phase, pltpu.VMEM((2, n_blk * BLK, half), BF16))


def solution(mesh):
    row_spec = P(('dp', 'ep', 'tp'), None)
    n_exp = 2 * mesh.shape['ep']

    def local_moe(tokens, expert_ids, gate_vals, w_up, w_down):
        n_tok, hidden = tokens.shape
        ffn = w_up.shape[2]
        cap = capacity(n_tok, expert_ids.shape[1], n_exp)
        n_piece, half = 4, hidden // 2
        any_spec = pl.BlockSpec(memory_space=pl.ANY)
        dma = pltpu.SemaphoreType.DMA

        def run(n_c, collective_id):
            vmem = pl.BlockSpec(memory_space=pltpu.VMEM)
            wide = 256
            n_last, first_t = last_block(n_c, wide)
            n_tail = n_tok - first_t * wide
            shapes = [((1, 1), I32), ((N_SRC, n_tok, hidden), BF16), ((math.prod(pack_parts(n_c)), hidden), BF16),
                      ((half, ffn), BF16), ((2, ffn // 2, half), BF16), ((hidden, ffn), BF16), ((2, ffn, half), BF16),
                      ((N_SRC, cap, hidden), BF16), ((N_SRC, cap, ffn), BF16), ((N_SRC, cap, hidden), F32),
                      ((2, N_SIDE, cap, half), BF16), ((2, N_SIDE, cap, half), BF16), ((2, n_c, half), BF16)]
            outs = pl.pallas_call(
                functools.partial(moe_kernel, cap, n_c),
                out_shape=[pltpu.VMEM((n_tok, half), BF16)] * 2 + [pltpu.VMEM((n_tail, n), F32) for n in (half, 128)] + [jax.ShapeDtypeStruct(s, d) for s, d in shapes],
                in_specs=[any_spec] * 5,
                out_specs=[vmem] * 4 + [pl.BlockSpec(memory_space=pltpu.SMEM)] + [any_spec] * (len(shapes) - 1),
                scratch_shapes=[
                    pltpu.VMEM((N_SIDE, 2, n_tok), I32), pltpu.VMEM((2, n_tok), F32), pltpu.VMEM((N_SRC, 4, n_tok), F32),
                    pltpu.VMEM((8, n_tok), I32), pltpu.VMEM((128, n_tok), F32),
                    pltpu.VMEM((n_tok, 128), F32), pltpu.VMEM((n_tok, 128), F32),
                    dma((N_SIDE,)), dma((N_SIDE,)), dma((N_SRC,)), dma((N_SRC,)), dma((N_SRC,)), dma((N_SRC,)), dma((4,)), dma((4,)),
                    dma((n_piece,)), dma((n_piece,)), dma((n_piece,)), dma((n_piece,)), dma((n_piece,)), dma((n_piece,)),
                    dma((N_SRC * 2,)), dma((N_SRC * 2,)), dma((2 * -(-n_c // BLK),)), dma((2 * -(-n_c // BLK),)),
                    dma((8,)),
                ],
                compiler_params=pltpu.CompilerParams(collective_id=collective_id, has_side_effects=True,
                                                     vmem_limit_bytes=53 * 1024 * 1024),
                name=f'moe_{n_c}',
            )(expert_ids.T, gate_vals.T, tokens, w_up, w_down)

            def last():
                return pl.pallas_call(
                    functools.partial(last_kernel, first_t, n_c),
                    out_shape=jax.ShapeDtypeStruct((n_tok, hidden), BF16),
                    in_specs=[vmem] * 4 + [any_spec],
                    out_specs=any_spec,
                    scratch_shapes=[pltpu.VMEM((n_tail // wide, wide, half), BF16), pltpu.VMEM((n_last, half), BF16),
                                    dma((n_tail // wide + 2,)), dma(())],
                    compiler_params=pltpu.CompilerParams(vmem_limit_bytes=10 * 1024 * 1024),
                    name=f'last_{n_c}',
                )(outs[0], outs[1], outs[2], outs[3], outs[-1])

            return last, outs[4]

        last, flag = run(n_tok * 101 // 128, 0)
        return lax.cond(flag[0, 0] > 0, lambda: run(n_tok, 1)[0](), last)

    return jax.shard_map(local_moe, mesh=mesh,
                         in_specs=(row_spec, row_spec, row_spec, P('ep', None, 'tp'), P('ep', 'tp', None)),
                         out_specs=row_spec, check_vma=False)
```

```python
import functools
import math

import jax
import jax.numpy as jnp
from jax import lax
from jax.experimental import pallas as pl
from jax.experimental.pallas import tpu as pltpu
from jax.sharding import PartitionSpec as P

MESH = pl.DeviceIdType.MESH
F32, BF16, I32 = jnp.float32, jnp.bfloat16, jnp.int32
OWN, C, X, XC, Y, YC, XY, XYC = range(8)
N_SRC, N_SIDE = 8, 4
BLK = 128


def capacity(tok_count, n_top, n_exp):
    return ((5 * tok_count * n_top) // (4 * n_exp) + 7) // 8 * 8


def gelu(x):
    c = math.sqrt(2.0 / math.pi)
    return x * (0.5 * (1.0 + jnp.tanh(c * (x + 0.044715 * (x * x * x)))))


def tile_of(i, size):
    return pl.ds(pl.multiple_of(i * size, size), size)


def spread(row, shape):
    return jnp.broadcast_to(row, shape)


def prefix(count):
    lane, step = lax.broadcasted_iota(I32, count.shape, 1), 1
    while step < count.shape[1]:
        count = count + jnp.where(lane >= step, pltpu.roll(count, step, 1), 0)
        step *= 2
    return count


def slots_of(ids, experts, cap):
    shape = experts.shape
    hit = (spread(ids[0:1], shape) == experts) | (spread(ids[1:2], shape) == experts)
    hits = jnp.where(hit, 1, 0)
    rank = prefix(hits) - hits
    return jnp.where(hit & (rank < cap), rank, -1)


def gates_of(ids, gates, experts):
    shape = experts.shape
    return (jnp.where(spread(ids[0:1], shape) == experts, spread(gates[0:1], shape), 0.0)
            + jnp.where(spread(ids[1:2], shape) == experts, spread(gates[1:2], shape), 0.0))


def pack_parts(n_c):
    n = 4 if n_c % 128 == 0 else 3
    return n, -(-n_c // (32 * n)) * 32


def last_block(n_c, wide):
    size = n_c % wide or wide
    return size, (n_c - size) // wide


def last_kernel(first_t, n_c, a_ref, b_ref, acc_ref, tab_ref, rows_hbm, o_hbm, buf, rows, sem, sem_r):
    n_t, wide, half = buf.shape
    n = rows.shape[0]
    get_r = pltpu.make_async_copy(rows_hbm.at[1, pl.ds(n_c - n, n)], rows, sem_r)
    get_r.start()
    lo = pl.ds(0, first_t * wide)
    puts = [pltpu.make_async_copy(a_ref, o_hbm.at[:, pl.ds(0, half)], sem.at[0]),
            pltpu.make_async_copy(b_ref.at[lo], o_hbm.at[lo, pl.ds(half, half)], sem.at[1])]
    for put in puts:
        put.start()
    get_r.wait()
    for i in range(n_t):
        r = pl.ds(i * wide, wide)
        want = (lax.broadcasted_iota(I32, (wide, n), 1) + (n_c - n)).astype(F32)
        p = jnp.where(spread(tab_ref[r, 24:25], want.shape) == want, 1.0, 0.0).astype(BF16)
        got = jnp.dot(p, rows[...], preferred_element_type=F32)
        buf[i] = (acc_ref[r, :] + spread(tab_ref[r, 16:17], got.shape) * got).astype(BF16)
        puts.append(pltpu.make_async_copy(buf.at[i], o_hbm.at[pl.ds((first_t + i) * wide, wide), pl.ds(half, half)], sem.at[2 + i]))
        puts[-1].start()
    for put in puts:
        put.wait()


def moe_kernel(cap, n_c, n_s, ids_hbm, gates_hbm, tokens, w_up, w_down,
               out_a, out_b, acc_t, tab_t, flag, tok, tokc, st_up, st_down, wuf, wdf, xs_hbm, h_hbm, part_hbm, rp, rh, sh_t, sh_m, rows_hbm,
               idsg, own_gates, meta, cur, pad, tab_h, tab_p,
               ids_s, ids_r, meta_s, meta_r, tok_s, tok_r, pk_s, pk_r, st_s, st_r, wo_s, wo_r, wm_s, wm_r, row_s, row_r, y_s, y_r, sh_s, sh_r, lsem):
    n_tok, hidden = tokens.shape
    ffn = w_up.shape[2]
    n_blk = -(-n_c // BLK)
    tp, ep = lax.axis_index('tp'), lax.axis_index('ep')
    core = lax.rem(ep, 2)

    def place(k):
        e = ep + (1 - 2 * core) if k & 1 else ep
        e = lax.rem(e + 2, 4) if k & 2 else e
        return (1 - tp if k & 4 else tp), e

    def rcopy(src, dst, send, recv, k):
        t, e = place(k)
        return pltpu.make_async_remote_copy(src_ref=src, dst_ref=dst, send_sem=send, recv_sem=recv,
                                            device_id={'tp': t, 'ep': e}, device_id_type=MESH)

    hops = {Y: (OWN, Y), X: (OWN, X), C: (OWN, C), XY: (Y, X), YC: (Y, C), XC: (X, C), XYC: (XY, C)}
    n_part, c_part = pack_parts(n_c)
    n_l = n_blk * BLK
    n_b = n_c - n_s
    spare = pl.ds(n_b, n_s)

    def tok_copy(k):
        frm, to = hops[k]
        if k < N_SIDE:
            return rcopy(tokens if frm == OWN else tok.at[frm], tok.at[k], tok_s.at[k], tok_r.at[k], to)
        rows = pl.ds(0, n_c)
        return rcopy(tok.at[frm, rows], tok.at[k, rows], tok_s.at[k], tok_r.at[k], to)

    def pack_copy(i):
        rows = pl.ds(i * c_part, min(c_part, n_b - i * c_part))
        return rcopy(tokc.at[rows], tok.at[Y, rows], pk_s.at[i], pk_r.at[i], Y)

    def share_copy(i, merged=None):
        j, c = (i, None) if i < 3 else ((i - 3) % 3, (i - 3) // 3)
        if i == 0:
            src, dst, to = tokc.at[spare], sh_t, C
        elif i == 1:
            src, dst, to = tokc.at[spare], tok.at[Y, spare], Y
        elif i == 2:
            src, dst, to = tok.at[Y, spare], tok.at[Y, spare], C
        elif j == 0:
            src, dst, to = merged.at[c, spare], sh_m.at[c], C
        elif j == 1:
            src, dst, to = merged.at[c, spare], rows_hbm.at[c, spare], Y
        else:
            src, dst, to = rows_hbm.at[c, spare], rows_hbm.at[c, spare], C
        return rcopy(src, dst, sh_s.at[i], sh_r.at[i], to)

    def on_core(which):
        return pl.when(core == which)

    def ids_copy(k):
        frm, to = hops[k]
        return rcopy(ids_hbm if frm == OWN else idsg.at[frm], idsg.at[k], ids_s.at[k], ids_r.at[k], to)

    def meta_copy(k):
        frm, to = hops[k]
        lanes = pl.ds(0, n_l)
        return rcopy(meta.at[frm, :, lanes], meta.at[k, :, lanes], meta_s.at[k], meta_r.at[k], to)

    u0 = 256
    um = u0 + (hidden - u0) // 2
    half = hidden // 2

    def piece(i, mate, w):
        if i < 2:
            rows = pl.ds(um, hidden - um) if mate else pl.ds(0, u0) if i == 0 else pl.ds(u0, um - u0)
            return w.at[rows]
        rows = pl.ds(ffn // 2 if mate else 0, ffn // 2)
        return w.at[rows, pl.ds((i - 2) * half, half)] if w.shape[-1] == hidden else w.at[i - 2, rows]

    def staged(i):
        return st_up.at[pl.ds(0, hidden - um)] if i == 1 else st_down.at[i - 2]

    def stage_copy(i):
        return rcopy(piece(i, True, (w_up if i < 2 else w_down).at[1 - tp]), staged(i), st_s.at[i], st_r.at[i], C)

    def own_copy(i):
        src, dst = (w_up, wuf) if i < 2 else (w_down, wdf)
        return rcopy(piece(i, False, src.at[1 - tp]), piece(i, False, dst), wo_s.at[i], wo_r.at[i], Y)

    def mate_copy(i):
        return rcopy(staged(i), piece(i, True, wuf if i < 2 else wdf), wm_s.at[i], wm_r.at[i], YC)

    pieces = (1, 2, 3)

    def wait_piece(i):
        own_copy(i).wait_recv()
        mate_copy(i).wait_recv()

    def send_weights():
        for i in pieces:
            stage_copy(i).wait_recv()
        for group in ((1,), (2, 3)):
            @pl.when(core == 0)
            def _():
                for i in group:
                    own_copy(i).start()
                for i in group:
                    mate_copy(i).start()

            @pl.when(core == 1)
            def _():
                for i in group:
                    mate_copy(i).start()
                for i in group:
                    own_copy(i).start()

    def ids_of(k):
        code = meta[k, 0:1, :].astype(I32)
        return jnp.concatenate([code >> 3, jnp.where(code < 0, -1, code & 7)], axis=0)

    def exp_rows(rels):
        row = lax.broadcasted_iota(I32, (8, n_tok), 0)
        experts = jnp.zeros((8, n_tok), I32)
        for i, k in enumerate(rels):
            t, e = place(k)
            experts = jnp.where(row == i, 2 * e + t, experts)
        return experts

    def turn(table):
        @pl.loop(0, n_tok // 128)
        def _(i):
            table[tile_of(i, 128), :] = jnp.transpose(pad[:, tile_of(i, 128)])

    def first_copy(ubuf):
        return rcopy(ubuf, piece(0, False, wuf), wo_s.at[0], wo_r.at[0], Y)

    def pack_phase(tokbuf, comp, cbuf, crow, ubuf, extra):
        get_u = pltpu.make_async_copy(piece(0, False, w_up.at[1 - tp]), ubuf, lsem.at[7])
        get_u.start()
        barrier = pltpu.get_barrier_semaphore()
        partners = (Y, X, C, YC, XC)
        for k in partners:
            t, e = place(k)
            pl.semaphore_signal(barrier, inc=1, device_id={'tp': t, 'ep': e}, device_id_type=MESH)
        pl.semaphore_wait(barrier, len(partners))

        get_u.wait()
        first_copy(ubuf).start()
        for k in (X, C):
            ids_copy(k).start()
            tok_copy(k).start()
        for i in pieces:
            stage_copy(i).start()

        get_i = pltpu.make_async_copy(ids_hbm, idsg.at[OWN], lsem.at[0])
        get_g = pltpu.make_async_copy(gates_hbm, own_gates, lsem.at[1])
        get_t = pltpu.make_async_copy(tokens, tokbuf, lsem.at[2])
        for get in (get_i, get_g, get_t):
            get.start()
        pad[...] = jnp.zeros_like(pad)
        if n_l < n_tok:
            for k in range(1, N_SRC):
                meta[k, :, n_l:n_tok] = jnp.full((4, n_tok - n_l), -1.0, F32)
        get_i.wait()
        get_g.wait()
        experts = exp_rows(range(N_SRC))
        slots = slots_of(idsg[OWN], experts, cap)
        gates = gates_of(idsg[OWN], own_gates[...], experts)
        far = (slots >= 0) & (lax.broadcasted_iota(I32, slots.shape, 0) >= N_SIDE)
        count = jnp.sum(jnp.where(far, 1.0, 0.0), axis=0, keepdims=True)
        gate = jnp.sum(jnp.where(far, gates, 0.0), axis=0, keepdims=True)
        cross = spread(jnp.where(count > 0.5, 1, 0), (8, n_tok))
        seen = prefix(cross)
        over = jnp.maximum(jnp.max(seen.astype(F32), axis=1, keepdims=True) - n_b, 0.0)
        shift = core * (n_s - spread(over, seen.shape).astype(I32))
        crow[...] = jnp.where(cross > 0, seen - 1 + jnp.where(seen > n_b, shift, 0), -1)
        pad[0:8, :] = slots.astype(F32)
        pad[8:16, :] = gates
        pad[16:24, :] = spread(jnp.where(count > 1.5, 1.0, gate), (8, n_tok))
        pad[24:32, :] = crow[...].astype(F32)
        turn(tab_h)
        get_t.wait()

        def put_c(i):
            return pltpu.make_async_copy(cbuf.at[i], tokc.at[pl.ds(i * c_part, c_part)], lsem.at[3 + i])

        def send_part(i):
            put_c(i).wait()
            pack_copy(i).start()

        @pl.loop(0, n_part)
        def _(i):
            @pl.loop(0, c_part // 32)
            def _(j):
                want = lax.broadcasted_iota(I32, (32, n_tok), 0) + (i * c_part + j * 32)
                comp[tile_of(j, 32), :] = jnp.where(spread(crow[0:1, :], want.shape) == want, 1.0, 0.0).astype(BF16)

            @pl.loop(0, hidden // 512)
            def _(n):
                cols = tile_of(n, 512)
                cbuf[i, :, cols] = jnp.dot(comp[...], tokbuf[:, cols], preferred_element_type=F32).astype(BF16)

            for ii in range(n_part):
                @pl.when(i == ii)
                def _():
                    put_c(ii).start()
                    if ii:
                        send_part(ii - 1)

        @pl.loop(0, n_tok // 128)
        def _(j):
            mask = spread(crow[0:1, :], (128, n_tok)) == lax.broadcasted_iota(I32, (128, n_tok), 0) + j * 128
            lane = lax.broadcasted_iota(I32, (128, 128), 1)
            block = jnp.zeros((128, 128), F32)
            for q in range(3):
                row = own_gates[q - 1:q, :] if q else (idsg[OWN][0:1] * 8 + idsg[OWN][1:2]).astype(F32) + 1.0
                col = jnp.sum(jnp.where(mask, spread(row, mask.shape), 0.0), axis=1, keepdims=True)
                block = jnp.where(lane == q, spread(col, (128, 128)), block)
            block = jnp.transpose(block)[0:8]
            row = lax.broadcasted_iota(I32, (8, 128), 0)
            block = jnp.where(row == 0, block - 1.0, jnp.where(row == 3, spread(over, (8, 128)), block))
            meta[OWN, :, tile_of(j, 128)] = block[0:4]

        send_part(n_part - 1)
        if n_s:
            @on_core(1)
            def _():
                share_copy(0).start()

            @on_core(0)
            def _():
                share_copy(0).wait_recv()
                get = pltpu.make_async_copy(sh_t, extra, lsem.at[0])
                get.start()
                get.wait()
                extra[...] = extra[...] + cbuf[n_part - 1, c_part - n_s:, :]
                put = pltpu.make_async_copy(extra, tokc.at[spare], lsem.at[0])
                put.start()
                put.wait()
                share_copy(1).start()

        first_copy(ubuf).wait_send()

    pl.run_scoped(pack_phase, pltpu.VMEM((n_tok, hidden), BF16), pltpu.VMEM((c_part, n_tok), BF16),
                  pltpu.VMEM((n_part, c_part, hidden), BF16), pltpu.VMEM((8, n_tok), I32),
                  pltpu.VMEM((u0, ffn), BF16), pltpu.VMEM((n_s or 16, hidden), BF16))
    for k in (Y, X, C):
        meta_copy(k).start()

    def proxy_table():
        experts = exp_rows(range(N_SIDE))
        ids = ids_of(Y)
        slots = slots_of(ids, experts, cap)
        near = (slots >= 0) & (lax.broadcasted_iota(I32, slots.shape, 0) < N_SIDE)
        gates = gates_of(ids, meta[Y, 1:3, :], experts)
        count = jnp.sum(jnp.where(near, 1.0, 0.0), axis=0, keepdims=True)
        pad[0:8, :] = slots.astype(F32)
        pad[8:16, :] = jnp.where(spread(count, gates.shape) > 1.5, gates, 1.0)
        turn(tab_p)

    my_exp = 2 * ep + tp

    def up_phase(tokbuf, xs, wu, wd, h, part):
        pick = h.at[1, :, pl.ds(0, n_tok)]
        load_d = pltpu.make_async_copy(w_down.at[tp], wd, lsem.at[2])
        load_d.start()

        def load(k):
            if k >= N_SIDE:
                rows = pl.ds(0, n_c)
                return pltpu.make_async_copy(tok.at[k, rows], tokbuf.at[rows], lsem.at[0])
            return pltpu.make_async_copy(tokens if k == OWN else tok.at[k], tokbuf, lsem.at[0])

        def put_x(k):
            return pltpu.make_async_copy(xs.at[0], xs_hbm.at[k], lsem.at[3])

        def put_part(k):
            return pltpu.make_async_copy(part, part_hbm.at[k], lsem.at[4])

        def arrive(k):
            if k == OWN:
                return
            if k < N_SIDE:
                ids_copy(k).wait_recv()
            else:
                meta_copy(k).wait_recv()
            if k == Y:
                for i in range(n_part):
                    pack_copy(i).wait_recv()
                if n_s:
                    @on_core(0)
                    def _():
                        share_copy(1).wait_recv()
                        share_copy(2).start()

                    @on_core(1)
                    def _():
                        share_copy(2).wait_recv()
            else:
                tok_copy(k).wait_recv()
            for j, (frm, _) in hops.items():
                if frm == k:
                    (ids_copy if j < N_SIDE else meta_copy)(j).start()
                    tok_copy(j).start()

        def at_top(k):
            if k == X:
                send_weights()
                arrive(Y)
                arrive(X)
                meta_copy(X).wait_recv()
                meta_copy(XC).start()
                meta_copy(C).wait_recv()
                proxy_table()
            elif k in (OWN, XY, XYC):
                arrive(k)
            if k in (OWN, X, XY, XYC):
                load(k).start()

        def after_pick(k):
            if k in (C, XC, Y, YC):
                if k != Y:
                    arrive(k)
                load(k).start()

        def up_tiles(x_slot, h_slot):
            @pl.loop(0, ffn // 256)
            def _(n):
                cols = tile_of(n, 256)
                h[h_slot, :, cols] = gelu(jnp.dot(xs[x_slot], wu[:, cols], preferred_element_type=F32)).astype(BF16)

        def near(k, lo):
            for kk in range(N_SRC):
                @pl.when(k == kk)
                def _():
                    at_top(kk)
                    cur[0:2, :] = idsg[kk] if kk < N_SIDE else ids_of(kk)
            slots = slots_of(cur[0:2, :], jnp.full((8, n_tok), my_exp, I32), cap)[0:1]

            @pl.loop(0, cap // 80)
            def _(i):
                want = lax.broadcasted_iota(I32, (80, n_tok), 0) + i * 80
                pick[tile_of(i, 80), :] = jnp.where(spread(slots, want.shape) == want, 1.0, 0.0).astype(BF16)

            for kk in (OWN, Y):
                @pl.when((k >= N_SIDE) if kk else (k < N_SIDE))
                def _():
                    load(kk).wait()

            @pl.when(k > lo)
            def _():
                put_x(k - 1).wait()

            @pl.loop(0, hidden // 512)
            def _(n):
                cols = tile_of(n, 512)
                xs[0, :, cols] = jnp.dot(pick[...], tokbuf[:, cols], preferred_element_type=F32).astype(BF16)

            put_x(k).start()
            for kk in range(N_SRC - 1):
                pl.when(k == kk)(functools.partial(after_pick, kk + 1))
            up_tiles(0, 0)

            @pl.when(k > lo)
            def _():
                put_part(k - 1).wait()

            @pl.loop(0, hidden // 512)
            def _(n):
                cols = tile_of(n, 512)
                part[:, cols] = jnp.dot(h[0], wd[:, cols], preferred_element_type=F32)

            put_part(k).start()

        def get_x(k, slot):
            return pltpu.make_async_copy(xs_hbm.at[k], xs.at[slot], lsem.at[3 + slot])

        def put_h(k, slot):
            return pltpu.make_async_copy(h.at[slot], h_hbm.at[k], lsem.at[5 + slot])

        @pl.loop(0, 2)
        def _(rnd):
            lo = rnd * (6 + 2 * core)
            hi = 8 - 2 * (1 - core) * (1 - rnd)

            @pl.when(lo < hi)
            def _():
                load_u = pltpu.make_async_copy(w_up.at[tp], wu, lsem.at[1])
                load_u.start()
                load_u.wait()

                @pl.when(rnd == 0)
                def _():
                    load_d.wait()

                @pl.loop(lo, hi)
                def _(k):
                    near(k, lo)

                put_x(hi - 1).wait()
                put_part(hi - 1).wait()

                @pl.when(rnd == 0)
                def _():
                    own_copy(0).wait_recv()
                    wait_piece(1)

                load_f = pltpu.make_async_copy(wuf, wu, lsem.at[1])
                load_f.start()
                get_x(lo, 0).start()
                load_f.wait()

                @pl.loop(lo, hi)
                def _(k):
                    slot = lax.rem(k, 2)
                    get_x(k, slot).wait()

                    @pl.when(k < hi - 1)
                    def _():
                        get_x(k + 1, 1 - slot).start()

                    @pl.when(k >= lo + 2)
                    def _():
                        put_h(k - 2, slot).wait()

                    up_tiles(slot, slot)
                    put_h(k, slot).start()

                put_h(hi - 2, 0).wait()
                put_h(hi - 1, 1).wait()

    pl.run_scoped(up_phase,
                  pltpu.VMEM((n_tok, hidden), BF16), pltpu.VMEM((2, cap, hidden), BF16),
                  pltpu.VMEM((hidden, ffn), BF16), pltpu.VMEM((ffn, hidden), BF16), pltpu.VMEM((2, cap, ffn), BF16),
                  pltpu.VMEM((cap, hidden), F32))

    meta_copy(XC).wait_recv()
    over = meta[OWN, 3:4, 0:128] + meta[C, 3:4, 0:128]
    for k in range(2, N_SRC, 2):
        over = jnp.maximum(over, meta[k, 3:4, 0:128] + meta[k + 1, 3:4, 0:128])
    flag[0, 0] = jnp.where(jnp.max(over) > n_s, 1, 0)

    order = (X, XC, OWN, C)

    def row_copy(block, k, c):
        dst = (rp if k >= N_SIDE else rh).at[c, k % N_SIDE]
        i = k * 2 + c
        if k == OWN:
            return pltpu.make_async_copy(block, dst, row_s.at[i])
        return rcopy(block, dst, row_s.at[i], row_r.at[i], k % N_SIDE)

    def y_copy(merged, c, b, n=BLK):
        rows = pl.ds(b * BLK if isinstance(b, int) else pl.multiple_of(b * BLK, BLK), n)
        i = c * n_blk + b
        return rcopy(merged.at[c, rows], rows_hbm.at[c, rows], y_s.at[i], y_r.at[i], Y)

    end = n_b - (n_blk - 1) * BLK

    def sent_all(merged):
        for k in range(1, N_SRC):
            if k < N_SIDE:
                ids_copy(k).wait_send()
            meta_copy(k).wait_send()
            if k != Y:
                tok_copy(k).wait_send()
        for i in range(n_part):
            pack_copy(i).wait_send()
        if n_s:
            @on_core(1)
            def _():
                for i in (0, 4, 5, 7, 8):
                    share_copy(i, merged).wait_send()

            @on_core(0)
            def _():
                for i in (1, 2, 3, 6):
                    share_copy(i, merged).wait_send()

        for i in pieces:
            stage_copy(i).wait_send()
            own_copy(i).wait_send()
            mate_copy(i).wait_send()
        for c in range(2):
            @pl.loop(0, n_blk - 1)
            def _(b):
                y_copy(merged, c, b).wait_send()

        y_copy(merged, 0, n_blk - 1, end).wait_send()

    def end_phase(merged):
        def finish_and_merge(res, wd, hb, p_in, rpv, selfv, tot, extra):
            def src(i):
                return jnp.where(i < N_SIDE, N_SIDE, 0) + lax.rem(i + 2, N_SIDE)

            def gets(i, c, slot):
                return (pltpu.make_async_copy(h_hbm.at[src(i)], hb.at[slot], lsem.at[slot]),
                        pltpu.make_async_copy(part_hbm.at[src(i), :, tile_of(c, half)], p_in.at[slot], lsem.at[2 + slot]))

            def finish(c):
                for get in gets(0, c, 0):
                    get.start()
                for cc in range(2):
                    pl.when(c == cc)(lambda: wait_piece(2 + cc))
                load_w = pltpu.make_async_copy(wdf.at[c], wd, lsem.at[4])
                load_w.start()
                load_w.wait()

                @pl.loop(0, N_SRC)
                def _(i):
                    slot = lax.rem(i, 2)
                    for get in gets(i, c, slot):
                        get.wait()

                    @pl.when(i < N_SRC - 1)
                    def _():
                        for get in gets(i + 1, c, 1 - slot):
                            get.start()

                    keys = [N_SIDE + k for k in order] + list(order)
                    for j, k in enumerate(keys):
                        if k % N_SIDE:
                            @pl.when((i == j) & (c > 0))
                            def _():
                                row_copy(res.at[j], k, 0).wait_send()

                    @pl.loop(0, half // 512)
                    def _(n):
                        cols = tile_of(n, 512)
                        value = p_in[slot, :, cols] + jnp.dot(hb[slot], wd[:, cols], preferred_element_type=F32)
                        res[i, :, cols] = value.astype(BF16)

                    for j, k in enumerate(keys):
                        @pl.when(i == j)
                        def _():
                            if k == Y:
                                selfv[c] = res[j]
                            elif k == OWN:
                                put = row_copy(res.at[j], k, c)
                                put.start()
                                put.wait()
                            else:
                                row_copy(res.at[j], k, c).start()

            def merge(c):
                fetch = [pltpu.make_async_copy(rp.at[c, e], rpv.at[e - 1], lsem.at[4 + e]) for e in range(1, N_SIDE)]
                for e in range(1, N_SIDE):
                    row_copy(res.at[0], N_SIDE + e, c).wait_recv()
                    fetch[e - 1].start()
                for get in fetch:
                    get.wait()

                @pl.loop(0, n_blk)
                def _(i):
                    b = lax.rem(i + n_blk - 1, n_blk)
                    rows = tile_of(b, BLK)
                    for e in range(N_SIDE):
                        want = lax.broadcasted_iota(I32, (BLK, cap), 1).astype(F32)
                        p = jnp.where(spread(tab_p[rows, e:e + 1], want.shape) == want, 1.0, 0.0).astype(BF16)
                        got = jnp.dot(p, rpv[e - 1] if e else selfv[c], preferred_element_type=F32)
                        got = spread(tab_p[rows, 8 + e:9 + e], got.shape) * got
                        tot[...] = tot[...] + got if e else got
                    merged[c, rows] = tot[...].astype(BF16)
                    pl.when(b < n_blk - 1)(lambda: y_copy(merged, c, b).start())
                    if n_s:
                        for cc in range(2):
                            @pl.when((i == 0) & (core == 0) & (c == cc))
                            def _():
                                share_copy(3 + 3 * cc, merged).start()

                            @pl.when((i == n_blk // 2) & (core == 1) & (c == cc))
                            def _():
                                share_copy(3 + 3 * cc, merged).wait_recv()
                                get = pltpu.make_async_copy(sh_m.at[cc], extra, lsem.at[4])
                                get.start()
                                get.wait()
                                merged[cc, spare] = merged[cc, spare] + extra[...]
                                share_copy(4 + 3 * cc, merged).start()

                y_copy(merged, c, n_blk - 1, end).start()

            @pl.loop(0, 4)
            def _(s):
                early = core == 0
                turn_f = jnp.where(early, s < 2, lax.rem(s, 2) == 0)
                pl.when(turn_f)(lambda: finish(jnp.where(early, s, s // 2)))
                pl.when(jnp.logical_not(turn_f))(lambda: merge(jnp.where(early, s - 2, s // 2)))

            for j, k in enumerate([N_SIDE + k for k in order] + list(order)):
                if k % N_SIDE:
                    row_copy(res.at[j], k, 1).wait_send()

        rows_t = pltpu.VMEM((2, cap, half), BF16)
        pl.run_scoped(finish_and_merge, pltpu.VMEM((N_SRC, cap, half), BF16), pltpu.VMEM((ffn, half), BF16),
                      pltpu.VMEM((2, cap, ffn), BF16), pltpu.VMEM((2, cap, half), F32),
                      pltpu.VMEM((N_SIDE - 1, cap, half), BF16), rows_t, pltpu.VMEM((BLK, half), F32),
                      pltpu.VMEM((n_s or 16, half), BF16))

        def home(acc, rbuf, ybuf):
            wide = 256
            n_wide = n_tok // wide
            n_last, first_t = last_block(n_c, wide)

            @pl.loop(0, 2)
            def _(c):
                fetch = [pltpu.make_async_copy(rh.at[c, e], rbuf.at[e], lsem.at[4 + e]) for e in range(N_SIDE)]
                for e in range(N_SIDE):
                    if e != OWN:
                        row_copy(rbuf.at[e], e, c).wait_recv()
                    fetch[e].start()
                for get in fetch:
                    get.wait()

                @pl.loop(0, n_wide)
                def _(i):
                    r = tile_of(i, wide)
                    for e in range(N_SIDE):
                        want = lax.broadcasted_iota(I32, (wide, cap), 1).astype(F32)
                        p = jnp.where(spread(tab_h[r, e:e + 1], want.shape) == want, 1.0, 0.0).astype(BF16)
                        got = jnp.dot(p, rbuf[e], preferred_element_type=F32)
                        got = spread(tab_h[r, 8 + e:9 + e], got.shape) * got
                        acc[r, :] = acc[r, :] + got if e else got

                if n_s:
                    for cc in range(2):
                        @pl.when((core == 1) & (c == cc))
                        def _():
                            share_copy(4 + 3 * cc, merged).wait_recv()
                            share_copy(5 + 3 * cc, merged).start()

                def emit(i, value):
                    for cc, out in enumerate((out_a, out_b)):
                        @pl.when(c == cc)
                        def _():
                            out[tile_of(i, wide), :] = value().astype(BF16)

                def returned(i, first, n):
                    r = tile_of(i, wide)
                    want = (lax.broadcasted_iota(I32, (wide, n), 1) + first).astype(F32)
                    p = jnp.where(spread(tab_h[r, 24:25], want.shape) == want, 1.0, 0.0).astype(BF16)
                    got = jnp.dot(p, ybuf[0:n, :], preferred_element_type=F32)
                    return acc[r, :] + spread(tab_h[r, 16:17], got.shape) * got

                def fetch_y(first, n):
                    get = pltpu.make_async_copy(rows_hbm.at[c, pl.ds(first, n)], ybuf.at[pl.ds(0, n)], lsem.at[0])
                    get.start()
                    get.wait()

                @pl.loop(0, (n_c - n_last) // wide)
                def _(i):
                    y_copy(merged, c, 2 * i).wait_recv()
                    y_copy(merged, c, 2 * i + 1).wait_recv()
                    fetch_y(pl.multiple_of(i * wide, wide), wide)
                    emit(i, lambda: returned(i, i * wide, wide))

                    @pl.loop(i + 1, n_wide)
                    def _(j):
                        acc[tile_of(j, wide), :] = returned(j, i * wide, wide)

                tail = pl.ds(first_t * wide, (n_wide - first_t) * wide)

                @pl.when(c == 1)
                def _():
                    acc_t[...] = acc[tail, :]
                    tab_t[...] = tab_h[tail, :]

                @pl.when(c == 1)
                def _():
                    sent_all(merged)

                if n_s:
                    for cc in range(2):
                        @pl.when((core == 0) & (c == cc))
                        def _():
                            share_copy(5 + 3 * cc, merged).wait_recv()

                for b in range((n_c - n_last) // BLK, n_blk):
                    y_copy(merged, c, b, end if b == n_blk - 1 else BLK).wait_recv()

                @pl.when(c == 0)
                def _():
                    fetch_y(n_c - n_last, n_last)

                    @pl.loop(first_t, n_wide)
                    def _(i):
                        emit(i, lambda: returned(i, n_c - n_last, n_last))

        pl.run_scoped(home, pltpu.VMEM((n_tok, half), F32), pltpu.VMEM((N_SIDE, cap, half), BF16),
                      pltpu.VMEM((256, half), BF16))

        y_copy(merged, 1, n_blk - 1, end).wait_send()

    pl.run_scoped(end_phase, pltpu.VMEM((2, n_blk * BLK, half), BF16))


def solution(mesh):
    row_spec = P(('dp', 'ep', 'tp'), None)
    n_exp = 2 * mesh.shape['ep']

    def local_moe(tokens, expert_ids, gate_vals, w_up, w_down):
        n_tok, hidden = tokens.shape
        ffn = w_up.shape[2]
        cap = capacity(n_tok, expert_ids.shape[1], n_exp)
        n_piece, half = 4, hidden // 2
        any_spec = pl.BlockSpec(memory_space=pl.ANY)
        dma = pltpu.SemaphoreType.DMA

        def run(n_c, n_s, collective_id):
            vmem = pl.BlockSpec(memory_space=pltpu.VMEM)
            wide = 256
            n_last, first_t = last_block(n_c, wide)
            n_tail = n_tok - first_t * wide
            shapes = [((1, 1), I32), ((N_SRC, n_tok, hidden), BF16), ((math.prod(pack_parts(n_c)), hidden), BF16),
                      ((half, ffn), BF16), ((2, ffn // 2, half), BF16), ((hidden, ffn), BF16), ((2, ffn, half), BF16),
                      ((N_SRC, cap, hidden), BF16), ((N_SRC, cap, ffn), BF16), ((N_SRC, cap, hidden), F32),
                      ((2, N_SIDE, cap, half), BF16), ((2, N_SIDE, cap, half), BF16), ((n_s or 16, hidden), BF16),
                      ((2, n_s or 16, half), BF16), ((2, n_c, half), BF16)]
            outs = pl.pallas_call(
                functools.partial(moe_kernel, cap, n_c, n_s),
                out_shape=[pltpu.VMEM((n_tok, half), BF16)] * 2 + [pltpu.VMEM((n_tail, n), F32) for n in (half, 128)] + [jax.ShapeDtypeStruct(s, d) for s, d in shapes],
                in_specs=[any_spec] * 5,
                out_specs=[vmem] * 4 + [pl.BlockSpec(memory_space=pltpu.SMEM)] + [any_spec] * (len(shapes) - 1),
                scratch_shapes=[
                    pltpu.VMEM((N_SIDE, 2, n_tok), I32), pltpu.VMEM((2, n_tok), F32), pltpu.VMEM((N_SRC, 4, n_tok), F32),
                    pltpu.VMEM((8, n_tok), I32), pltpu.VMEM((128, n_tok), F32),
                    pltpu.VMEM((n_tok, 128), F32), pltpu.VMEM((n_tok, 128), F32),
                    dma((N_SIDE,)), dma((N_SIDE,)), dma((N_SRC,)), dma((N_SRC,)), dma((N_SRC,)), dma((N_SRC,)), dma((4,)), dma((4,)),
                    dma((n_piece,)), dma((n_piece,)), dma((n_piece,)), dma((n_piece,)), dma((n_piece,)), dma((n_piece,)),
                    dma((N_SRC * 2,)), dma((N_SRC * 2,)), dma((2 * -(-n_c // BLK),)), dma((2 * -(-n_c // BLK),)), dma((9,)), dma((9,)),
                    dma((8,)),
                ],
                compiler_params=pltpu.CompilerParams(collective_id=collective_id, has_side_effects=True,
                                                     vmem_limit_bytes=53 * 1024 * 1024),
                name=f'moe_{n_c}',
            )(expert_ids.T, gate_vals.T, tokens, w_up, w_down)

            def last():
                return pl.pallas_call(
                    functools.partial(last_kernel, first_t, n_c),
                    out_shape=jax.ShapeDtypeStruct((n_tok, hidden), BF16),
                    in_specs=[vmem] * 4 + [any_spec],
                    out_specs=any_spec,
                    scratch_shapes=[pltpu.VMEM((n_tail // wide, wide, half), BF16), pltpu.VMEM((n_last, half), BF16),
                                    dma((n_tail // wide + 2,)), dma(())],
                    compiler_params=pltpu.CompilerParams(vmem_limit_bytes=10 * 1024 * 1024),
                    name=f'last_{n_c}',
                )(outs[0], outs[1], outs[2], outs[3], outs[-1])

            return last, outs[4]

        last, flag = run(n_tok * 51 // 64, n_tok // 32, 0)
        return lax.cond(flag[0, 0] > 0, lambda: run(n_tok, 0, 1)[0](), last)

    return jax.shard_map(local_moe, mesh=mesh,
                         in_specs=(row_spec, row_spec, row_spec, P('ep', None, 'tp'), P('ep', 'tp', None)),
                         out_specs=row_spec, check_vma=False)
```
